32 devices in a mesh: dp: 2 (over x), pp: 4 (over z), ep: 4 (over y, core).
Axes of the slice: x: 2, y: 2, z: 4, core: 2. Of those that a mesh axis runs over, the one named last changes fastest.
Arguments:
- x_a: bfloat16 [8, 4, 128, 768], P(('dp', 'pp'), 'ep'), parts along dimension 0
- x_b: bfloat16 [8, 4, 128, 768], P(('dp', 'pp'), 'ep'), parts along dimension 0
- g_b: bfloat16 [8, 4, 128, 768], P(('dp', 'pp'), 'ep'), parts along dimension 0
- ids_a: int32 [8, 4, 128, 2], P(('dp', 'pp'), 'ep'), parts along dimension 0
- ids_b: int32 [8, 4, 128, 2], P(('dp', 'pp'), 'ep'), parts along dimension 0
- count_a: int32 [8, 4, 8], P(('dp', 'pp'), 'ep'), parts along dimension 0
- count_b: int32 [8, 4, 8], P(('dp', 'pp'), 'ep'), parts along dimension 0
- gain_1: bfloat16 [4, 768], P('pp')
- gain_2: bfloat16 [4, 768], P('pp')
- w_q: bfloat16 [4, 768, 6, 128], P('pp')
- w_k: bfloat16 [4, 768, 1, 128], P('pp')
- w_v: bfloat16 [4, 768, 1, 128], P('pp')
- w_o: bfloat16 [4, 6, 128, 768], P('pp')
- w_r: bfloat16 [4, 768, 8], P('pp')
- w_1: bfloat16 [4, 8, 768, 2048], P('pp', 'ep')
- w_3: bfloat16 [4, 8, 768, 2048], P('pp', 'ep')
- w_2: bfloat16 [4, 8, 2048, 768], P('pp', 'ep')
Outputs:
- output 1: bfloat16 [8, 4, 128, 768], P(('dp', 'pp'), 'ep'), parts along dimension 0
- output 2: bfloat16 [8, 4, 128, 768], P(('dp', 'pp'), 'ep'), parts along dimension 0
- output 3: float32 [8, 768], P(('dp', 'pp')), parts along dimension 0
- output 4: float32 [8, 768], P(('dp', 'pp')), parts along dimension 0
- output 5: float32 [8, 768, 6, 128], P(('dp', 'pp')), parts along dimension 0
- output 6: float32 [8, 768, 1, 128], P(('dp', 'pp')), parts along dimension 0
- output 7: float32 [8, 768, 1, 128], P(('dp', 'pp')), parts along dimension 0
- output 8: float32 [8, 6, 128, 768], P(('dp', 'pp')), parts along dimension 0
- output 9: float32 [8, 768, 8], P(('dp', 'pp')), parts along dimension 0
- output 10: float32 [8, 8, 768, 2048], P(('dp', 'pp'), 'ep'), parts along dimension 0
- output 11: float32 [8, 8, 768, 2048], P(('dp', 'pp'), 'ep'), parts along dimension 0
- output 12: float32 [8, 8, 2048, 768], P(('dp', 'pp'), 'ep'), parts along dimension 0
There are 2 independent parts. The reference program is written for one: setup_inputs(seed, part) draws one part's arguments, and reference() takes and returns one part's arrays. A program takes and returns all parts, laid end to end along the dimension named above; an argument that names none is the same for every part.
All inputs are finite; a program needn't handle non-finite values.
Results may differ from the reference program's by a relative error of at most 0.019921.
Values are sent between devices in bfloat16 or wider.
A program may use at most 1 GiB of HBM per device.

```python
import jax
import jax.numpy as jnp
from jax import lax

D_MODEL = 768
HEADS = 6
KV_HEADS = 1
HEAD_DIM = 128
EXPERTS = 8
FFN_DIM = 2048
TOP_K = 2
SEQ_COUNT = 1
SEQ_LEN = 128
PP_SIZE = 4
EP_SIZE = 4
LOAD_FACTOR = 4
TOK_DEV = SEQ_COUNT * SEQ_LEN
CAPACITY = min(TOK_DEV, LOAD_FACTOR * TOK_DEV * TOP_K // EXPERTS)
HOT_EXPERTS = max(1, EXPERTS // 8)
NORM_EPS = 1e-6


def normal_bf(rng_key, arr_shape, w_scale):
    return (jax.random.normal(rng_key, arr_shape, jnp.float32) * w_scale).astype(jnp.bfloat16)


def routing_draw(rng_key):
    perm_key, tok_key = jax.random.split(rng_key)
    rest_count = EXPERTS - HOT_EXPERTS
    rest_total = TOK_DEV * TOP_K - HOT_EXPERTS * CAPACITY
    rest_loads = rest_total // rest_count + (jnp.arange(rest_count) < rest_total % rest_count).astype(jnp.int32)
    ordered = jnp.concatenate([jnp.full((HOT_EXPERTS,), CAPACITY, jnp.int32), rest_loads.astype(jnp.int32)])
    counts = jnp.zeros((EXPERTS,), jnp.int32).at[jax.random.permutation(perm_key, EXPERTS)].set(ordered)
    bounds = jnp.cumsum(counts)
    position = jnp.arange(TOK_DEV * TOP_K)
    column_ids = jnp.sum((position[:, None] >= bounds[None, :]).astype(jnp.int32), axis=1)
    route_ids = column_ids.reshape(TOP_K, TOK_DEV).T[jax.random.permutation(tok_key, TOK_DEV)]
    return route_ids.reshape(SEQ_COUNT, SEQ_LEN, TOP_K), counts


def routing_tables(rng_key):
    route_ids, counts = jax.vmap(routing_draw)(jax.random.split(rng_key, PP_SIZE * EP_SIZE))
    return (route_ids.reshape(PP_SIZE, EP_SIZE * SEQ_COUNT, SEQ_LEN, TOP_K), counts.reshape(PP_SIZE, EP_SIZE, EXPERTS))


def setup_inputs(seed: int = 0, part: int = 0) -> dict:
    weight_root, part_root = jax.random.split(jax.random.key(seed))
    part_keys = jax.random.split(jax.random.fold_in(part_root, part), 5)
    w_keys = jax.random.split(weight_root, 11)
    tok_shape = (PP_SIZE, EP_SIZE * SEQ_COUNT, SEQ_LEN, D_MODEL)
    ids_a, count_a = routing_tables(part_keys[3])
    ids_b, count_b = routing_tables(part_keys[4])
    return {
        'x_a': normal_bf(part_keys[0], tok_shape, 1.0),
        'x_b': normal_bf(part_keys[1], tok_shape, 1.0),
        'g_b': normal_bf(part_keys[2], tok_shape, 1.0),
        'ids_a': ids_a,
        'ids_b': ids_b,
        'count_a': count_a,
        'count_b': count_b,
        'gain_1': (1.0 + 0.3 * jax.random.normal(w_keys[0], (PP_SIZE, D_MODEL), jnp.float32)).astype(jnp.bfloat16),
        'gain_2': (1.0 + 0.3 * jax.random.normal(w_keys[1], (PP_SIZE, D_MODEL), jnp.float32)).astype(jnp.bfloat16),
        'w_q': normal_bf(w_keys[2], (PP_SIZE, D_MODEL, HEADS, HEAD_DIM), D_MODEL ** -0.5),
        'w_k': normal_bf(w_keys[3], (PP_SIZE, D_MODEL, KV_HEADS, HEAD_DIM), D_MODEL ** -0.5),
        'w_v': normal_bf(w_keys[4], (PP_SIZE, D_MODEL, KV_HEADS, HEAD_DIM), D_MODEL ** -0.5),
        'w_o': normal_bf(w_keys[5], (PP_SIZE, HEADS, HEAD_DIM, D_MODEL), (HEADS * HEAD_DIM) ** -0.5),
        'w_r': normal_bf(w_keys[6], (PP_SIZE, D_MODEL, EXPERTS), D_MODEL ** -0.5),
        'w_1': normal_bf(w_keys[7], (PP_SIZE, EXPERTS, D_MODEL, FFN_DIM), D_MODEL ** -0.5),
        'w_3': normal_bf(w_keys[8], (PP_SIZE, EXPERTS, D_MODEL, FFN_DIM), D_MODEL ** -0.5),
        'w_2': normal_bf(w_keys[9], (PP_SIZE, EXPERTS, FFN_DIM, D_MODEL), FFN_DIM ** -0.5),
    }


def rms_scale(x_f32, gain):
    inv_rms = lax.rsqrt(jnp.mean(x_f32 * x_f32, axis=-1, keepdims=True) + NORM_EPS)
    return (x_f32 * inv_rms * gain.astype(jnp.float32)).astype(jnp.bfloat16)


def attention_one(seq_args):
    query_s, key_s, value_s = seq_args
    scores = jnp.einsum('sgrk,tgk->grst', query_s.astype(jnp.float32), key_s.astype(jnp.float32)) * HEAD_DIM ** -0.5
    causal = jnp.arange(SEQ_LEN)[:, None] >= jnp.arange(SEQ_LEN)[None, :]
    probs_f32 = jax.nn.softmax(jnp.where(causal, scores, -1e30), axis=-1)
    probs_bf = probs_f32.astype(jnp.bfloat16).astype(jnp.float32)
    return jnp.einsum('grst,tgk->sgrk', probs_bf, value_s.astype(jnp.float32)).astype(jnp.bfloat16)


def expert_one(expert_args):
    row_block, e_w1, e_w3, e_w2 = expert_args
    gate_pre = jnp.dot(row_block, e_w1, preferred_element_type=jnp.float32)
    up_pre = jnp.dot(row_block, e_w3, preferred_element_type=jnp.float32)
    act_bf = (jax.nn.silu(gate_pre) * up_pre).astype(jnp.bfloat16)
    return jnp.dot(act_bf, e_w2, preferred_element_type=jnp.float32).astype(jnp.bfloat16)


def layer_forward(x_seq, route_ids, counts, gain_1, gain_2, w_q, w_k, w_v, w_o, w_r, w_1, w_3, w_2):
    group_rep = HEADS // KV_HEADS
    n_tok = EP_SIZE * TOK_DEV
    x_f32 = x_seq.reshape(n_tok, D_MODEL).astype(jnp.float32)
    normed = rms_scale(x_f32, gain_1)
    query_all = jnp.dot(normed, w_q.reshape(D_MODEL, HEADS * HEAD_DIM), preferred_element_type=jnp.float32).astype(jnp.bfloat16).reshape(-1, SEQ_LEN, KV_HEADS, group_rep, HEAD_DIM)
    key_all = jnp.dot(normed, w_k.reshape(D_MODEL, KV_HEADS * HEAD_DIM), preferred_element_type=jnp.float32).astype(jnp.bfloat16).reshape(-1, SEQ_LEN, KV_HEADS, HEAD_DIM)
    value_all = jnp.dot(normed, w_v.reshape(D_MODEL, KV_HEADS * HEAD_DIM), preferred_element_type=jnp.float32).astype(jnp.bfloat16).reshape(-1, SEQ_LEN, KV_HEADS, HEAD_DIM)
    attn_out = lax.map(attention_one, (query_all, key_all, value_all))
    attn_proj = jnp.dot(attn_out.reshape(n_tok, HEADS * HEAD_DIM), w_o.reshape(HEADS * HEAD_DIM, D_MODEL), preferred_element_type=jnp.float32)
    hid_f32 = (x_f32 + attn_proj).astype(jnp.bfloat16).astype(jnp.float32)
    normed_2 = rms_scale(hid_f32, gain_2)
    logits = jnp.dot(normed_2, w_r, preferred_element_type=jnp.float32)
    sel_ids = route_ids.reshape(n_tok, TOP_K)
    chosen = sel_ids[:, :, None] == jnp.arange(EXPERTS)[None, None, :]
    gate_w = jax.nn.softmax(jnp.sum(jnp.where(chosen, logits[:, None, :], 0.0), axis=-1), axis=-1)
    per_src = chosen.reshape(EP_SIZE, TOK_DEV * TOP_K, EXPERTS).astype(jnp.int32)
    rank_idx = jnp.sum(per_src * (jnp.cumsum(per_src, axis=1) - 1), axis=2).reshape(n_tok, TOP_K)
    src_dev = jnp.arange(n_tok) // TOK_DEV
    limit_cnt = jnp.sum(jnp.where(chosen, counts[src_dev][:, None, :], 0), axis=-1)
    keep_mask = rank_idx < limit_cnt
    slot_idx = jnp.where(keep_mask, src_dev[:, None] * CAPACITY + rank_idx, EP_SIZE * CAPACITY)
    updates = jnp.broadcast_to(normed_2[:, None, :], (n_tok, TOP_K, D_MODEL))
    buffer = jnp.zeros((EXPERTS, EP_SIZE * CAPACITY, D_MODEL), normed_2.dtype).at[sel_ids, slot_idx].add(updates, mode='drop')
    expert_out = lax.map(expert_one, (buffer, w_1, w_3, w_2))
    picked = expert_out[sel_ids, jnp.minimum(slot_idx, EP_SIZE * CAPACITY - 1)]
    weight = jnp.where(keep_mask, gate_w, 0.0)
    y_out = hid_f32 + jnp.sum(weight[:, :, None] * picked.astype(jnp.float32), axis=1)
    return y_out.astype(jnp.bfloat16).reshape(x_seq.shape)


def reference(x_a, x_b, g_b, ids_a, ids_b, count_a, count_b, gain_1, gain_2, w_q, w_k, w_v, w_o, w_r, w_1, w_3, w_2):
    def stage_tick(stage_args):
        x_fwd, x_bwd, g_bwd, ids_fwd, ids_bwd, cnt_fwd, cnt_bwd = stage_args[:7]
        weights = stage_args[7:]
        y_fwd = layer_forward(x_fwd, ids_fwd, cnt_fwd, *weights)

        def layer_bwd(x_in, *params):
            return layer_forward(x_in, ids_bwd, cnt_bwd, *params)
        _, pullback = jax.vjp(layer_bwd, x_bwd, *weights)
        grad_list = pullback(g_bwd)
        return (y_fwd, grad_list[0]) + tuple(grad_part.astype(jnp.float32) for grad_part in grad_list[1:])
    stage_outs = lax.map(stage_tick, (x_a, x_b, g_b, ids_a, ids_b, count_a, count_b, gain_1, gain_2, w_q, w_k, w_v, w_o, w_r, w_1, w_3, w_2))
    return (jnp.roll(stage_outs[0], 1, axis=0), jnp.roll(stage_outs[1], -1, axis=0), stage_outs[2], stage_outs[3], stage_outs[4], stage_outs[5], stage_outs[6], stage_outs[7], stage_outs[8], stage_outs[9], stage_outs[10], stage_outs[11])
```

```python
import functools

import jax
import jax.numpy as jnp
from jax import lax
from jax.experimental import pallas as pl
from jax.experimental.pallas import tpu as pltpu
from jax.sharding import PartitionSpec as P

NORM_EPS = 1e-6
MASK_VALUE = -1e30
F32 = jnp.float32
BF16 = jnp.bfloat16
MESH = pl.DeviceIdType.MESH
VMEM = pltpu.VMEM
FFN_TILE = 256
LANES = 128


def dot_nn(lhs, rhs):
    return lax.dot_general(lhs, rhs, (((1,), (0,)), ((), ())), preferred_element_type=F32)


def dot_nt(lhs, rhs):
    return lax.dot_general(lhs, rhs, (((1,), (1,)), ((), ())), preferred_element_type=F32)


def dot_tn(lhs, rhs):
    return lax.dot_general(lhs, rhs, (((0,), (0,)), ((), ())), preferred_element_type=F32)


def ep_peers():
    me = lax.axis_index('ep')
    partner = me + 1 - 2 * lax.rem(me, 2)
    across = lax.rem(me + 2, 4)
    diag = lax.rem(partner + 2, 4)
    return me, partner, across, diag


def greet(peers):
    barrier = pltpu.get_barrier_semaphore()
    for peer in peers:
        pl.semaphore_signal(barrier, inc=1, device_id=peer, device_id_type=MESH)
    pl.semaphore_wait(barrier, len(peers))


def push(src, dst, sems, idx, peer):
    return pltpu.make_async_remote_copy(src_ref=src, dst_ref=dst, send_sem=sems[0].at[idx], recv_sem=sems[1].at[idx],
                                        device_id=peer, device_id_type=MESH)


def stack_heads(wide, heads, head_dim):
    return jnp.concatenate([wide[:, h * head_dim:(h + 1) * head_dim] for h in range(heads)], axis=0)


def unstack_heads(tall, heads, seq_len):
    return jnp.concatenate([tall[h * seq_len:(h + 1) * seq_len] for h in range(heads)], axis=1)


def rms_inv(x_f32):
    return lax.rsqrt(jnp.mean(x_f32 * x_f32, axis=-1, keepdims=True) + NORM_EPS)


def attention_rows(x_bf, gain, wq, wk, wv, wo, n_seq, heads):
    seq_len, head_dim = x_bf.shape[0] // n_seq, wk.shape[1]
    x_f32 = x_bf.astype(F32)
    normed = (x_f32 * rms_inv(x_f32) * gain).astype(BF16)
    query = dot_nn(normed, wq).astype(BF16)
    key = dot_nn(normed, wk).astype(BF16)
    value = dot_nn(normed, wv).astype(BF16)
    row = lax.rem(lax.broadcasted_iota(jnp.int32, (heads * seq_len, seq_len), 0), seq_len)
    col = lax.broadcasted_iota(jnp.int32, (heads * seq_len, seq_len), 1)
    causal = row >= col
    outs, probs_all = [], []
    for s in range(n_seq):
        rows = slice(s * seq_len, (s + 1) * seq_len)
        scores = dot_nt(stack_heads(query[rows], heads, head_dim), key[rows]) * head_dim ** -0.5
        scores = jnp.where(causal, scores, MASK_VALUE)
        expd = jnp.exp(scores - jnp.max(scores, axis=-1, keepdims=True))
        probs = expd / jnp.sum(expd, axis=-1, keepdims=True)
        probs_all.append(probs)
        outs.append(unstack_heads(dot_nn(probs.astype(BF16), value[rows]).astype(BF16), heads, seq_len))
    attn = jnp.concatenate(outs, axis=0)
    hidden = (x_f32 + dot_nn(attn, wo)).astype(BF16)
    return hidden, (normed, query, key, value, probs_all, attn)


def route_rows(hidden, gain, wr, cols, counts, base, n_seq):
    seq_len = hidden.shape[0] // n_seq
    h_f32 = hidden.astype(F32)
    normed = (h_f32 * rms_inv(h_f32) * gain).astype(BF16)
    logits = dot_nn(normed, wr)
    lane = lax.broadcasted_iota(jnp.int32, (seq_len, LANES), 1).astype(F32)
    lower = (lax.broadcasted_iota(jnp.int32, (seq_len, seq_len), 0)
             > lax.broadcasted_iota(jnp.int32, (seq_len, seq_len), 1)).astype(F32).astype(BF16)
    weights, masks, routes = [], [], []
    for s in range(n_seq):
        id0, id1 = cols[s][base], cols[s][base + 1]
        hot0, hot1 = (lane == id0).astype(F32), (lane == id1).astype(F32)
        rank = dot_nn(lower, (hot0 + hot1).astype(BF16))
        rank1 = rank + (id0 == id1).astype(F32)
        kept0 = hot0 * (rank < counts[s]).astype(F32)
        kept1 = hot1 * (rank1 < counts[s]).astype(F32)
        part = logits[s * seq_len:(s + 1) * seq_len]
        sel0 = jnp.sum(jnp.where(hot0 > 0, part, 0.0), axis=-1, keepdims=True)
        sel1 = jnp.sum(jnp.where(hot1 > 0, part, 0.0), axis=-1, keepdims=True)
        top = jnp.maximum(sel0, sel1)
        exp0, exp1 = jnp.exp(sel0 - top), jnp.exp(sel1 - top)
        gate0, gate1 = exp0 / (exp0 + exp1), exp1 / (exp0 + exp1)
        weights.append(kept0 * gate0 + kept1 * gate1)
        masks.append(jnp.maximum(kept0, kept1))
        keep0 = jnp.sum(kept0, axis=-1, keepdims=True)
        keep1 = jnp.sum(kept1, axis=-1, keepdims=True)
        route = jnp.zeros((seq_len, LANES), F32)
        for i, item in enumerate((id0, id1, gate0, gate1, keep0, keep1)):
            route = jnp.where(lane == i, item, route)
        routes.append(route)
    return normed, jnp.concatenate(weights, 0), jnp.concatenate(masks, 0), jnp.concatenate(routes, 0)


def head_kernel(n_ep, heads, pk_ref, xa_ref, xb_ref, gb_ref, gain1_ref, gain2_ref, wq_ref, wk_ref, wv_ref, wo_ref, wr_ref,
                xb_all, gb_all, n2a_ref, n2b_ref, wta_ref, ma_ref, wtb_ref, mb_ref, rtb_ref, ha_ref, hb_ref,
                n1_ref, q_ref, k_ref, v_ref, p_ref, o_ref,
                xa_all, pk_all, wq_s, wr_s, send_sem, recv_sem):
    me, partner, across, diag = ep_peers()
    seq_len = xa_ref.shape[0]
    sems = (send_sem, recv_sem)
    greet(({'ep': partner}, {'ep': across}))
    own, landing = (pk_ref, xb_ref, xa_ref, gb_ref), (pk_all, xb_all, xa_all, gb_all)
    near, far, relay = [], [], []
    for i in range(4):
        far.append(push(own[i], landing[i].at[me], sems, 3 * i, {'ep': across}))
        far[i].start()
        near.append(push(own[i], landing[i].at[me], sems, 3 * i + 1, {'ep': partner}))
        near[i].start()
        relay.append(push(landing[i].at[across], landing[i].at[across], sems, 3 * i + 2, {'ep': partner}))
        landing[i][me] = own[i][...]

    def arrive(i):
        far[i].wait_recv()
        relay[i].start()
        near[i].wait_recv()
        relay[i].wait_recv()

    for h in range(heads):
        wq_s[:, h * LANES:(h + 1) * LANES] = wq_ref[h]
    wr_s[...] = jnp.zeros_like(wr_s)
    wr_s[0:wr_ref.shape[0], :] = wr_ref[...]
    wr = wr_s[...].T
    gain1, gain2 = gain1_ref[...].astype(F32), gain2_ref[...].astype(F32)

    arrive(0)
    packed = pk_all[...].astype(F32)
    flat = jnp.concatenate([packed[s] for s in range(n_ep)] + [jnp.zeros((LANES - 8 * n_ep, LANES), F32)], axis=0).T
    cols = [[flat[:, 8 * s + r:8 * s + r + 1] for r in range(4)] for s in range(n_ep)]
    counts_a = [packed[s, 4:5, :] for s in range(n_ep)]
    counts_b = [packed[s, 5:6, :] for s in range(n_ep)]

    def rows_of(ref):
        return jnp.concatenate([ref[s] for s in range(n_ep)], axis=0)

    arrive(1)
    hidden, (normed, query, key, value, probs, attn) = attention_rows(
        rows_of(xb_all), gain1, wq_s[...], wk_ref[...], wv_ref[...], wo_ref[...], n_ep, heads)
    n1_ref[...], q_ref[...], k_ref[...], v_ref[...], o_ref[...] = normed, query, key, value, attn
    for s in range(n_ep):
        p_ref[s] = probs[s]
    hb_ref[...] = hidden
    n2b_ref[...], wtb_ref[...], mb_ref[...], rtb_ref[...] = route_rows(hidden, gain2, wr, cols, counts_b, 2, n_ep)

    arrive(2)
    hidden, _ = attention_rows(rows_of(xa_all), gain1, wq_s[...], wk_ref[...], wv_ref[...], wo_ref[...], n_ep, heads)
    ha_ref[...] = hidden
    n2a_ref[...], wta_ref[...], ma_ref[...], _ = route_rows(hidden, gain2, wr, cols, counts_a, 0, n_ep)

    arrive(3)
    for i in range(4):
        far[i].wait_send()
        near[i].wait_send()
        relay[i].wait_send()


def moe_kernel(e_local, n2a_ref, n2b_ref, g_ref, wta_ref, ma_ref, wtb_ref, mb_ref, w1_ref, w3_ref, w2_ref,
               ra_ref, rb_ref, dw1_ref, dw3_ref, dw2_ref, xm, xbt, dexp, acc, dacc, col):
    expert, tile = pl.program_id(0), pl.program_id(1)
    n_tok, d_model = n2a_ref.shape
    here = lax.axis_index('ep') * e_local + expert

    @pl.when(tile == 0)
    def _():
        lane = lax.broadcasted_iota(jnp.int32, (n_tok, LANES), 1)
        mine = lane == here

        def column(ref):
            return jnp.sum(jnp.where(mine, ref[...], 0.0), axis=-1, keepdims=True)
        wt_a, m_a, wt_b, m_b = column(wta_ref), column(ma_ref), column(wtb_ref), column(mb_ref)
        for i, item in enumerate((wt_a, m_a, m_b)):
            col[i] = jnp.broadcast_to(item, (n_tok, LANES))
        xm[0:n_tok, :] = jnp.where(m_a > 0, n2a_ref[...].astype(F32), 0.0).astype(BF16)
        x_b = jnp.where(m_b > 0, n2b_ref[...].astype(F32), 0.0)
        xm[n_tok:, :] = x_b.astype(BF16)
        xbt[...] = x_b.T.astype(BF16)
        dexp[...] = jnp.where(m_b > 0, wt_b * g_ref[...].astype(F32), 0.0).astype(BF16)
        acc[...] = jnp.zeros_like(acc)
        dacc[...] = jnp.zeros_like(dacc)

    @pl.when((tile == 0) & (expert == 0))
    def _():
        ra_ref[...] = jnp.zeros_like(ra_ref)
        rb_ref[...] = jnp.zeros_like(rb_ref)

    w1, w3, w2 = w1_ref[0], w3_ref[0], w2_ref[0]
    x_all = xm[...]
    gate_pre, up_pre = dot_nn(x_all, w1), dot_nn(x_all, w3)
    sig = jax.nn.sigmoid(gate_pre)
    act = (gate_pre * sig * up_pre).astype(BF16)
    acc[...] += dot_nn(act, w2)
    gate_b, up_b, sig_b = gate_pre[n_tok:], up_pre[n_tok:], sig[n_tok:]
    d_exp = dexp[...]
    d_act = dot_nt(d_exp, w2).astype(BF16).astype(F32)
    d_up = (d_act * gate_b * sig_b).astype(BF16)
    d_gate = (d_act * up_b * sig_b * (1.0 + gate_b * (1.0 - sig_b))).astype(BF16)
    x_t = xbt[...]
    dw1_ref[0] = dot_nn(x_t, d_gate)
    dw3_ref[0] = dot_nn(x_t, d_up)
    dw2_ref[0] = dot_tn(act[n_tok:], d_exp)
    dacc[...] += dot_nt(d_gate, w1) + dot_nt(d_up, w3)

    @pl.when(tile == pl.num_programs(1) - 1)
    def _():
        out_a = acc[0:n_tok, :].astype(BF16).astype(F32)
        ra_ref[...] += jnp.where(col[1][:, 0:1] > 0, col[0][:, 0:1] * out_a, 0.0)
        out_b = acc[n_tok:, :].astype(BF16).astype(F32)
        in_b = col[2][:, 0:1] > 0
        rb_ref[:, 0:d_model] += jnp.where(in_b, dacc[...].astype(BF16).astype(F32), 0.0)
        pick = jnp.sum(jnp.where(in_b, out_b * g_ref[...].astype(F32), 0.0), axis=-1, keepdims=True)
        lane = lax.broadcasted_iota(jnp.int32, (n_tok, LANES), 1)
        rb_ref[:, d_model:] += jnp.where(lane == here, pick, 0.0)


def tail_kernel(n_ep, n_pp, heads, ra_ref, rb_ref, ha_ref, hb_ref, n2b_ref, gb_ref, rtb_ref, x_ref, n1_ref, q_ref, k_ref, v_ref,
                p_ref, o_ref, gain1_ref, gain2_ref, wq_ref, wk_ref, wv_ref, wo_ref, wr_ref,
                y_ref, dx_ref, dwq_ref, dwk_ref, dwv_ref, dwo_ref, dg1_ref, dg2_ref, dwr_ref,
                near_b, swap_b, sum_b, far_b, near_a, swap_a, sum_a, far_a, dh_all, small, small_1, small_2, small_3,
                y_own, dx_all, wq_s, wr_s, send_sem, recv_sem):
    me, partner, across, diag = ep_peers()
    stage = lax.axis_index('pp')
    later, earlier = lax.rem(stage + 1, n_pp), lax.rem(stage + n_pp - 1, n_pp)
    seq_len, d_model = y_ref.shape
    sems = (send_sem, recv_sem)
    near, over = {'ep': partner}, {'ep': across}
    greet((near, over, {'pp': later}, {'pp': earlier}))
    swap_b_c = push(rb_ref.at[diag], swap_b, sems, 0, near)
    near_b_c = push(rb_ref.at[partner], near_b, sems, 1, near)
    swap_a_c = push(ra_ref.at[diag], swap_a, sems, 2, near)
    near_a_c = push(ra_ref.at[partner], near_a, sems, 3, near)
    far_b_c = push(sum_b, far_b, sems, 4, over)
    far_a_c = push(sum_a, far_a, sems, 5, over)
    swap_b_c.start()
    near_b_c.start()
    swap_a_c.start()
    near_a_c.start()
    for h in range(heads):
        wq_s[:, h * LANES:(h + 1) * LANES] = wq_ref[h]
    wr_s[...] = jnp.zeros_like(wr_s)
    wr_s[0:wr_ref.shape[0], :] = wr_ref[...]
    swap_b_c.wait_recv()
    sum_b[...] = rb_ref[across] + swap_b[...]
    far_b_c.start()
    swap_a_c.wait_recv()
    sum_a[...] = ra_ref[across] + swap_a[...]

    gain1, gain2 = gain1_ref[...].astype(F32), gain2_ref[...].astype(F32)
    mine = pl.ds(pl.multiple_of(me * seq_len, seq_len), seq_len)
    route = rtb_ref[mine, :]
    id0, id1, gate0, gate1, keep0, keep1 = [route[:, i:i + 1] for i in range(6)]
    lane = lax.broadcasted_iota(jnp.int32, (seq_len, LANES), 1).astype(F32)
    hot0, hot1 = (lane == id0).astype(F32), (lane == id1).astype(F32)
    h_f32 = hb_ref[mine, :].astype(F32)
    inv = rms_inv(h_f32)
    h_hat = h_f32 * inv
    near_b_c.wait_recv()
    far_b_c.wait_recv()
    total = rb_ref[me] + near_b[...] + far_b[...]
    dots = total[:, d_model:]
    d_gate0 = jnp.where(keep0 > 0, jnp.sum(hot0 * dots, axis=-1, keepdims=True), 0.0)
    d_gate1 = jnp.where(keep1 > 0, jnp.sum(hot1 * dots, axis=-1, keepdims=True), 0.0)
    mean_gate = gate0 * d_gate0 + gate1 * d_gate1
    d_logits = (hot0 * (gate0 * (d_gate0 - mean_gate)) + hot1 * (gate1 * (d_gate1 - mean_gate))).astype(BF16)
    d_normed = total[:, :d_model] + dot_nn(d_logits, wr_s[...])
    d_hat = d_normed * gain2
    d_in = inv * (d_hat - h_hat * jnp.mean(d_hat * h_hat, axis=-1, keepdims=True))
    dh_all[me] = (d_in + gb_ref[me].astype(F32)).astype(BF16)
    dh_far = push(dh_all.at[me], dh_all.at[me], sems, 6, over)
    dh_near = push(dh_all.at[me], dh_all.at[me], sems, 7, near)
    dh_relay = push(dh_all.at[across], dh_all.at[across], sems, 8, near)
    dh_far.start()
    dh_near.start()
    small[0:8, :] = dot_tn(d_logits, n2b_ref[mine, :])[0:8, :]
    small[8:16, :] = jnp.broadcast_to(jnp.sum(d_normed * h_hat, axis=0, keepdims=True), (8, d_model))
    small_near = push(small, small_1, sems, 9, near)
    small_near.start()
    small_near.wait_recv()
    small_2[...] = small[...] + small_1[...]
    small_far = push(small_2, small_3, sems, 10, over)
    small_far.start()
    far_a_c.start()
    dh_far.wait_recv()
    dh_relay.start()
    dh_near.wait_recv()
    dh_relay.wait_recv()

    head_dim = wk_ref.shape[1]
    d_hid = jnp.concatenate([dh_all[s] for s in range(n_ep)], axis=0)
    d_attn = dot_nt(d_hid, wo_ref[...]).astype(BF16)
    d_q, d_k, d_v = [], [], []
    for s in range(n_ep):
        rows = slice(s * seq_len, (s + 1) * seq_len)
        d_out = stack_heads(d_attn[rows], heads, head_dim)
        probs = p_ref[s]
        d_probs = dot_nt(d_out, v_ref[rows, :])
        d_v.append(dot_tn(probs.astype(BF16), d_out).astype(BF16))
        d_scores = (probs * (d_probs - jnp.sum(probs * d_probs, axis=-1, keepdims=True)) * head_dim ** -0.5).astype(BF16)
        d_q.append(unstack_heads(dot_nn(d_scores, k_ref[rows, :]).astype(BF16), heads, seq_len))
        d_k.append(dot_tn(d_scores, stack_heads(q_ref[rows, :], heads, head_dim)).astype(BF16))
    d_q, d_k, d_v = [jnp.concatenate(part, axis=0) for part in (d_q, d_k, d_v)]
    d_norm1 = dot_nt(d_q, wq_s[...]) + dot_nt(d_k, wk_ref[...]) + dot_nt(d_v, wv_ref[...])
    x_f32 = jnp.concatenate([x_ref[s] for s in range(n_ep)], axis=0).astype(F32)
    inv1 = rms_inv(x_f32)
    x_hat = x_f32 * inv1
    d_hat1 = d_norm1 * gain1
    d_x = inv1 * (d_hat1 - x_hat * jnp.mean(d_hat1 * x_hat, axis=-1, keepdims=True)) + d_hid.astype(F32)
    dx_all[...] = d_x.astype(BF16)
    dx_c = push(dx_all.at[mine], dx_ref, sems, 11, {'pp': earlier})
    dx_c.start()
    dg1_ref[...] = jnp.sum(d_norm1 * x_hat, axis=0, keepdims=True)

    near_a_c.wait_recv()
    far_a_c.wait_recv()
    y_own[...] = (ha_ref[mine, :].astype(F32) + (ra_ref[me] + near_a[...] + far_a[...])).astype(BF16)
    y_c = push(y_own, y_ref, sems, 12, {'pp': later})
    y_c.start()
    normed = n1_ref[...]
    d_w_q = dot_tn(normed, d_q)
    for h in range(heads):
        dwq_ref[h] = d_w_q[:, h * LANES:(h + 1) * LANES]
    dwk_ref[...] = dot_tn(normed, d_k)
    dwv_ref[...] = dot_tn(normed, d_v)
    dwo_ref[...] = dot_tn(o_ref[...], d_hid)
    small_far.wait_recv()
    sums = small_2[...] + small_3[...]
    dwr_ref[...] = sums[0:8, :]
    dg2_ref[...] = sums[8:9, :]
    dx_c.wait_recv()
    y_c.wait_recv()
    for copy in (swap_b_c, near_b_c, swap_a_c, near_a_c, far_b_c, far_a_c, dh_far, dh_near, dh_relay, small_near, small_far,
                 dx_c, y_c):
        copy.wait_send()


def shape_of(shape, dtype):
    return jax.ShapeDtypeStruct(shape, dtype)


def solution(mesh):
    n_ep, n_pp = mesh.shape['ep'], mesh.shape['pp']
    whole = pl.BlockSpec(memory_space=VMEM)

    def device_tick(x_a, x_b, g_b, ids_a, ids_b, count_a, count_b, gain_1, gain_2, w_q, w_k, w_v, w_o, w_r, w_1, w_3, w_2):
        seq_len, d_model = x_a.shape[2], x_a.shape[3]
        heads, head_dim = w_q.shape[2], w_q.shape[3]
        n_exp, e_local, ffn = w_r.shape[2], w_1.shape[1], w_1.shape[3]
        n_tok = n_ep * seq_len
        width = heads * head_dim
        xa, xb, gb = x_a[0, 0], x_b[0, 0], g_b[0, 0]
        wq = jnp.transpose(w_q[0], (1, 0, 2))
        wk, wv, wo = w_k[0, :, 0], w_v[0, :, 0], w_o[0].reshape(width, d_model)
        wr = jnp.transpose(w_r[0])
        packed = jnp.concatenate([
            ids_a[0, 0].T, ids_b[0, 0].T, jnp.pad(count_a[0], ((0, 0), (0, LANES - n_exp))),
            jnp.pad(count_b[0], ((0, 0), (0, LANES - n_exp))), jnp.zeros((2, LANES), jnp.int32)], axis=0)
        tok, rows = (n_ep, seq_len, d_model), (n_tok, d_model)
        head_out = [shape_of(tok, BF16), shape_of(tok, BF16), shape_of(rows, BF16), shape_of(rows, BF16),
                    shape_of((n_tok, LANES), F32), shape_of((n_tok, LANES), F32), shape_of((n_tok, LANES), F32),
                    shape_of((n_tok, LANES), F32), shape_of((n_tok, LANES), F32), shape_of(rows, BF16), shape_of(rows, BF16),
                    shape_of(rows, BF16), shape_of((n_tok, width), BF16), shape_of((n_tok, head_dim), BF16),
                    shape_of((n_tok, head_dim), BF16), shape_of((n_ep, heads * seq_len, seq_len), F32),
                    shape_of((n_tok, width), BF16)]
        (xb_all, gb_all, n2a, n2b, wta, m_a, wtb, m_b, rtb, ha, hb, n1, q, k, v, probs, attn) = pl.pallas_call(
            functools.partial(head_kernel, n_ep, heads),
            out_shape=head_out,
            in_specs=[whole] * 11,
            out_specs=[whole] * len(head_out),
            scratch_shapes=[VMEM(tok, BF16), VMEM((n_ep, 8, LANES), jnp.int32), VMEM((d_model, width), BF16),
                            VMEM((LANES, d_model), BF16), pltpu.SemaphoreType.DMA((12,)), pltpu.SemaphoreType.DMA((12,))],
            compiler_params=pltpu.CompilerParams(collective_id=0, has_side_effects=True, vmem_limit_bytes=60 * 2 ** 20),
            name='head',
        )(packed, xa, xb, gb, gain_1, gain_2, wq, wk, wv, wo, wr)

        n_tile = ffn // FFN_TILE

        def const(*shape):
            return pl.BlockSpec(shape, lambda e, f: (0,) * len(shape))
        in_tile = pl.BlockSpec((1, d_model, FFN_TILE), lambda e, f: (e, 0, f))
        out_tile = pl.BlockSpec((1, FFN_TILE, d_model), lambda e, f: (e, f, 0))
        r_a, r_b, dw1, dw3, dw2 = pl.pallas_call(
            functools.partial(moe_kernel, e_local),
            grid=(e_local, n_tile),
            out_shape=[shape_of(rows, F32), shape_of((n_tok, d_model + LANES), F32), shape_of((e_local, d_model, ffn), F32),
                       shape_of((e_local, d_model, ffn), F32), shape_of((e_local, ffn, d_model), F32)],
            in_specs=[const(*rows)] * 3 + [const(n_tok, LANES)] * 4 + [in_tile, in_tile, out_tile],
            out_specs=[const(*rows), const(n_tok, d_model + LANES), in_tile, in_tile, out_tile],
            scratch_shapes=[VMEM((2 * n_tok, d_model), BF16), VMEM((d_model, n_tok), BF16), VMEM(rows, BF16),
                            VMEM((2 * n_tok, d_model), F32), VMEM(rows, F32), VMEM((3, n_tok, LANES), F32)],
            compiler_params=pltpu.CompilerParams(dimension_semantics=('arbitrary', 'arbitrary'),
                                                 vmem_limit_bytes=60 * 2 ** 20),
            name='moe',
        )(n2a, n2b, gb_all.reshape(rows), wta, m_a, wtb, m_b, w_1[0], w_3[0], w_2[0])

        small = (16, d_model)
        block, wide = (seq_len, d_model), (seq_len, d_model + LANES)
        y_next, dx_prev, dwq, dwk, dwv, dwo, dg1, dg2, dwr = pl.pallas_call(
            functools.partial(tail_kernel, n_ep, n_pp, heads),
            out_shape=[shape_of(block, BF16), shape_of(block, BF16), shape_of((heads, d_model, head_dim), F32),
                       shape_of((d_model, head_dim), F32), shape_of((d_model, head_dim), F32), shape_of((width, d_model), F32),
                       shape_of((1, d_model), F32), shape_of((1, d_model), F32), shape_of((n_exp, d_model), F32)],
            in_specs=[whole] * 21,
            out_specs=[whole] * 9,
            scratch_shapes=[VMEM(wide, F32)] * 4 + [VMEM(block, F32)] * 4 + [VMEM(tok, BF16)] + [VMEM(small, F32)] * 4
            + [VMEM(block, BF16), VMEM(rows, BF16), VMEM((d_model, width), BF16), VMEM((LANES, d_model), BF16),
               pltpu.SemaphoreType.DMA((13,)), pltpu.SemaphoreType.DMA((13,))],
            compiler_params=pltpu.CompilerParams(collective_id=1, has_side_effects=True, vmem_limit_bytes=60 * 2 ** 20),
            name='tail',
        )(r_a.reshape(tok), r_b.reshape((n_ep,) + wide), ha, hb, n2b, gb_all, rtb, xb_all, n1, q, k, v, probs, attn,
          gain_1, gain_2, wq, wk, wv, wo, wr)
        return (y_next[None, None], dx_prev[None, None], dg1, dg2, jnp.transpose(dwq, (1, 0, 2))[None], dwk[None, :, None],
                dwv[None, :, None], dwo.reshape(w_o.shape), jnp.transpose(dwr)[None], dw1[None], dw3[None], dw2[None])

    tok_spec = P(('dp', 'pp'), 'ep', None, None)
    cnt_spec = P(('dp', 'pp'), 'ep', None)
    gain_spec = P('pp', None)
    attn_spec = P('pp', None, None, None)
    router_spec = P('pp', None, None)
    expert_spec = P('pp', 'ep', None, None)
    gain_out = P(('dp', 'pp'), None)
    attn_out_spec = P(('dp', 'pp'), None, None, None)
    router_out = P(('dp', 'pp'), None, None)
    expert_out_spec = P(('dp', 'pp'), 'ep', None, None)
    in_specs = (tok_spec, tok_spec, tok_spec, tok_spec, tok_spec, cnt_spec, cnt_spec, gain_spec, gain_spec,
                attn_spec, attn_spec, attn_spec, attn_spec, router_spec, expert_spec, expert_spec, expert_spec)
    out_specs = (tok_spec, tok_spec, gain_out, gain_out, attn_out_spec, attn_out_spec, attn_out_spec, attn_out_spec,
                 router_out, expert_out_spec, expert_out_spec, expert_out_spec)
    return jax.shard_map(device_tick, mesh=mesh, in_specs=in_specs, out_specs=out_specs, check_vma=False)
```

```python
import functools

import jax
import jax.numpy as jnp
from jax import lax
from jax.experimental import pallas as pl
from jax.experimental.pallas import tpu as pltpu
from jax.sharding import PartitionSpec as P

NORM_EPS = 1e-6
MASK_VALUE = -1e30
F32 = jnp.float32
BF16 = jnp.bfloat16
MESH = pl.DeviceIdType.MESH
VMEM = pltpu.VMEM
FFN_TILE = 256
LANES = 128
HEAD_VMEM = 34 * 2 ** 20
MOE_VMEM = 44 * 2 ** 20
TAIL_VMEM = 30 * 2 ** 20
DENSE_VMEM = 24 * 2 ** 20


def dot_nn(lhs, rhs):
    return lax.dot_general(lhs, rhs, (((1,), (0,)), ((), ())), preferred_element_type=F32)


def dot_nt(lhs, rhs):
    return lax.dot_general(lhs, rhs, (((1,), (1,)), ((), ())), preferred_element_type=F32)


def dot_tn(lhs, rhs):
    return lax.dot_general(lhs, rhs, (((0,), (0,)), ((), ())), preferred_element_type=F32)


def ep_peers():
    me = lax.axis_index('ep')
    partner = me + 1 - 2 * lax.rem(me, 2)
    across = lax.rem(me + 2, 4)
    diag = lax.rem(partner + 2, 4)
    return me, partner, across, diag


def greet(peers):
    barrier = pltpu.get_barrier_semaphore()
    for peer in peers:
        pl.semaphore_signal(barrier, inc=1, device_id=peer, device_id_type=MESH)
    pl.semaphore_wait(barrier, len(peers))


def push(src, dst, sems, idx, peer):
    return pltpu.make_async_remote_copy(src_ref=src, dst_ref=dst, send_sem=sems[0].at[idx], recv_sem=sems[1].at[idx],
                                        device_id=peer, device_id_type=MESH)


def stack_heads(wide, heads, head_dim):
    return jnp.concatenate([wide[:, h * head_dim:(h + 1) * head_dim] for h in range(heads)], axis=0)


def unstack_heads(tall, heads, seq_len):
    return jnp.concatenate([tall[h * seq_len:(h + 1) * seq_len] for h in range(heads)], axis=1)


def rms_inv(x_f32):
    return lax.rsqrt(jnp.mean(x_f32 * x_f32, axis=-1, keepdims=True) + NORM_EPS)


def attention_rows(x_bf, gain, wq, wk, wv, wo, n_seq, heads):
    seq_len, head_dim = x_bf.shape[0] // n_seq, wk.shape[1]
    x_f32 = x_bf.astype(F32)
    normed = (x_f32 * rms_inv(x_f32) * gain).astype(BF16)
    query = dot_nn(normed, wq).astype(BF16)
    key = dot_nn(normed, wk).astype(BF16)
    value = dot_nn(normed, wv).astype(BF16)
    row = lax.rem(lax.broadcasted_iota(jnp.int32, (heads * seq_len, seq_len), 0), seq_len)
    col = lax.broadcasted_iota(jnp.int32, (heads * seq_len, seq_len), 1)
    causal = row >= col
    outs, probs_all = [], []
    for s in range(n_seq):
        rows = slice(s * seq_len, (s + 1) * seq_len)
        scores = dot_nt(stack_heads(query[rows], heads, head_dim), key[rows]) * head_dim ** -0.5
        scores = jnp.where(causal, scores, MASK_VALUE)
        expd = jnp.exp(scores - jnp.max(scores, axis=-1, keepdims=True))
        probs = expd / jnp.sum(expd, axis=-1, keepdims=True)
        probs_all.append(probs)
        outs.append(unstack_heads(dot_nn(probs.astype(BF16), value[rows]).astype(BF16), heads, seq_len))
    attn = jnp.concatenate(outs, axis=0)
    hidden = (x_f32 + dot_nn(attn, wo)).astype(BF16)
    return hidden, (normed, query, key, value, probs_all, attn)


def route_rows(hidden, gain, wr, cols, counts, base, n_seq):
    seq_len = hidden.shape[0] // n_seq
    h_f32 = hidden.astype(F32)
    normed = (h_f32 * rms_inv(h_f32) * gain).astype(BF16)
    logits = dot_nn(normed, wr)
    lane = lax.broadcasted_iota(jnp.int32, (seq_len, LANES), 1).astype(F32)
    lower = (lax.broadcasted_iota(jnp.int32, (seq_len, seq_len), 0)
             > lax.broadcasted_iota(jnp.int32, (seq_len, seq_len), 1)).astype(F32).astype(BF16)
    weights, masks, routes = [], [], []
    for s in range(n_seq):
        id0, id1 = cols[s][base], cols[s][base + 1]
        hot0, hot1 = (lane == id0).astype(F32), (lane == id1).astype(F32)
        rank = dot_nn(lower, (hot0 + hot1).astype(BF16))
        rank1 = rank + (id0 == id1).astype(F32)
        kept0 = hot0 * (rank < counts[s]).astype(F32)
        kept1 = hot1 * (rank1 < counts[s]).astype(F32)
        part = logits[s * seq_len:(s + 1) * seq_len]
        sel0 = jnp.sum(jnp.where(hot0 > 0, part, 0.0), axis=-1, keepdims=True)
        sel1 = jnp.sum(jnp.where(hot1 > 0, part, 0.0), axis=-1, keepdims=True)
        top = jnp.maximum(sel0, sel1)
        exp0, exp1 = jnp.exp(sel0 - top), jnp.exp(sel1 - top)
        gate0, gate1 = exp0 / (exp0 + exp1), exp1 / (exp0 + exp1)
        weights.append(kept0 * gate0 + kept1 * gate1)
        masks.append(jnp.maximum(kept0, kept1))
        keep0 = jnp.sum(kept0, axis=-1, keepdims=True)
        keep1 = jnp.sum(kept1, axis=-1, keepdims=True)
        route = jnp.zeros((seq_len, LANES), F32)
        for i, item in enumerate((id0, id1, gate0, gate1, keep0, keep1)):
            route = jnp.where(lane == i, item, route)
        routes.append(route)
    return normed, jnp.concatenate(weights, 0), jnp.concatenate(masks, 0), jnp.concatenate(routes, 0)


def head_kernel(n_ep, heads, ida_ref, idb_ref, cta_ref, ctb_ref, xa_ref, xb_ref, gb_ref, gain1_ref, gain2_ref, wq_ref, wk_ref, wv_ref, wo_ref, wr_ref,
                xb_all, gb_all, n2a_ref, n2b_ref, wta_ref, ma_ref, wtb_ref, mb_ref, rtb_ref, ha_ref, hb_ref,
                n1_ref, q_ref, k_ref, v_ref, p_ref, o_ref,
                xa_all, pk_ref, pk_all, wq_s, wr_s, send_sem, recv_sem):
    me, partner, across, diag = ep_peers()
    sems = (send_sem, recv_sem)
    pk_ref[...] = jnp.zeros_like(pk_ref)
    pk_ref[0:2, :] = ida_ref[...]
    pk_ref[2:4, :] = idb_ref[...]
    pk_ref[4:5, 0:cta_ref.shape[1]] = cta_ref[...]
    pk_ref[5:6, 0:ctb_ref.shape[1]] = ctb_ref[...]
    greet(({'ep': partner}, {'ep': across}))
    own, landing = (pk_ref, xb_ref, xa_ref, gb_ref), (pk_all, xb_all, xa_all, gb_all)
    near, far, relay = [], [], []
    for i in range(4):
        far.append(push(own[i], landing[i].at[me], sems, 3 * i, {'ep': across}))
        far[i].start()
        near.append(push(own[i], landing[i].at[me], sems, 3 * i + 1, {'ep': partner}))
        near[i].start()
        relay.append(push(landing[i].at[across], landing[i].at[across], sems, 3 * i + 2, {'ep': partner}))
        landing[i][me] = own[i][...]

    def arrive(i):
        far[i].wait_recv()
        relay[i].start()
        near[i].wait_recv()
        relay[i].wait_recv()

    for h in range(heads):
        wq_s[:, h * LANES:(h + 1) * LANES] = wq_ref[h]
    wr_s[...] = jnp.zeros_like(wr_s)
    wr_s[0:wr_ref.shape[0], :] = wr_ref[...]
    wr = wr_s[...].T
    gain1, gain2 = gain1_ref[...].astype(F32), gain2_ref[...].astype(F32)

    arrive(0)
    packed = pk_all[...].astype(F32)
    flat = jnp.concatenate([packed[s] for s in range(n_ep)] + [jnp.zeros((LANES - 8 * n_ep, LANES), F32)], axis=0).T
    cols = [[flat[:, 8 * s + r:8 * s + r + 1] for r in range(4)] for s in range(n_ep)]
    counts_a = [packed[s, 4:5, :] for s in range(n_ep)]
    counts_b = [packed[s, 5:6, :] for s in range(n_ep)]

    def rows_of(ref):
        return jnp.concatenate([ref[s] for s in range(n_ep)], axis=0)

    arrive(1)
    hidden, (normed, query, key, value, probs, attn) = attention_rows(
        rows_of(xb_all), gain1, wq_s[...], wk_ref[...], wv_ref[...], wo_ref[...], n_ep, heads)
    n1_ref[...], q_ref[...], k_ref[...], v_ref[...], o_ref[...] = normed, query, key, value, attn
    for s in range(n_ep):
        p_ref[s] = probs[s]
    hb_ref[...] = hidden
    n2b_ref[...], wtb_ref[...], mb_ref[...], rtb_ref[...] = route_rows(hidden, gain2, wr, cols, counts_b, 2, n_ep)

    arrive(2)
    hidden, _ = attention_rows(rows_of(xa_all), gain1, wq_s[...], wk_ref[...], wv_ref[...], wo_ref[...], n_ep, heads)
    ha_ref[...] = hidden
    n2a_ref[...], wta_ref[...], ma_ref[...], _ = route_rows(hidden, gain2, wr, cols, counts_a, 0, n_ep)

    arrive(3)
    for i in range(4):
        far[i].wait_send()
        near[i].wait_send()
        relay[i].wait_send()


def moe_kernel(e_local, n2a_ref, n2b_ref, g_ref, wta_ref, ma_ref, wtb_ref, mb_ref, w1_ref, w3_ref, w2_ref,
               ra_ref, rb_ref, dw1_ref, dw3_ref, dw2_ref, xm, xbt, dexp, acc, dacc, col):
    expert, tile = pl.program_id(0), pl.program_id(1)
    n_tok, d_model = n2a_ref.shape
    here = lax.axis_index('ep') * e_local + expert

    @pl.when(tile == 0)
    def _():
        lane = lax.broadcasted_iota(jnp.int32, (n_tok, LANES), 1)
        mine = lane == here

        def column(ref):
            return jnp.sum(jnp.where(mine, ref[...], 0.0), axis=-1, keepdims=True)
        wt_a, m_a, wt_b, m_b = column(wta_ref), column(ma_ref), column(wtb_ref), column(mb_ref)
        for i, item in enumerate((wt_a, m_a, m_b)):
            col[i] = jnp.broadcast_to(item, (n_tok, LANES))
        xm[0:n_tok, :] = jnp.where(m_a > 0, n2a_ref[...].astype(F32), 0.0).astype(BF16)
        x_b = jnp.where(m_b > 0, n2b_ref[...].astype(F32), 0.0)
        xm[n_tok:, :] = x_b.astype(BF16)
        xbt[...] = x_b.T.astype(BF16)
        dexp[...] = jnp.where(m_b > 0, wt_b * g_ref[...].astype(F32), 0.0).astype(BF16)
        acc[...] = jnp.zeros_like(acc)
        dacc[...] = jnp.zeros_like(dacc)

    @pl.when((tile == 0) & (expert == 0))
    def _():
        ra_ref[...] = jnp.zeros_like(ra_ref)
        rb_ref[...] = jnp.zeros_like(rb_ref)

    w1, w3, w2 = w1_ref[0], w3_ref[0], w2_ref[0]
    x_all = xm[...]
    gate_pre, up_pre = dot_nn(x_all, w1), dot_nn(x_all, w3)
    sig = jax.nn.sigmoid(gate_pre)
    act = (gate_pre * sig * up_pre).astype(BF16)
    acc[...] += dot_nn(act, w2)
    gate_b, up_b, sig_b = gate_pre[n_tok:], up_pre[n_tok:], sig[n_tok:]
    d_exp = dexp[...]
    d_act = dot_nt(d_exp, w2).astype(BF16).astype(F32)
    d_up = (d_act * gate_b * sig_b).astype(BF16)
    d_gate = (d_act * up_b * sig_b * (1.0 + gate_b * (1.0 - sig_b))).astype(BF16)
    x_t = xbt[...]
    dw1_ref[0] = dot_nn(x_t, d_gate)
    dw3_ref[0] = dot_nn(x_t, d_up)
    dw2_ref[0] = dot_tn(act[n_tok:], d_exp)
    dacc[...] += dot_nt(d_gate, w1) + dot_nt(d_up, w3)

    @pl.when(tile == pl.num_programs(1) - 1)
    def _():
        out_a = acc[0:n_tok, :].astype(BF16).astype(F32)
        ra_ref[...] += jnp.where(col[1][:, 0:1] > 0, col[0][:, 0:1] * out_a, 0.0)
        out_b = acc[n_tok:, :].astype(BF16).astype(F32)
        in_b = col[2][:, 0:1] > 0
        rb_ref[:, 0:d_model] += jnp.where(in_b, dacc[...].astype(BF16).astype(F32), 0.0)
        pick = jnp.sum(jnp.where(in_b, out_b * g_ref[...].astype(F32), 0.0), axis=-1, keepdims=True)
        lane = lax.broadcasted_iota(jnp.int32, (n_tok, LANES), 1)
        rb_ref[:, d_model:] += jnp.where(lane == here, pick, 0.0)


def tail_kernel(n_ep, n_pp, heads, ra_ref, rb_ref, ha_ref, hb_ref, n2b_ref, gb_ref, rtb_ref, x_ref, q_ref, k_ref, v_ref,
                p_ref, gain1_ref, gain2_ref, wq_ref, wk_ref, wv_ref, wo_ref, wr_ref,
                y_ref, dx_ref, dq_ref, dk_ref, dv_ref, dh_all, dg1_ref, sums_ref,
                near_b, swap_b, sum_b, far_b, near_a, swap_a, sum_a, far_a, small, small_1, small_2, small_3,
                y_own, dx_own, wq_s, wr_s, send_sem, recv_sem):
    me, partner, across, diag = ep_peers()
    stage = lax.axis_index('pp')
    later, earlier = lax.rem(stage + 1, n_pp), lax.rem(stage + n_pp - 1, n_pp)
    seq_len, d_model = y_ref.shape
    sems = (send_sem, recv_sem)
    near, over = {'ep': partner}, {'ep': across}
    greet((near, over, {'pp': later}, {'pp': earlier}))
    swap_b_c = push(rb_ref.at[diag], swap_b, sems, 0, near)
    near_b_c = push(rb_ref.at[partner], near_b, sems, 1, near)
    swap_a_c = push(ra_ref.at[diag], swap_a, sems, 2, near)
    near_a_c = push(ra_ref.at[partner], near_a, sems, 3, near)
    far_b_c = push(sum_b, far_b, sems, 4, over)
    far_a_c = push(sum_a, far_a, sems, 5, over)
    swap_b_c.start()
    near_b_c.start()
    swap_a_c.start()
    near_a_c.start()
    for h in range(heads):
        wq_s[:, h * LANES:(h + 1) * LANES] = wq_ref[h]
    wr_s[...] = jnp.zeros_like(wr_s)
    wr_s[0:wr_ref.shape[0], :] = wr_ref[...]
    swap_b_c.wait_recv()
    sum_b[...] = rb_ref[across] + swap_b[...]
    far_b_c.start()
    swap_a_c.wait_recv()
    sum_a[...] = ra_ref[across] + swap_a[...]

    gain1, gain2 = gain1_ref[...].astype(F32), gain2_ref[...].astype(F32)
    mine = pl.ds(pl.multiple_of(me * seq_len, seq_len), seq_len)
    route = rtb_ref[mine, :]
    id0, id1, gate0, gate1, keep0, keep1 = [route[:, i:i + 1] for i in range(6)]
    lane = lax.broadcasted_iota(jnp.int32, (seq_len, LANES), 1).astype(F32)
    hot0, hot1 = (lane == id0).astype(F32), (lane == id1).astype(F32)
    h_f32 = hb_ref[mine, :].astype(F32)
    inv = rms_inv(h_f32)
    h_hat = h_f32 * inv
    near_b_c.wait_recv()
    far_b_c.wait_recv()
    total = rb_ref[me] + near_b[...] + far_b[...]
    dots = total[:, d_model:]
    d_gate0 = jnp.where(keep0 > 0, jnp.sum(hot0 * dots, axis=-1, keepdims=True), 0.0)
    d_gate1 = jnp.where(keep1 > 0, jnp.sum(hot1 * dots, axis=-1, keepdims=True), 0.0)
    mean_gate = gate0 * d_gate0 + gate1 * d_gate1
    d_logits = (hot0 * (gate0 * (d_gate0 - mean_gate)) + hot1 * (gate1 * (d_gate1 - mean_gate))).astype(BF16)
    d_normed = total[:, :d_model] + dot_nn(d_logits, wr_s[...])
    d_hat = d_normed * gain2
    d_in = inv * (d_hat - h_hat * jnp.mean(d_hat * h_hat, axis=-1, keepdims=True))
    dh_all[me] = (d_in + gb_ref[me].astype(F32)).astype(BF16)
    dh_far = push(dh_all.at[me], dh_all.at[me], sems, 6, over)
    dh_near = push(dh_all.at[me], dh_all.at[me], sems, 7, near)
    dh_relay = push(dh_all.at[across], dh_all.at[across], sems, 8, near)
    dh_far.start()
    dh_near.start()
    small[0:8, :] = dot_tn(d_logits, n2b_ref[mine, :])[0:8, :]
    small[8:16, :] = jnp.broadcast_to(jnp.sum(d_normed * h_hat, axis=0, keepdims=True), (8, d_model))
    small_near = push(small, small_1, sems, 9, near)
    small_near.start()

    head_dim = wk_ref.shape[1]

    def attention_back(s):
        rows = pl.ds(pl.multiple_of(s * seq_len, seq_len), seq_len)
        d_hid = dh_all[s]
        d_out = stack_heads(dot_nt(d_hid, wo_ref[...]).astype(BF16), heads, head_dim)
        probs = p_ref[s]
        d_probs = dot_nt(d_out, v_ref[rows, :])
        d_v = dot_tn(probs.astype(BF16), d_out).astype(BF16)
        d_scores = (probs * (d_probs - jnp.sum(probs * d_probs, axis=-1, keepdims=True)) * head_dim ** -0.5).astype(BF16)
        d_q = unstack_heads(dot_nn(d_scores, k_ref[rows, :]).astype(BF16), heads, seq_len)
        d_k = dot_tn(d_scores, stack_heads(q_ref[rows, :], heads, head_dim)).astype(BF16)
        dq_ref[rows, :], dk_ref[rows, :], dv_ref[rows, :] = d_q, d_k, d_v
        d_norm1 = dot_nt(d_q, wq_s[...]) + dot_nt(d_k, wk_ref[...]) + dot_nt(d_v, wv_ref[...])
        x_f32 = x_ref[s].astype(F32)
        inv1 = rms_inv(x_f32)
        x_hat = x_f32 * inv1
        dg1_ref[s] = jnp.broadcast_to(jnp.sum(d_norm1 * x_hat, axis=0, keepdims=True), (8, d_model))
        return d_hid, d_norm1, inv1, x_hat

    d_hid, d_norm1, inv1, x_hat = attention_back(me)
    d_hat1 = d_norm1 * gain1
    d_x = inv1 * (d_hat1 - x_hat * jnp.mean(d_hat1 * x_hat, axis=-1, keepdims=True)) + d_hid.astype(F32)
    dx_own[...] = d_x.astype(BF16)
    dx_c = push(dx_own, dx_ref, sems, 11, {'pp': earlier})
    dx_c.start()
    small_near.wait_recv()
    small_2[...] = small[...] + small_1[...]
    small_far = push(small_2, small_3, sems, 10, over)
    small_far.start()
    far_a_c.start()
    dh_near.wait_recv()
    attention_back(partner)
    dh_far.wait_recv()
    dh_relay.start()
    attention_back(across)
    dh_relay.wait_recv()
    attention_back(diag)

    near_a_c.wait_recv()
    far_a_c.wait_recv()
    y_own[...] = (ha_ref[mine, :].astype(F32) + (ra_ref[me] + near_a[...] + far_a[...])).astype(BF16)
    y_c = push(y_own, y_ref, sems, 12, {'pp': later})
    y_c.start()
    small_far.wait_recv()
    sums_ref[...] = small_2[...] + small_3[...]
    dx_c.wait_recv()
    y_c.wait_recv()
    for copy in (swap_b_c, near_b_c, swap_a_c, near_a_c, far_b_c, far_a_c, dh_far, dh_near, dh_relay, small_near, small_far,
                 dx_c, y_c):
        copy.wait_send()


def dense_kernel(n1_ref, o_ref, dq_ref, dk_ref, dv_ref, dh_ref, dg1_in, sums_in, y_in, dx_in,
                 dwq_ref, dwk_ref, dwv_ref, dwo_ref, dg1_ref, dg2_ref, dwr_ref, y_ref, dx_ref, n1t):
    step = pl.program_id(0)

    @pl.when(step == 0)
    def _():
        n1t[...] = n1_ref[...].astype(F32).T.astype(BF16)
        dwk_ref[...] = dot_nn(n1t[...], dk_ref[...])
        dwv_ref[...] = dot_nn(n1t[...], dv_ref[...])
        dg1_ref[...] = sum(dg1_in[s] for s in range(dg1_in.shape[0]))[0:1]
        dwr_ref[...] = sums_in[0:8, :]
        dg2_ref[...] = sums_in[8:9, :]
        y_ref[...] = y_in[...]
        dx_ref[...] = dx_in[...]

    pair = dot_nn(n1t[...], dq_ref[...])
    for i in range(dwq_ref.shape[0]):
        dwq_ref[i] = pair[:, i * LANES:(i + 1) * LANES]
    dwo_ref[...] = dot_tn(o_ref[...], dh_ref[...])


def shape_of(shape, dtype):
    return jax.ShapeDtypeStruct(shape, dtype)


def solution(mesh):
    n_ep, n_pp = mesh.shape['ep'], mesh.shape['pp']
    whole = pl.BlockSpec(memory_space=VMEM)

    def device_tick(x_a, x_b, g_b, ids_a, ids_b, count_a, count_b, gain_1, gain_2, w_q, w_k, w_v, w_o, w_r, w_1, w_3, w_2):
        seq_len, d_model = x_a.shape[2], x_a.shape[3]
        heads, head_dim = w_q.shape[2], w_q.shape[3]
        n_exp, e_local, ffn = w_r.shape[2], w_1.shape[1], w_1.shape[3]
        n_tok = n_ep * seq_len
        width = heads * head_dim
        xa, xb, gb = x_a[0, 0], x_b[0, 0], g_b[0, 0]
        wq = jnp.transpose(w_q[0], (1, 0, 2))
        wk, wv, wo = w_k[0, :, 0], w_v[0, :, 0], w_o[0].reshape(width, d_model)
        wr = jnp.transpose(w_r[0])
        tok, rows = (n_ep, seq_len, d_model), (n_tok, d_model)
        head_out = [shape_of(tok, BF16), shape_of(tok, BF16), shape_of(rows, BF16), shape_of(rows, BF16),
                    shape_of((n_tok, LANES), F32), shape_of((n_tok, LANES), F32), shape_of((n_tok, LANES), F32),
                    shape_of((n_tok, LANES), F32), shape_of((n_tok, LANES), F32), shape_of(rows, BF16), shape_of(rows, BF16),
                    shape_of(rows, BF16), shape_of((n_tok, width), BF16), shape_of((n_tok, head_dim), BF16),
                    shape_of((n_tok, head_dim), BF16), shape_of((n_ep, heads * seq_len, seq_len), F32),
                    shape_of((n_tok, width), BF16)]
        (xb_all, gb_all, n2a, n2b, wta, m_a, wtb, m_b, rtb, ha, hb, n1, q, k, v, probs, attn) = pl.pallas_call(
            functools.partial(head_kernel, n_ep, heads),
            out_shape=head_out,
            in_specs=[whole] * 14,
            out_specs=[whole] * len(head_out),
            scratch_shapes=[VMEM(tok, BF16), VMEM((8, LANES), jnp.int32), VMEM((n_ep, 8, LANES), jnp.int32), VMEM((d_model, width), BF16),
                            VMEM((LANES, d_model), BF16), pltpu.SemaphoreType.DMA((12,)), pltpu.SemaphoreType.DMA((12,))],
            compiler_params=pltpu.CompilerParams(collective_id=0, has_side_effects=True, vmem_limit_bytes=HEAD_VMEM),
            name='head',
        )(ids_a[0, 0].T, ids_b[0, 0].T, count_a[0], count_b[0], xa, xb, gb, gain_1, gain_2, wq, wk, wv, wo, wr)

        n_tile = ffn // FFN_TILE

        def const(*shape):
            return pl.BlockSpec(shape, lambda e, f: (0,) * len(shape))
        in_tile = pl.BlockSpec((1, d_model, FFN_TILE), lambda e, f: (e, 0, f))
        out_tile = pl.BlockSpec((1, FFN_TILE, d_model), lambda e, f: (e, f, 0))
        r_a, r_b, dw1, dw3, dw2 = pl.pallas_call(
            functools.partial(moe_kernel, e_local),
            grid=(e_local, n_tile),
            out_shape=[shape_of(rows, F32), shape_of((n_tok, d_model + LANES), F32), shape_of((e_local, d_model, ffn), F32),
                       shape_of((e_local, d_model, ffn), F32), shape_of((e_local, ffn, d_model), F32)],
            in_specs=[const(*rows)] * 3 + [const(n_tok, LANES)] * 4 + [in_tile, in_tile, out_tile],
            out_specs=[const(*rows), const(n_tok, d_model + LANES), in_tile, in_tile, out_tile],
            scratch_shapes=[VMEM((2 * n_tok, d_model), BF16), VMEM((d_model, n_tok), BF16), VMEM(rows, BF16),
                            VMEM((2 * n_tok, d_model), F32), VMEM(rows, F32), VMEM((3, n_tok, LANES), F32)],
            compiler_params=pltpu.CompilerParams(dimension_semantics=('arbitrary', 'arbitrary'),
                                                 vmem_limit_bytes=MOE_VMEM),
            name='moe',
        )(n2a, n2b, gb_all.reshape(rows), wta, m_a, wtb, m_b, w_1[0], w_3[0], w_2[0])

        small = (16, d_model)
        block, wide = (seq_len, d_model), (seq_len, d_model + LANES)
        y_in, dx_in, dq, dk, dv, dh, dg1_in, sums = pl.pallas_call(
            functools.partial(tail_kernel, n_ep, n_pp, heads),
            out_shape=[shape_of(block, BF16), shape_of(block, BF16), shape_of((n_tok, width), BF16),
                       shape_of((n_tok, head_dim), BF16), shape_of((n_tok, head_dim), BF16), shape_of(tok, BF16),
                       shape_of((n_ep, 8, d_model), F32), shape_of(small, F32)],
            in_specs=[whole] * 19,
            out_specs=[whole] * 8,
            scratch_shapes=[VMEM(wide, F32)] * 4 + [VMEM(block, F32)] * 4 + [VMEM(small, F32)] * 4
            + [VMEM(block, BF16), VMEM(block, BF16), VMEM((d_model, width), BF16), VMEM((LANES, d_model), BF16),
               pltpu.SemaphoreType.DMA((13,)), pltpu.SemaphoreType.DMA((13,))],
            compiler_params=pltpu.CompilerParams(collective_id=1, has_side_effects=True, vmem_limit_bytes=TAIL_VMEM),
            name='tail',
        )(r_a.reshape(tok), r_b.reshape((n_ep,) + wide), ha, hb, n2b, gb_all, rtb, xb_all, q, k, v, probs,
          gain_1, gain_2, wq, wk, wv, wo, wr)

        pair = 2
        steps = heads // pair

        def held(*shape):
            return pl.BlockSpec(shape, lambda i: (0,) * len(shape))
        cols = pl.BlockSpec((n_tok, pair * head_dim), lambda i: (0, i))
        dwq, dwk, dwv, dwo, dg1, dg2, dwr, y_next, dx_prev = pl.pallas_call(
            dense_kernel,
            grid=(steps,),
            out_shape=[shape_of((heads, d_model, head_dim), F32), shape_of((d_model, head_dim), F32),
                       shape_of((d_model, head_dim), F32), shape_of((width, d_model), F32), shape_of((1, d_model), F32),
                       shape_of((1, d_model), F32), shape_of((n_exp, d_model), F32), shape_of(block, BF16), shape_of(block, BF16)],
            in_specs=[held(*rows), cols, cols, held(n_tok, head_dim), held(n_tok, head_dim), held(*rows),
                      held(n_ep, 8, d_model), held(*small), held(*block), held(*block)],
            out_specs=[pl.BlockSpec((pair, d_model, head_dim), lambda i: (i, 0, 0)), held(d_model, head_dim),
                       held(d_model, head_dim), pl.BlockSpec((pair * head_dim, d_model), lambda i: (i, 0)),
                       held(1, d_model), held(1, d_model), held(n_exp, d_model), held(*block), held(*block)],
            scratch_shapes=[VMEM((d_model, n_tok), BF16)],
            compiler_params=pltpu.CompilerParams(dimension_semantics=('arbitrary',), vmem_limit_bytes=DENSE_VMEM),
            name='dense',
        )(n1, attn, dq, dk, dv, dh.reshape(rows), dg1_in, sums, y_in, dx_in)
        return (y_next[None, None], dx_prev[None, None], dg1, dg2, jnp.transpose(dwq, (1, 0, 2))[None], dwk[None, :, None],
                dwv[None, :, None], dwo.reshape(w_o.shape), jnp.transpose(dwr)[None], dw1[None], dw3[None], dw2[None])

    tok_spec = P(('dp', 'pp'), 'ep', None, None)
    cnt_spec = P(('dp', 'pp'), 'ep', None)
    gain_spec = P('pp', None)
    attn_spec = P('pp', None, None, None)
    router_spec = P('pp', None, None)
    expert_spec = P('pp', 'ep', None, None)
    gain_out = P(('dp', 'pp'), None)
    attn_out_spec = P(('dp', 'pp'), None, None, None)
    router_out = P(('dp', 'pp'), None, None)
    expert_out_spec = P(('dp', 'pp'), 'ep', None, None)
    in_specs = (tok_spec, tok_spec, tok_spec, tok_spec, tok_spec, cnt_spec, cnt_spec, gain_spec, gain_spec,
                attn_spec, attn_spec, attn_spec, attn_spec, router_spec, expert_spec, expert_spec, expert_spec)
    out_specs = (tok_spec, tok_spec, gain_out, gain_out, attn_out_spec, attn_out_spec, attn_out_spec, attn_out_spec,
                 router_out, expert_out_spec, expert_out_spec, expert_out_spec)
    return jax.shard_map(device_tick, mesh=mesh, in_specs=in_specs, out_specs=out_specs, check_vma=False)
```

```python
import functools

import jax
import jax.numpy as jnp
from jax import lax
from jax.experimental import pallas as pl
from jax.experimental.pallas import tpu as pltpu
from jax.sharding import PartitionSpec as P

NORM_EPS = 1e-6
MASK_VALUE = -1e30
F32 = jnp.float32
BF16 = jnp.bfloat16
MESH = pl.DeviceIdType.MESH
VMEM = pltpu.VMEM
FFN_TILE = 256
LANES = 128
ROW_BLOCK = 128
HEAD_VMEM = 34 * 2 ** 20
MOE_VMEM = 44 * 2 ** 20
TAIL_VMEM = 30 * 2 ** 20
DENSE_VMEM = 24 * 2 ** 20


def dot_nn(lhs, rhs):
    return lax.dot_general(lhs, rhs, (((1,), (0,)), ((), ())), preferred_element_type=F32)


def dot_nt(lhs, rhs):
    return lax.dot_general(lhs, rhs, (((1,), (1,)), ((), ())), preferred_element_type=F32)


def dot_tn(lhs, rhs):
    return lax.dot_general(lhs, rhs, (((0,), (0,)), ((), ())), preferred_element_type=F32)


def ep_peers():
    me = lax.axis_index('ep')
    partner = me + 1 - 2 * lax.rem(me, 2)
    across = lax.rem(me + 2, 4)
    diag = lax.rem(partner + 2, 4)
    return me, partner, across, diag


def greet(peers):
    barrier = pltpu.get_barrier_semaphore()
    for peer in peers:
        pl.semaphore_signal(barrier, inc=1, device_id=peer, device_id_type=MESH)
    pl.semaphore_wait(barrier, len(peers))


def push(src, dst, sems, idx, peer):
    return pltpu.make_async_remote_copy(src_ref=src, dst_ref=dst, send_sem=sems[0].at[idx], recv_sem=sems[1].at[idx],
                                        device_id=peer, device_id_type=MESH)


def stack_heads(wide, heads, head_dim):
    return jnp.concatenate([wide[:, h * head_dim:(h + 1) * head_dim] for h in range(heads)], axis=0)


def unstack_heads(tall, heads, seq_len):
    return jnp.concatenate([tall[h * seq_len:(h + 1) * seq_len] for h in range(heads)], axis=1)


def rms_inv(x_f32):
    return lax.rsqrt(jnp.mean(x_f32 * x_f32, axis=-1, keepdims=True) + NORM_EPS)


def attention_rows(x_bf, gain, wq, wk, wv, wo, n_seq, heads):
    seq_len, head_dim = x_bf.shape[0] // n_seq, wk.shape[1]
    x_f32 = x_bf.astype(F32)
    normed = (x_f32 * rms_inv(x_f32) * gain).astype(BF16)
    query = dot_nn(normed, wq).astype(BF16)
    key = dot_nn(normed, wk).astype(BF16)
    value = dot_nn(normed, wv).astype(BF16)
    row = lax.rem(lax.broadcasted_iota(jnp.int32, (heads * seq_len, seq_len), 0), seq_len)
    col = lax.broadcasted_iota(jnp.int32, (heads * seq_len, seq_len), 1)
    causal = row >= col
    outs, probs_all = [], []
    for s in range(n_seq):
        rows = slice(s * seq_len, (s + 1) * seq_len)
        scores = dot_nt(stack_heads(query[rows], heads, head_dim), key[rows]) * head_dim ** -0.5
        scores = jnp.where(causal, scores, MASK_VALUE)
        expd = jnp.exp(scores - jnp.max(scores, axis=-1, keepdims=True))
        probs = expd / jnp.sum(expd, axis=-1, keepdims=True)
        probs_all.append(probs)
        outs.append(unstack_heads(dot_nn(probs.astype(BF16), value[rows]).astype(BF16), heads, seq_len))
    attn = jnp.concatenate(outs, axis=0)
    hidden = (x_f32 + dot_nn(attn, wo)).astype(BF16)
    return hidden, (normed, query, key, value, probs_all, attn)


def route_rows(hidden, gain, wr, cols, counts, base, n_seq):
    seq_len = hidden.shape[0] // n_seq
    h_f32 = hidden.astype(F32)
    normed = (h_f32 * rms_inv(h_f32) * gain).astype(BF16)
    logits = dot_nn(normed, wr)
    lane = lax.broadcasted_iota(jnp.int32, (seq_len, LANES), 1).astype(F32)
    lower = (lax.broadcasted_iota(jnp.int32, (seq_len, seq_len), 0)
             > lax.broadcasted_iota(jnp.int32, (seq_len, seq_len), 1)).astype(F32).astype(BF16)
    weights, masks, routes = [], [], []
    for s in range(n_seq):
        id0, id1 = cols[s][base], cols[s][base + 1]
        hot0, hot1 = (lane == id0).astype(F32), (lane == id1).astype(F32)
        rank = dot_nn(lower, (hot0 + hot1).astype(BF16))
        rank1 = rank + (id0 == id1).astype(F32)
        kept0 = hot0 * (rank < counts[s]).astype(F32)
        kept1 = hot1 * (rank1 < counts[s]).astype(F32)
        part = logits[s * seq_len:(s + 1) * seq_len]
        sel0 = jnp.sum(jnp.where(hot0 > 0, part, 0.0), axis=-1, keepdims=True)
        sel1 = jnp.sum(jnp.where(hot1 > 0, part, 0.0), axis=-1, keepdims=True)
        top = jnp.maximum(sel0, sel1)
        exp0, exp1 = jnp.exp(sel0 - top), jnp.exp(sel1 - top)
        gate0, gate1 = exp0 / (exp0 + exp1), exp1 / (exp0 + exp1)
        weights.append(kept0 * gate0 + kept1 * gate1)
        masks.append(jnp.maximum(kept0, kept1))
        keep0 = jnp.sum(kept0, axis=-1, keepdims=True)
        keep1 = jnp.sum(kept1, axis=-1, keepdims=True)
        route = jnp.zeros((seq_len, LANES), F32)
        for i, item in enumerate((id0, id1, gate0, gate1, keep0, keep1)):
            route = jnp.where(lane == i, item, route)
        routes.append(route)
    return normed, jnp.concatenate(weights, 0), jnp.concatenate(masks, 0), jnp.concatenate(routes, 0)


def head_kernel(n_ep, heads, ida_hbm, idb_hbm, cta_hbm, ctb_hbm, xa_hbm, xb_hbm, gb_hbm, gain1_hbm, gain2_hbm, wq_hbm, wk_hbm,
                wv_hbm, wo_hbm, wr_hbm,
                xb_all, gb_all, n2a_ref, n2b_ref, wta_ref, ma_ref, wtb_ref, mb_ref, rtb_ref, ha_ref, hb_ref,
                n1_ref, q_ref, k_ref, v_ref, p_ref, o_ref,
                xa_all, pk_ref, pk_all, ida_ref, idb_ref, cta_ref, ctb_ref, gain1_ref, gain2_ref, wq_s, wk_ref, wv_ref, wo_ref,
                wr_ref, wr_s, load_sem, send_sem, recv_sem):
    me, partner, across, diag = ep_peers()
    sems = (send_sem, recv_sem)
    moves = [(ida_hbm, ida_ref), (idb_hbm, idb_ref), (cta_hbm, cta_ref), (ctb_hbm, ctb_ref), (xb_hbm, xb_all.at[me]),
             (xa_hbm, xa_all.at[me]), (gb_hbm, gb_all.at[me]), (gain1_hbm, gain1_ref), (gain2_hbm, gain2_ref)]
    moves += [(wq_hbm.at[h], wq_s.at[:, pl.ds(h * LANES, LANES)]) for h in range(heads)]
    moves += [(wk_hbm, wk_ref), (wv_hbm, wv_ref), (wo_hbm, wo_ref), (wr_hbm, wr_ref)]
    loads = [pltpu.make_async_copy(src, dst, load_sem.at[i]) for i, (src, dst) in enumerate(moves)]
    for load in loads:
        load.start()
    greet(({'ep': partner}, {'ep': across}))
    landing = (pk_all, xb_all, xa_all, gb_all)
    far, near, relay = [], [], []
    for i in range(4):
        own = pk_ref if i == 0 else landing[i].at[me]
        far.append(push(own, landing[i].at[me], sems, 3 * i, {'ep': across}))
        near.append(push(own, landing[i].at[me], sems, 3 * i + 1, {'ep': partner}))
        relay.append(push(landing[i].at[across], landing[i].at[across], sems, 3 * i + 2, {'ep': partner}))

    def leave(i):
        far[i].start()
        near[i].start()

    def arrive(i):
        far[i].wait_recv()
        relay[i].start()
        near[i].wait_recv()
        relay[i].wait_recv()

    for load in loads[0:4]:
        load.wait()
    pk_ref[...] = jnp.zeros_like(pk_ref)
    pk_ref[0:2, :] = ida_ref[...]
    pk_ref[2:4, :] = idb_ref[...]
    pk_ref[4:5, 0:cta_ref.shape[1]] = cta_ref[...]
    pk_ref[5:6, 0:ctb_ref.shape[1]] = ctb_ref[...]
    pk_all[me] = pk_ref[...]
    loads[4].wait()
    leave(1)
    leave(0)
    loads[5].wait()
    leave(2)
    loads[6].wait()
    leave(3)
    for load in loads[7:]:
        load.wait()
    wr_s[...] = jnp.zeros_like(wr_s)
    wr_s[0:wr_ref.shape[0], :] = wr_ref[...]
    wr = wr_s[...].T
    gain1, gain2 = gain1_ref[...].astype(F32), gain2_ref[...].astype(F32)

    arrive(0)
    packed = pk_all[...].astype(F32)
    flat = jnp.concatenate([packed[s] for s in range(n_ep)] + [jnp.zeros((LANES - 8 * n_ep, LANES), F32)], axis=0).T
    cols = [[flat[:, 8 * s + r:8 * s + r + 1] for r in range(4)] for s in range(n_ep)]
    counts_a = [packed[s, 4:5, :] for s in range(n_ep)]
    counts_b = [packed[s, 5:6, :] for s in range(n_ep)]

    def rows_of(ref):
        return jnp.concatenate([ref[s] for s in range(n_ep)], axis=0)

    arrive(1)
    hidden, (normed, query, key, value, probs, attn) = attention_rows(
        rows_of(xb_all), gain1, wq_s[...], wk_ref[...], wv_ref[...], wo_ref[...], n_ep, heads)
    n1_ref[...], q_ref[...], k_ref[...], v_ref[...], o_ref[...] = normed, query, key, value, attn
    for s in range(n_ep):
        p_ref[s] = probs[s]
    hb_ref[...] = hidden
    n2b_ref[...], wtb_ref[...], mb_ref[...], rtb_ref[...] = route_rows(hidden, gain2, wr, cols, counts_b, 2, n_ep)

    arrive(2)
    hidden, _ = attention_rows(rows_of(xa_all), gain1, wq_s[...], wk_ref[...], wv_ref[...], wo_ref[...], n_ep, heads)
    ha_ref[...] = hidden
    n2a_ref[...], wta_ref[...], ma_ref[...], _ = route_rows(hidden, gain2, wr, cols, counts_a, 0, n_ep)

    arrive(3)
    for i in range(4):
        far[i].wait_send()
        near[i].wait_send()
        relay[i].wait_send()


def moe_kernel(e_local, n2a_ref, n2b_ref, g_ref, wta_ref, ma_ref, wtb_ref, mb_ref, w1_ref, w3_ref, w2_ref,
               ra_ref, rb_ref, dw1_ref, dw3_ref, dw2_ref, x_a, x_b, xbt, dexp, acc_a, acc_b, dacc, put_a, put_b, wcol, blocks):
    expert, tile = pl.program_id(0), pl.program_id(1)
    n_tok, d_model = n2a_ref.shape
    here = lax.axis_index('ep') * e_local + expert
    n_block = n_tok // ROW_BLOCK

    def by_rows(which, work):
        for count in range(1, n_block + 1):
            pl.when(blocks[which] == count)(functools.partial(work, count * ROW_BLOCK))

    @pl.when(tile == 0)
    def _():
        mine = lax.broadcasted_iota(jnp.int32, (n_tok, LANES), 1) == here
        mine_t = lax.broadcasted_iota(jnp.int32, (LANES, n_tok), 0) == here
        lower = (lax.broadcasted_iota(jnp.int32, (n_tok, n_tok), 0)
                 > lax.broadcasted_iota(jnp.int32, (n_tok, n_tok), 1)).astype(F32).astype(BF16)
        slot_col = lax.broadcasted_iota(jnp.int32, (n_tok, n_tok), 1).astype(F32)
        slot_row = lax.broadcasted_iota(jnp.int32, (n_tok, n_tok), 0).astype(F32)

        def plan(which, mask_ref, put):
            mask = mask_ref[...]
            place = jnp.where(mask > 0, dot_nn(lower, mask.astype(BF16)), -1.0)
            place_col = jnp.sum(jnp.where(mine, place, 0.0), axis=-1, keepdims=True)
            place_row = jnp.sum(jnp.where(mine_t, place.T, 0.0), axis=0, keepdims=True)
            put[...] = (slot_col == place_col).astype(F32).astype(BF16)
            total = jnp.sum(jnp.where(mine, mask, 0.0)).astype(jnp.int32)
            blocks[which] = jnp.maximum((total + ROW_BLOCK - 1) // ROW_BLOCK, 1)
            return (slot_row == place_row).astype(F32).astype(BF16)

        take_a, take_b = plan(0, ma_ref, put_a), plan(1, mb_ref, put_b)
        wcol[...] = jnp.broadcast_to(jnp.sum(jnp.where(mine, wta_ref[...], 0.0), axis=-1, keepdims=True), (n_tok, LANES))
        wt_b = jnp.sum(jnp.where(mine, wtb_ref[...], 0.0), axis=-1, keepdims=True)
        scaled = (wt_b * g_ref[...].astype(F32)).astype(BF16)

        def fetch_a(rows):
            x_a[0:rows, :] = dot_nn(take_a[0:rows], n2a_ref[...]).astype(BF16)
            acc_a[0:rows, :] = jnp.zeros((rows, d_model), F32)

        def fetch_b(rows):
            fetched = dot_nn(take_b[0:rows], n2b_ref[...])
            x_b[0:rows, :] = fetched.astype(BF16)
            xbt[:, 0:rows] = fetched.T.astype(BF16)
            dexp[0:rows, :] = dot_nn(take_b[0:rows], scaled).astype(BF16)
            acc_b[0:rows, :] = jnp.zeros((rows, d_model), F32)
            dacc[0:rows, :] = jnp.zeros((rows, d_model), F32)

        by_rows(0, fetch_a)
        by_rows(1, fetch_b)

    @pl.when((tile == 0) & (expert == 0))
    def _():
        ra_ref[...] = jnp.zeros_like(ra_ref)
        rb_ref[...] = jnp.zeros_like(rb_ref)

    def forward(x, rows):
        gate_pre, up_pre = dot_nn(x[0:rows, :], w1_ref[0]), dot_nn(x[0:rows, :], w3_ref[0])
        sig = jax.nn.sigmoid(gate_pre)
        return gate_pre, up_pre, sig, (gate_pre * sig * up_pre).astype(BF16)

    def run_a(rows):
        act = forward(x_a, rows)[3]
        acc_a[0:rows, :] += dot_nn(act, w2_ref[0])

    def run_b(rows):
        gate_pre, up_pre, sig, act = forward(x_b, rows)
        acc_b[0:rows, :] += dot_nn(act, w2_ref[0])
        d_exp = dexp[0:rows, :]
        d_act = dot_nt(d_exp, w2_ref[0]).astype(BF16).astype(F32)
        d_up = (d_act * gate_pre * sig).astype(BF16)
        d_gate = (d_act * up_pre * sig * (1.0 + gate_pre * (1.0 - sig))).astype(BF16)
        dw1_ref[0] = dot_nn(xbt[:, 0:rows], d_gate)
        dw3_ref[0] = dot_nn(xbt[:, 0:rows], d_up)
        dw2_ref[0] = dot_tn(act, d_exp)
        dacc[0:rows, :] += dot_nt(d_gate, w1_ref[0]) + dot_nt(d_up, w3_ref[0])

    by_rows(0, run_a)
    by_rows(1, run_b)

    def return_a(rows):
        ra_ref[...] += wcol[:, 0:1] * dot_nn(put_a[:, 0:rows], acc_a[0:rows, :].astype(BF16))

    def return_b(rows):
        put = put_b[:, 0:rows]
        rb_ref[:, 0:d_model] += dot_nn(put, dacc[0:rows, :].astype(BF16))
        out_b = dot_nn(put, acc_b[0:rows, :].astype(BF16))
        pick = jnp.sum(out_b * g_ref[...].astype(F32), axis=-1, keepdims=True)
        lane = lax.broadcasted_iota(jnp.int32, (n_tok, LANES), 1)
        rb_ref[:, d_model:] += jnp.where(lane == here, pick, 0.0)

    @pl.when(tile == pl.num_programs(1) - 1)
    def _():
        by_rows(0, return_a)
        by_rows(1, return_b)


def tail_kernel(n_ep, n_pp, heads, ra_ref, rb_ref, ha_ref, hb_ref, n2b_ref, gb_ref, rtb_ref, x_ref, q_ref, k_ref, v_ref,
                p_ref, gain1_ref, gain2_ref, wq_ref, wk_ref, wv_ref, wo_ref, wr_ref,
                y_ref, dx_ref, dq_ref, dk_ref, dv_ref, dh_all, dg1_ref, sums_ref,
                near_b, swap_b, sum_b, far_b, near_a, swap_a, sum_a, far_a, small, small_1, small_2, small_3,
                y_own, dx_own, wq_s, wr_s, send_sem, recv_sem):
    me, partner, across, diag = ep_peers()
    stage = lax.axis_index('pp')
    later, earlier = lax.rem(stage + 1, n_pp), lax.rem(stage + n_pp - 1, n_pp)
    seq_len, d_model = y_ref.shape
    sems = (send_sem, recv_sem)
    near, over = {'ep': partner}, {'ep': across}
    greet((near, over, {'pp': later}, {'pp': earlier}))
    swap_b_c = push(rb_ref.at[diag], swap_b, sems, 0, near)
    near_b_c = push(rb_ref.at[partner], near_b, sems, 1, near)
    swap_a_c = push(ra_ref.at[diag], swap_a, sems, 2, near)
    near_a_c = push(ra_ref.at[partner], near_a, sems, 3, near)
    far_b_c = push(sum_b, far_b, sems, 4, over)
    far_a_c = push(sum_a, far_a, sems, 5, over)
    swap_b_c.start()
    near_b_c.start()
    swap_a_c.start()
    near_a_c.start()
    for h in range(heads):
        wq_s[:, h * LANES:(h + 1) * LANES] = wq_ref[h]
    wr_s[...] = jnp.zeros_like(wr_s)
    wr_s[0:wr_ref.shape[0], :] = wr_ref[...]
    swap_b_c.wait_recv()
    sum_b[...] = rb_ref[across] + swap_b[...]
    far_b_c.start()
    swap_a_c.wait_recv()
    sum_a[...] = ra_ref[across] + swap_a[...]

    gain1, gain2 = gain1_ref[...].astype(F32), gain2_ref[...].astype(F32)
    mine = pl.ds(pl.multiple_of(me * seq_len, seq_len), seq_len)
    route = rtb_ref[mine, :]
    id0, id1, gate0, gate1, keep0, keep1 = [route[:, i:i + 1] for i in range(6)]
    lane = lax.broadcasted_iota(jnp.int32, (seq_len, LANES), 1).astype(F32)
    hot0, hot1 = (lane == id0).astype(F32), (lane == id1).astype(F32)
    h_f32 = hb_ref[mine, :].astype(F32)
    inv = rms_inv(h_f32)
    h_hat = h_f32 * inv
    near_b_c.wait_recv()
    far_b_c.wait_recv()
    total = rb_ref[me] + near_b[...] + far_b[...]
    dots = total[:, d_model:]
    d_gate0 = jnp.where(keep0 > 0, jnp.sum(hot0 * dots, axis=-1, keepdims=True), 0.0)
    d_gate1 = jnp.where(keep1 > 0, jnp.sum(hot1 * dots, axis=-1, keepdims=True), 0.0)
    mean_gate = gate0 * d_gate0 + gate1 * d_gate1
    d_logits = (hot0 * (gate0 * (d_gate0 - mean_gate)) + hot1 * (gate1 * (d_gate1 - mean_gate))).astype(BF16)
    d_normed = total[:, :d_model] + dot_nn(d_logits, wr_s[...])
    d_hat = d_normed * gain2
    d_in = inv * (d_hat - h_hat * jnp.mean(d_hat * h_hat, axis=-1, keepdims=True))
    dh_all[me] = (d_in + gb_ref[me].astype(F32)).astype(BF16)
    dh_far = push(dh_all.at[me], dh_all.at[me], sems, 6, over)
    dh_near = push(dh_all.at[me], dh_all.at[me], sems, 7, near)
    dh_relay = push(dh_all.at[across], dh_all.at[across], sems, 8, near)
    dh_far.start()
    dh_near.start()
    small[0:8, :] = dot_tn(d_logits, n2b_ref[mine, :])[0:8, :]
    small[8:16, :] = jnp.broadcast_to(jnp.sum(d_normed * h_hat, axis=0, keepdims=True), (8, d_model))
    small_near = push(small, small_1, sems, 9, near)
    small_near.start()

    head_dim = wk_ref.shape[1]

    def attention_back(s):
        rows = pl.ds(pl.multiple_of(s * seq_len, seq_len), seq_len)
        d_hid = dh_all[s]
        d_out = stack_heads(dot_nt(d_hid, wo_ref[...]).astype(BF16), heads, head_dim)
        probs = p_ref[s]
        d_probs = dot_nt(d_out, v_ref[rows, :])
        d_v = dot_tn(probs.astype(BF16), d_out).astype(BF16)
        d_scores = (probs * (d_probs - jnp.sum(probs * d_probs, axis=-1, keepdims=True)) * head_dim ** -0.5).astype(BF16)
        d_q = unstack_heads(dot_nn(d_scores, k_ref[rows, :]).astype(BF16), heads, seq_len)
        d_k = dot_tn(d_scores, stack_heads(q_ref[rows, :], heads, head_dim)).astype(BF16)
        dq_ref[rows, :], dk_ref[rows, :], dv_ref[rows, :] = d_q, d_k, d_v
        d_norm1 = dot_nt(d_q, wq_s[...]) + dot_nt(d_k, wk_ref[...]) + dot_nt(d_v, wv_ref[...])
        x_f32 = x_ref[s].astype(F32)
        inv1 = rms_inv(x_f32)
        x_hat = x_f32 * inv1
        dg1_ref[s] = jnp.broadcast_to(jnp.sum(d_norm1 * x_hat, axis=0, keepdims=True), (8, d_model))
        return d_hid, d_norm1, inv1, x_hat

    d_hid, d_norm1, inv1, x_hat = attention_back(me)
    d_hat1 = d_norm1 * gain1
    d_x = inv1 * (d_hat1 - x_hat * jnp.mean(d_hat1 * x_hat, axis=-1, keepdims=True)) + d_hid.astype(F32)
    dx_own[...] = d_x.astype(BF16)
    dx_c = push(dx_own, dx_ref, sems, 11, {'pp': earlier})
    dx_c.start()
    small_near.wait_recv()
    small_2[...] = small[...] + small_1[...]
    small_far = push(small_2, small_3, sems, 10, over)
    small_far.start()
    far_a_c.start()
    dh_near.wait_recv()
    attention_back(partner)
    dh_far.wait_recv()
    dh_relay.start()
    attention_back(across)
    dh_relay.wait_recv()
    attention_back(diag)

    near_a_c.wait_recv()
    far_a_c.wait_recv()
    y_own[...] = (ha_ref[mine, :].astype(F32) + (ra_ref[me] + near_a[...] + far_a[...])).astype(BF16)
    y_c = push(y_own, y_ref, sems, 12, {'pp': later})
    y_c.start()
    small_far.wait_recv()
    sums_ref[...] = small_2[...] + small_3[...]
    dx_c.wait_recv()
    y_c.wait_recv()
    for copy in (swap_b_c, near_b_c, swap_a_c, near_a_c, far_b_c, far_a_c, dh_far, dh_near, dh_relay, small_near, small_far,
                 dx_c, y_c):
        copy.wait_send()


def dense_kernel(n1_ref, o_ref, dq_ref, dk_ref, dv_ref, dh_ref, dg1_in, sums_in, y_in, dx_in,
                 dwq_ref, dwk_ref, dwv_ref, dwo_ref, dg1_ref, dg2_ref, dwr_ref, y_ref, dx_ref, n1t):
    step = pl.program_id(0)

    @pl.when(step == 0)
    def _():
        n1t[...] = n1_ref[...].astype(F32).T.astype(BF16)
        dwk_ref[...] = dot_nn(n1t[...], dk_ref[...])
        dwv_ref[...] = dot_nn(n1t[...], dv_ref[...])
        dg1_ref[...] = sum(dg1_in[s] for s in range(dg1_in.shape[0]))[0:1]
        dwr_ref[...] = sums_in[0:8, :]
        dg2_ref[...] = sums_in[8:9, :]
        y_ref[...] = y_in[...]
        dx_ref[...] = dx_in[...]

    pair = dot_nn(n1t[...], dq_ref[...])
    for i in range(dwq_ref.shape[0]):
        dwq_ref[i] = pair[:, i * LANES:(i + 1) * LANES]
    dwo_ref[...] = dot_tn(o_ref[...], dh_ref[...])


def shape_of(shape, dtype):
    return jax.ShapeDtypeStruct(shape, dtype)


def solution(mesh):
    n_ep, n_pp = mesh.shape['ep'], mesh.shape['pp']
    whole = pl.BlockSpec(memory_space=VMEM)

    def device_tick(x_a, x_b, g_b, ids_a, ids_b, count_a, count_b, gain_1, gain_2, w_q, w_k, w_v, w_o, w_r, w_1, w_3, w_2):
        seq_len, d_model = x_a.shape[2], x_a.shape[3]
        heads, head_dim = w_q.shape[2], w_q.shape[3]
        n_exp, e_local, ffn = w_r.shape[2], w_1.shape[1], w_1.shape[3]
        n_tok = n_ep * seq_len
        width = heads * head_dim
        xa, xb, gb = x_a[0, 0], x_b[0, 0], g_b[0, 0]
        wq = jnp.transpose(w_q[0], (1, 0, 2))
        wk, wv, wo = w_k[0, :, 0], w_v[0, :, 0], w_o[0].reshape(width, d_model)
        wr = jnp.transpose(w_r[0])
        tok, rows = (n_ep, seq_len, d_model), (n_tok, d_model)
        head_out = [shape_of(tok, BF16), shape_of(tok, BF16), shape_of(rows, BF16), shape_of(rows, BF16),
                    shape_of((n_tok, LANES), F32), shape_of((n_tok, LANES), F32), shape_of((n_tok, LANES), F32),
                    shape_of((n_tok, LANES), F32), shape_of((n_tok, LANES), F32), shape_of(rows, BF16), shape_of(rows, BF16),
                    shape_of(rows, BF16), shape_of((n_tok, width), BF16), shape_of((n_tok, head_dim), BF16),
                    shape_of((n_tok, head_dim), BF16), shape_of((n_ep, heads * seq_len, seq_len), F32),
                    shape_of((n_tok, width), BF16)]
        (xb_all, gb_all, n2a, n2b, wta, m_a, wtb, m_b, rtb, ha, hb, n1, q, k, v, probs, attn) = pl.pallas_call(
            functools.partial(head_kernel, n_ep, heads),
            out_shape=head_out,
            in_specs=[pl.BlockSpec(memory_space=pltpu.HBM)] * 14,
            out_specs=[whole] * len(head_out),
            scratch_shapes=[VMEM(tok, BF16), VMEM((8, LANES), jnp.int32), VMEM((n_ep, 8, LANES), jnp.int32),
                            VMEM((2, seq_len), jnp.int32), VMEM((2, seq_len), jnp.int32), VMEM((1, n_exp), jnp.int32),
                            VMEM((1, n_exp), jnp.int32), VMEM((1, d_model), BF16), VMEM((1, d_model), BF16),
                            VMEM((d_model, width), BF16), VMEM((d_model, head_dim), BF16), VMEM((d_model, head_dim), BF16),
                            VMEM((width, d_model), BF16), VMEM((n_exp, d_model), BF16), VMEM((LANES, d_model), BF16),
                            pltpu.SemaphoreType.DMA((13 + heads,)), pltpu.SemaphoreType.DMA((12,)),
                            pltpu.SemaphoreType.DMA((12,))],
            compiler_params=pltpu.CompilerParams(collective_id=0, has_side_effects=True, vmem_limit_bytes=HEAD_VMEM),
            name='head',
        )(*[pltpu.with_memory_space_constraint(arg, pltpu.HBM) for arg in (
            ids_a[0, 0].T, ids_b[0, 0].T, count_a[0], count_b[0], xa, xb, gb, gain_1, gain_2, wq, wk, wv, wo, wr)])

        n_tile = ffn // FFN_TILE

        def const(*shape):
            return pl.BlockSpec(shape, lambda e, f: (0,) * len(shape))
        in_tile = pl.BlockSpec((1, d_model, FFN_TILE), lambda e, f: (e, 0, f))
        out_tile = pl.BlockSpec((1, FFN_TILE, d_model), lambda e, f: (e, f, 0))
        r_a, r_b, dw1, dw3, dw2 = pl.pallas_call(
            functools.partial(moe_kernel, e_local),
            grid=(e_local, n_tile),
            out_shape=[shape_of(rows, F32), shape_of((n_tok, d_model + LANES), F32), shape_of((e_local, d_model, ffn), F32),
                       shape_of((e_local, d_model, ffn), F32), shape_of((e_local, ffn, d_model), F32)],
            in_specs=[const(*rows)] * 3 + [const(n_tok, LANES)] * 4 + [in_tile, in_tile, out_tile],
            out_specs=[const(*rows), const(n_tok, d_model + LANES), in_tile, in_tile, out_tile],
            scratch_shapes=[VMEM(rows, BF16), VMEM(rows, BF16), VMEM((d_model, n_tok), BF16), VMEM(rows, BF16),
                            VMEM(rows, F32), VMEM(rows, F32), VMEM(rows, F32), VMEM((n_tok, n_tok), BF16),
                            VMEM((n_tok, n_tok), BF16), VMEM((n_tok, LANES), F32), pltpu.SMEM((2,), jnp.int32)],
            compiler_params=pltpu.CompilerParams(dimension_semantics=('arbitrary', 'arbitrary'),
                                                 vmem_limit_bytes=MOE_VMEM),
            name='moe',
        )(n2a, n2b, gb_all.reshape(rows), wta, m_a, wtb, m_b, w_1[0], w_3[0], w_2[0])

        small = (16, d_model)
        block, wide = (seq_len, d_model), (seq_len, d_model + LANES)
        y_in, dx_in, dq, dk, dv, dh, dg1_in, sums = pl.pallas_call(
            functools.partial(tail_kernel, n_ep, n_pp, heads),
            out_shape=[shape_of(block, BF16), shape_of(block, BF16), shape_of((n_tok, width), BF16),
                       shape_of((n_tok, head_dim), BF16), shape_of((n_tok, head_dim), BF16), shape_of(tok, BF16),
                       shape_of((n_ep, 8, d_model), F32), shape_of(small, F32)],
            in_specs=[whole] * 19,
            out_specs=[whole] * 8,
            scratch_shapes=[VMEM(wide, F32)] * 4 + [VMEM(block, F32)] * 4 + [VMEM(small, F32)] * 4
            + [VMEM(block, BF16), VMEM(block, BF16), VMEM((d_model, width), BF16), VMEM((LANES, d_model), BF16),
               pltpu.SemaphoreType.DMA((13,)), pltpu.SemaphoreType.DMA((13,))],
            compiler_params=pltpu.CompilerParams(collective_id=1, has_side_effects=True, vmem_limit_bytes=TAIL_VMEM),
            name='tail',
        )(r_a.reshape(tok), r_b.reshape((n_ep,) + wide), ha, hb, n2b, gb_all, rtb, xb_all, q, k, v, probs,
          gain_1, gain_2, wq, wk, wv, wo, wr)

        pair = 2
        steps = heads // pair

        def held(*shape):
            return pl.BlockSpec(shape, lambda i: (0,) * len(shape))
        cols = pl.BlockSpec((n_tok, pair * head_dim), lambda i: (0, i))
        dwq, dwk, dwv, dwo, dg1, dg2, dwr, y_next, dx_prev = pl.pallas_call(
            dense_kernel,
            grid=(steps,),
            out_shape=[shape_of((heads, d_model, head_dim), F32), shape_of((d_model, head_dim), F32),
                       shape_of((d_model, head_dim), F32), shape_of((width, d_model), F32), shape_of((1, d_model), F32),
                       shape_of((1, d_model), F32), shape_of((n_exp, d_model), F32), shape_of(block, BF16), shape_of(block, BF16)],
            in_specs=[held(*rows), cols, cols, held(n_tok, head_dim), held(n_tok, head_dim), held(*rows),
                      held(n_ep, 8, d_model), held(*small), held(*block), held(*block)],
            out_specs=[pl.BlockSpec((pair, d_model, head_dim), lambda i: (i, 0, 0)), held(d_model, head_dim),
                       held(d_model, head_dim), pl.BlockSpec((pair * head_dim, d_model), lambda i: (i, 0)),
                       held(1, d_model), held(1, d_model), held(n_exp, d_model), held(*block), held(*block)],
            scratch_shapes=[VMEM((d_model, n_tok), BF16)],
            compiler_params=pltpu.CompilerParams(dimension_semantics=('arbitrary',), vmem_limit_bytes=DENSE_VMEM),
            name='dense',
        )(n1, attn, dq, dk, dv, dh.reshape(rows), dg1_in, sums, y_in, dx_in)
        return (y_next[None, None], dx_prev[None, None], dg1, dg2, jnp.transpose(dwq, (1, 0, 2))[None], dwk[None, :, None],
                dwv[None, :, None], dwo.reshape(w_o.shape), jnp.transpose(dwr)[None], dw1[None], dw3[None], dw2[None])

    tok_spec = P(('dp', 'pp'), 'ep', None, None)
    cnt_spec = P(('dp', 'pp'), 'ep', None)
    gain_spec = P('pp', None)
    attn_spec = P('pp', None, None, None)
    router_spec = P('pp', None, None)
    expert_spec = P('pp', 'ep', None, None)
    gain_out = P(('dp', 'pp'), None)
    attn_out_spec = P(('dp', 'pp'), None, None, None)
    router_out = P(('dp', 'pp'), None, None)
    expert_out_spec = P(('dp', 'pp'), 'ep', None, None)
    in_specs = (tok_spec, tok_spec, tok_spec, tok_spec, tok_spec, cnt_spec, cnt_spec, gain_spec, gain_spec,
                attn_spec, attn_spec, attn_spec, attn_spec, router_spec, expert_spec, expert_spec, expert_spec)
    out_specs = (tok_spec, tok_spec, gain_out, gain_out, attn_out_spec, attn_out_spec, attn_out_spec, attn_out_spec,
                 router_out, expert_out_spec, expert_out_spec, expert_out_spec)
    return jax.shard_map(device_tick, mesh=mesh, in_specs=in_specs, out_specs=out_specs, check_vma=False)
```

```python
import functools

import jax
import jax.numpy as jnp
from jax import lax
from jax.experimental import pallas as pl
from jax.experimental.pallas import tpu as pltpu
from jax.sharding import PartitionSpec as P

NORM_EPS = 1e-6
MASK_VALUE = -1e30
F32 = jnp.float32
BF16 = jnp.bfloat16
MESH = pl.DeviceIdType.MESH
VMEM = pltpu.VMEM
FFN_TILE = 256
LANES = 128
ROW_BLOCK = 128
RING = 3
HEAD_VMEM = 34 * 2 ** 20
MOE_VMEM = 44 * 2 ** 20
TAIL_VMEM = 30 * 2 ** 20
DENSE_VMEM = 24 * 2 ** 20


def dot_nn(lhs, rhs):
    return lax.dot_general(lhs, rhs, (((1,), (0,)), ((), ())), preferred_element_type=F32)


def dot_nt(lhs, rhs):
    return lax.dot_general(lhs, rhs, (((1,), (1,)), ((), ())), preferred_element_type=F32)


def dot_tn(lhs, rhs):
    return lax.dot_general(lhs, rhs, (((0,), (0,)), ((), ())), preferred_element_type=F32)


def ep_peers():
    me = lax.axis_index('ep')
    partner = me + 1 - 2 * lax.rem(me, 2)
    across = lax.rem(me + 2, 4)
    diag = lax.rem(partner + 2, 4)
    return me, partner, across, diag


def greet(peers):
    barrier = pltpu.get_barrier_semaphore()
    for peer in peers:
        pl.semaphore_signal(barrier, inc=1, device_id=peer, device_id_type=MESH)
    pl.semaphore_wait(barrier, len(peers))


def push(src, dst, sems, idx, peer):
    return pltpu.make_async_remote_copy(src_ref=src, dst_ref=dst, send_sem=sems[0].at[idx], recv_sem=sems[1].at[idx],
                                        device_id=peer, device_id_type=MESH)


def stack_heads(wide, heads, head_dim):
    return jnp.concatenate([wide[:, h * head_dim:(h + 1) * head_dim] for h in range(heads)], axis=0)


def unstack_heads(tall, heads, seq_len):
    return jnp.concatenate([tall[h * seq_len:(h + 1) * seq_len] for h in range(heads)], axis=1)


def rms_inv(x_f32):
    return lax.rsqrt(jnp.mean(x_f32 * x_f32, axis=-1, keepdims=True) + NORM_EPS)


def attention_rows(x_bf, gain, wq, wk, wv, wo, n_seq, heads):
    seq_len, head_dim = x_bf.shape[0] // n_seq, wk.shape[1]
    x_f32 = x_bf.astype(F32)
    normed = (x_f32 * rms_inv(x_f32) * gain).astype(BF16)
    query = dot_nn(normed, wq).astype(BF16)
    key = dot_nn(normed, wk).astype(BF16)
    value = dot_nn(normed, wv).astype(BF16)
    row = lax.rem(lax.broadcasted_iota(jnp.int32, (heads * seq_len, seq_len), 0), seq_len)
    col = lax.broadcasted_iota(jnp.int32, (heads * seq_len, seq_len), 1)
    causal = row >= col
    outs, probs_all = [], []
    for s in range(n_seq):
        rows = slice(s * seq_len, (s + 1) * seq_len)
        scores = dot_nt(stack_heads(query[rows], heads, head_dim), key[rows]) * head_dim ** -0.5
        scores = jnp.where(causal, scores, MASK_VALUE)
        expd = jnp.exp(scores - jnp.max(scores, axis=-1, keepdims=True))
        probs = expd / jnp.sum(expd, axis=-1, keepdims=True)
        probs_all.append(probs)
        outs.append(unstack_heads(dot_nn(probs.astype(BF16), value[rows]).astype(BF16), heads, seq_len))
    attn = jnp.concatenate(outs, axis=0)
    hidden = (x_f32 + dot_nn(attn, wo)).astype(BF16)
    return hidden, (normed, query, key, value, probs_all, attn)


def route_rows(hidden, gain, wr, cols, counts, base, n_seq):
    seq_len = hidden.shape[0] // n_seq
    h_f32 = hidden.astype(F32)
    normed = (h_f32 * rms_inv(h_f32) * gain).astype(BF16)
    logits = dot_nn(normed, wr)
    lane = lax.broadcasted_iota(jnp.int32, (seq_len, LANES), 1).astype(F32)
    lower = (lax.broadcasted_iota(jnp.int32, (seq_len, seq_len), 0)
             > lax.broadcasted_iota(jnp.int32, (seq_len, seq_len), 1)).astype(F32).astype(BF16)
    weights, masks, routes = [], [], []
    for s in range(n_seq):
        id0, id1 = cols[s][base], cols[s][base + 1]
        hot0, hot1 = (lane == id0).astype(F32), (lane == id1).astype(F32)
        rank = dot_nn(lower, (hot0 + hot1).astype(BF16))
        rank1 = rank + (id0 == id1).astype(F32)
        kept0 = hot0 * (rank < counts[s]).astype(F32)
        kept1 = hot1 * (rank1 < counts[s]).astype(F32)
        part = logits[s * seq_len:(s + 1) * seq_len]
        sel0 = jnp.sum(jnp.where(hot0 > 0, part, 0.0), axis=-1, keepdims=True)
        sel1 = jnp.sum(jnp.where(hot1 > 0, part, 0.0), axis=-1, keepdims=True)
        top = jnp.maximum(sel0, sel1)
        exp0, exp1 = jnp.exp(sel0 - top), jnp.exp(sel1 - top)
        gate0, gate1 = exp0 / (exp0 + exp1), exp1 / (exp0 + exp1)
        weights.append(kept0 * gate0 + kept1 * gate1)
        masks.append(jnp.maximum(kept0, kept1))
        keep0 = jnp.sum(kept0, axis=-1, keepdims=True)
        keep1 = jnp.sum(kept1, axis=-1, keepdims=True)
        route = jnp.zeros((seq_len, LANES), F32)
        for i, item in enumerate((id0, id1, gate0, gate1, keep0, keep1)):
            route = jnp.where(lane == i, item, route)
        routes.append(route)
    return normed, jnp.concatenate(weights, 0), jnp.concatenate(masks, 0), jnp.concatenate(routes, 0)


def head_kernel(n_ep, heads, ida_hbm, idb_hbm, cta_hbm, ctb_hbm, xa_hbm, xb_hbm, gb_hbm, gain1_hbm, gain2_hbm, wq_hbm, wk_hbm,
                wv_hbm, wo_hbm, wr_hbm,
                xb_all, gb_all, n2a_ref, n2b_ref, wta_ref, ma_ref, wtb_ref, mb_ref, rtb_ref, ha_ref, hb_ref,
                n1_ref, q_ref, k_ref, v_ref, p_ref, o_ref,
                xa_all, pk_ref, pk_all, ida_ref, idb_ref, cta_ref, ctb_ref, gain1_ref, gain2_ref, wq_s, wk_ref, wv_ref, wo_ref,
                wr_ref, wr_s, load_sem, send_sem, recv_sem):
    me, partner, across, diag = ep_peers()
    sems = (send_sem, recv_sem)
    moves = [(ida_hbm, ida_ref), (idb_hbm, idb_ref), (cta_hbm, cta_ref), (ctb_hbm, ctb_ref), (xb_hbm, xb_all.at[me]),
             (xa_hbm, xa_all.at[me]), (gb_hbm, gb_all.at[me]), (gain1_hbm, gain1_ref), (gain2_hbm, gain2_ref)]
    moves += [(wq_hbm.at[h], wq_s.at[:, pl.ds(h * LANES, LANES)]) for h in range(heads)]
    moves += [(wk_hbm, wk_ref), (wv_hbm, wv_ref), (wo_hbm, wo_ref), (wr_hbm, wr_ref)]
    loads = [pltpu.make_async_copy(src, dst, load_sem.at[i]) for i, (src, dst) in enumerate(moves)]
    for load in loads:
        load.start()
    greet(({'ep': partner}, {'ep': across}))
    landing = (pk_all, xb_all, xa_all, gb_all)
    far, near, relay = [], [], []
    for i in range(4):
        own = pk_ref if i == 0 else landing[i].at[me]
        far.append(push(own, landing[i].at[me], sems, 3 * i, {'ep': across}))
        near.append(push(own, landing[i].at[me], sems, 3 * i + 1, {'ep': partner}))
        relay.append(push(landing[i].at[across], landing[i].at[across], sems, 3 * i + 2, {'ep': partner}))

    def leave(i):
        far[i].start()
        near[i].start()

    def arrive(i):
        far[i].wait_recv()
        relay[i].start()
        near[i].wait_recv()
        relay[i].wait_recv()

    for load in loads[0:4]:
        load.wait()
    pk_ref[...] = jnp.zeros_like(pk_ref)
    pk_ref[0:2, :] = ida_ref[...]
    pk_ref[2:4, :] = idb_ref[...]
    pk_ref[4:5, 0:cta_ref.shape[1]] = cta_ref[...]
    pk_ref[5:6, 0:ctb_ref.shape[1]] = ctb_ref[...]
    pk_all[me] = pk_ref[...]
    loads[4].wait()
    leave(1)
    leave(0)
    loads[5].wait()
    leave(2)
    loads[6].wait()
    leave(3)
    for load in loads[7:]:
        load.wait()
    wr_s[...] = jnp.zeros_like(wr_s)
    wr_s[0:wr_ref.shape[0], :] = wr_ref[...]
    wr = wr_s[...].T
    gain1, gain2 = gain1_ref[...].astype(F32), gain2_ref[...].astype(F32)

    arrive(0)
    packed = pk_all[...].astype(F32)
    flat = jnp.concatenate([packed[s] for s in range(n_ep)] + [jnp.zeros((LANES - 8 * n_ep, LANES), F32)], axis=0).T
    cols = [[flat[:, 8 * s + r:8 * s + r + 1] for r in range(4)] for s in range(n_ep)]
    counts_a = [packed[s, 4:5, :] for s in range(n_ep)]
    counts_b = [packed[s, 5:6, :] for s in range(n_ep)]

    def rows_of(ref):
        return jnp.concatenate([ref[s] for s in range(n_ep)], axis=0)

    arrive(1)
    hidden, (normed, query, key, value, probs, attn) = attention_rows(
        rows_of(xb_all), gain1, wq_s[...], wk_ref[...], wv_ref[...], wo_ref[...], n_ep, heads)
    n1_ref[...], q_ref[...], k_ref[...], v_ref[...], o_ref[...] = normed, query, key, value, attn
    for s in range(n_ep):
        p_ref[s] = probs[s]
    hb_ref[...] = hidden
    n2b_ref[...], wtb_ref[...], mb_ref[...], rtb_ref[...] = route_rows(hidden, gain2, wr, cols, counts_b, 2, n_ep)

    arrive(2)
    hidden, _ = attention_rows(rows_of(xa_all), gain1, wq_s[...], wk_ref[...], wv_ref[...], wo_ref[...], n_ep, heads)
    ha_ref[...] = hidden
    n2a_ref[...], wta_ref[...], ma_ref[...], _ = route_rows(hidden, gain2, wr, cols, counts_a, 0, n_ep)

    arrive(3)
    for i in range(4):
        far[i].wait_send()
        near[i].wait_send()
        relay[i].wait_send()


def moe_kernel(e_local, n2a_ref, n2b_ref, g_ref, wta_ref, ma_ref, wtb_ref, mb_ref, w1_hbm, w3_hbm, w2_hbm,
               ra_ref, rb_ref, dw1_ref, dw3_ref, dw2_ref, x_a, x_b, xbt, dexp, acc_a, acc_b, dacc, put_a, put_b, wcol, ring_1, ring_3, ring_2,
               w1_all, w3_all, w2_all, ring_sem, load_sem, blocks):
    expert, tile = pl.program_id(0), pl.program_id(1)
    n_tile = pl.num_programs(1)
    step = expert * n_tile + tile
    slot = lax.rem(step, RING)

    def leaving(step, slot):
        expert, start = step // n_tile, pl.multiple_of(lax.rem(step, n_tile) * FFN_TILE, FFN_TILE)
        span = pl.ds(start, FFN_TILE)
        return [pltpu.make_async_copy(ring_1.at[slot], dw1_ref.at[expert, :, span], ring_sem.at[slot, 0]),
                pltpu.make_async_copy(ring_3.at[slot], dw3_ref.at[expert, :, span], ring_sem.at[slot, 1]),
                pltpu.make_async_copy(ring_2.at[slot], dw2_ref.at[expert, span, :], ring_sem.at[slot, 2])]

    def coming(step, slot):
        expert, start = step // n_tile, pl.multiple_of(lax.rem(step, n_tile) * FFN_TILE, FFN_TILE)
        span = pl.ds(start, FFN_TILE)
        return [pltpu.make_async_copy(w1_hbm.at[expert, :, span], w1_all.at[slot], load_sem.at[slot, 0]),
                pltpu.make_async_copy(w3_hbm.at[expert, :, span], w3_all.at[slot], load_sem.at[slot, 1]),
                pltpu.make_async_copy(w2_hbm.at[expert, span, :], w2_all.at[slot], load_sem.at[slot, 2])]

    @pl.when(step == 0)
    def _():
        for ahead in range(RING):
            for copy in coming(ahead, ahead):
                copy.start()

    n_tok, d_model = n2a_ref.shape
    here = lax.axis_index('ep') * e_local + expert
    n_block = n_tok // ROW_BLOCK

    def by_rows(which, work):
        for count in range(1, n_block + 1):
            pl.when(blocks[which] == count)(functools.partial(work, count * ROW_BLOCK))

    @pl.when(tile == 0)
    def _():
        mine = lax.broadcasted_iota(jnp.int32, (n_tok, LANES), 1) == here
        mine_t = lax.broadcasted_iota(jnp.int32, (LANES, n_tok), 0) == here
        lower = (lax.broadcasted_iota(jnp.int32, (n_tok, n_tok), 0)
                 > lax.broadcasted_iota(jnp.int32, (n_tok, n_tok), 1)).astype(F32).astype(BF16)
        slot_col = lax.broadcasted_iota(jnp.int32, (n_tok, n_tok), 1).astype(F32)
        slot_row = lax.broadcasted_iota(jnp.int32, (n_tok, n_tok), 0).astype(F32)

        def plan(which, mask_ref, put):
            mask = mask_ref[...]
            place = jnp.where(mask > 0, dot_nn(lower, mask.astype(BF16)), -1.0)
            place_col = jnp.sum(jnp.where(mine, place, 0.0), axis=-1, keepdims=True)
            place_row = jnp.sum(jnp.where(mine_t, place.T, 0.0), axis=0, keepdims=True)
            put[...] = (slot_col == place_col).astype(F32).astype(BF16)
            total = jnp.sum(jnp.where(mine, mask, 0.0)).astype(jnp.int32)
            blocks[which] = jnp.maximum((total + ROW_BLOCK - 1) // ROW_BLOCK, 1)
            return (slot_row == place_row).astype(F32).astype(BF16)

        take_a, take_b = plan(0, ma_ref, put_a), plan(1, mb_ref, put_b)
        wcol[...] = jnp.broadcast_to(jnp.sum(jnp.where(mine, wta_ref[...], 0.0), axis=-1, keepdims=True), (n_tok, LANES))
        wt_b = jnp.sum(jnp.where(mine, wtb_ref[...], 0.0), axis=-1, keepdims=True)
        scaled = (wt_b * g_ref[...].astype(F32)).astype(BF16)

        def fetch_a(rows):
            x_a[0:rows, :] = dot_nn(take_a[0:rows], n2a_ref[...]).astype(BF16)
            acc_a[0:rows, :] = jnp.zeros((rows, d_model), F32)

        def fetch_b(rows):
            fetched = dot_nn(take_b[0:rows], n2b_ref[...])
            x_b[0:rows, :] = fetched.astype(BF16)
            xbt[:, 0:rows] = fetched.T.astype(BF16)
            dexp[0:rows, :] = dot_nn(take_b[0:rows], scaled).astype(BF16)
            acc_b[0:rows, :] = jnp.zeros((rows, d_model), F32)
            dacc[0:rows, :] = jnp.zeros((rows, d_model), F32)

        by_rows(0, fetch_a)
        by_rows(1, fetch_b)

    @pl.when((tile == 0) & (expert == 0))
    def _():
        ra_ref[...] = jnp.zeros_like(ra_ref)
        rb_ref[...] = jnp.zeros_like(rb_ref)

    for copy in coming(step, slot):
        copy.wait()

    @pl.when(step >= RING)
    def _():
        for copy in leaving(step - RING, slot):
            copy.wait()

    w1_ref, w3_ref, w2_ref = w1_all.at[slot], w3_all.at[slot], w2_all.at[slot]

    def forward(x, rows):
        gate_pre, up_pre = dot_nn(x[0:rows, :], w1_ref[...]), dot_nn(x[0:rows, :], w3_ref[...])
        sig = jax.nn.sigmoid(gate_pre)
        return gate_pre, up_pre, sig, (gate_pre * sig * up_pre).astype(BF16)

    def run_a(rows):
        act = forward(x_a, rows)[3]
        acc_a[0:rows, :] += dot_nn(act, w2_ref[...])

    def run_b(rows):
        gate_pre, up_pre, sig, act = forward(x_b, rows)
        acc_b[0:rows, :] += dot_nn(act, w2_ref[...])
        d_exp = dexp[0:rows, :]
        d_act = dot_nt(d_exp, w2_ref[...]).astype(BF16).astype(F32)
        d_up = (d_act * gate_pre * sig).astype(BF16)
        d_gate = (d_act * up_pre * sig * (1.0 + gate_pre * (1.0 - sig))).astype(BF16)
        ring_1[slot] = dot_nn(xbt[:, 0:rows], d_gate)
        ring_3[slot] = dot_nn(xbt[:, 0:rows], d_up)
        ring_2[slot] = dot_tn(act, d_exp)
        dacc[0:rows, :] += dot_nt(d_gate, w1_ref[...]) + dot_nt(d_up, w3_ref[...])

    by_rows(1, run_b)
    for copy in leaving(step, slot):
        copy.start()
    by_rows(0, run_a)

    @pl.when(step + RING < pl.num_programs(0) * n_tile)
    def _():
        for copy in coming(step + RING, slot):
            copy.start()

    def return_a(rows):
        ra_ref[...] += wcol[:, 0:1] * dot_nn(put_a[:, 0:rows], acc_a[0:rows, :].astype(BF16))

    def return_b(rows):
        put = put_b[:, 0:rows]
        rb_ref[:, 0:d_model] += dot_nn(put, dacc[0:rows, :].astype(BF16))
        out_b = dot_nn(put, acc_b[0:rows, :].astype(BF16))
        pick = jnp.sum(out_b * g_ref[...].astype(F32), axis=-1, keepdims=True)
        lane = lax.broadcasted_iota(jnp.int32, (n_tok, LANES), 1)
        rb_ref[:, d_model:] += jnp.where(lane == here, pick, 0.0)

    @pl.when(tile == pl.num_programs(1) - 1)
    def _():
        by_rows(0, return_a)
        by_rows(1, return_b)

    @pl.when(step == pl.num_programs(0) * n_tile - 1)
    def _():
        for back in range(RING - 1, -1, -1):
            for copy in leaving(step - back, lax.rem(step - back, RING)):
                copy.wait()


def tail_kernel(n_ep, n_pp, heads, ra_ref, rb_ref, ha_ref, hb_ref, n2b_ref, gb_ref, rtb_ref, x_ref, q_ref, k_ref, v_ref,
                p_ref, gain1_ref, gain2_ref, wq_ref, wk_ref, wv_ref, wo_ref, wr_ref,
                y_ref, dx_ref, dq_ref, dk_ref, dv_ref, dh_all, dg1_ref, sums_ref,
                near_b, swap_b, sum_b, far_b, near_a, swap_a, sum_a, far_a, small, small_1, small_2, small_3,
                y_own, dx_own, wq_s, wr_s, send_sem, recv_sem):
    me, partner, across, diag = ep_peers()
    stage = lax.axis_index('pp')
    later, earlier = lax.rem(stage + 1, n_pp), lax.rem(stage + n_pp - 1, n_pp)
    seq_len, d_model = y_ref.shape
    sems = (send_sem, recv_sem)
    near, over = {'ep': partner}, {'ep': across}
    greet((near, over, {'pp': later}, {'pp': earlier}))
    swap_b_c = push(rb_ref.at[diag], swap_b, sems, 0, near)
    near_b_c = push(rb_ref.at[partner], near_b, sems, 1, near)
    swap_a_c = push(ra_ref.at[diag], swap_a, sems, 2, near)
    near_a_c = push(ra_ref.at[partner], near_a, sems, 3, near)
    far_b_c = push(sum_b, far_b, sems, 4, over)
    far_a_c = push(sum_a, far_a, sems, 5, over)
    swap_b_c.start()
    near_b_c.start()
    swap_a_c.start()
    near_a_c.start()
    for h in range(heads):
        wq_s[:, h * LANES:(h + 1) * LANES] = wq_ref[h]
    wr_s[...] = jnp.zeros_like(wr_s)
    wr_s[0:wr_ref.shape[0], :] = wr_ref[...]
    swap_b_c.wait_recv()
    sum_b[...] = rb_ref[across] + swap_b[...]
    far_b_c.start()
    swap_a_c.wait_recv()
    sum_a[...] = ra_ref[across] + swap_a[...]

    gain1, gain2 = gain1_ref[...].astype(F32), gain2_ref[...].astype(F32)
    mine = pl.ds(pl.multiple_of(me * seq_len, seq_len), seq_len)
    route = rtb_ref[mine, :]
    id0, id1, gate0, gate1, keep0, keep1 = [route[:, i:i + 1] for i in range(6)]
    lane = lax.broadcasted_iota(jnp.int32, (seq_len, LANES), 1).astype(F32)
    hot0, hot1 = (lane == id0).astype(F32), (lane == id1).astype(F32)
    h_f32 = hb_ref[mine, :].astype(F32)
    inv = rms_inv(h_f32)
    h_hat = h_f32 * inv
    near_b_c.wait_recv()
    far_b_c.wait_recv()
    total = rb_ref[me] + near_b[...] + far_b[...]
    dots = total[:, d_model:]
    d_gate0 = jnp.where(keep0 > 0, jnp.sum(hot0 * dots, axis=-1, keepdims=True), 0.0)
    d_gate1 = jnp.where(keep1 > 0, jnp.sum(hot1 * dots, axis=-1, keepdims=True), 0.0)
    mean_gate = gate0 * d_gate0 + gate1 * d_gate1
    d_logits = (hot0 * (gate0 * (d_gate0 - mean_gate)) + hot1 * (gate1 * (d_gate1 - mean_gate))).astype(BF16)
    d_normed = total[:, :d_model] + dot_nn(d_logits, wr_s[...])
    d_hat = d_normed * gain2
    d_in = inv * (d_hat - h_hat * jnp.mean(d_hat * h_hat, axis=-1, keepdims=True))
    dh_all[me] = (d_in + gb_ref[me].astype(F32)).astype(BF16)
    dh_far = push(dh_all.at[me], dh_all.at[me], sems, 6, over)
    dh_near = push(dh_all.at[me], dh_all.at[me], sems, 7, near)
    dh_relay = push(dh_all.at[across], dh_all.at[across], sems, 8, near)
    dh_far.start()
    dh_near.start()
    small[0:8, :] = dot_tn(d_logits, n2b_ref[mine, :])[0:8, :]
    small[8:16, :] = jnp.broadcast_to(jnp.sum(d_normed * h_hat, axis=0, keepdims=True), (8, d_model))
    small_near = push(small, small_1, sems, 9, near)
    small_near.start()

    head_dim = wk_ref.shape[1]

    def attention_back(s):
        rows = pl.ds(pl.multiple_of(s * seq_len, seq_len), seq_len)
        d_hid = dh_all[s]
        d_out = stack_heads(dot_nt(d_hid, wo_ref[...]).astype(BF16), heads, head_dim)
        probs = p_ref[s]
        d_probs = dot_nt(d_out, v_ref[rows, :])
        d_v = dot_tn(probs.astype(BF16), d_out).astype(BF16)
        d_scores = (probs * (d_probs - jnp.sum(probs * d_probs, axis=-1, keepdims=True)) * head_dim ** -0.5).astype(BF16)
        d_q = unstack_heads(dot_nn(d_scores, k_ref[rows, :]).astype(BF16), heads, seq_len)
        d_k = dot_tn(d_scores, stack_heads(q_ref[rows, :], heads, head_dim)).astype(BF16)
        dq_ref[rows, :], dk_ref[rows, :], dv_ref[rows, :] = d_q, d_k, d_v
        d_norm1 = dot_nt(d_q, wq_s[...]) + dot_nt(d_k, wk_ref[...]) + dot_nt(d_v, wv_ref[...])
        x_f32 = x_ref[s].astype(F32)
        inv1 = rms_inv(x_f32)
        x_hat = x_f32 * inv1
        dg1_ref[s] = jnp.broadcast_to(jnp.sum(d_norm1 * x_hat, axis=0, keepdims=True), (8, d_model))
        return d_hid, d_norm1, inv1, x_hat

    d_hid, d_norm1, inv1, x_hat = attention_back(me)
    d_hat1 = d_norm1 * gain1
    d_x = inv1 * (d_hat1 - x_hat * jnp.mean(d_hat1 * x_hat, axis=-1, keepdims=True)) + d_hid.astype(F32)
    dx_own[...] = d_x.astype(BF16)
    dx_c = push(dx_own, dx_ref, sems, 11, {'pp': earlier})
    dx_c.start()
    small_near.wait_recv()
    small_2[...] = small[...] + small_1[...]
    small_far = push(small_2, small_3, sems, 10, over)
    small_far.start()
    far_a_c.start()
    dh_near.wait_recv()
    attention_back(partner)
    dh_far.wait_recv()
    dh_relay.start()
    attention_back(across)
    dh_relay.wait_recv()
    attention_back(diag)

    near_a_c.wait_recv()
    far_a_c.wait_recv()
    y_own[...] = (ha_ref[mine, :].astype(F32) + (ra_ref[me] + near_a[...] + far_a[...])).astype(BF16)
    y_c = push(y_own, y_ref, sems, 12, {'pp': later})
    y_c.start()
    small_far.wait_recv()
    sums_ref[...] = small_2[...] + small_3[...]
    dx_c.wait_recv()
    y_c.wait_recv()
    for copy in (swap_b_c, near_b_c, swap_a_c, near_a_c, far_b_c, far_a_c, dh_far, dh_near, dh_relay, small_near, small_far,
                 dx_c, y_c):
        copy.wait_send()


def dense_kernel(n1_ref, o_ref, dq_ref, dk_ref, dv_ref, dh_ref, dg1_in, sums_in, y_in, dx_in,
                 dwq_ref, dwk_ref, dwv_ref, dwo_ref, dg1_ref, dg2_ref, dwr_ref, y_ref, dx_ref, n1t):
    step = pl.program_id(0)

    @pl.when(step == 0)
    def _():
        n1t[...] = n1_ref[...].astype(F32).T.astype(BF16)
        dwk_ref[...] = dot_nn(n1t[...], dk_ref[...])
        dwv_ref[...] = dot_nn(n1t[...], dv_ref[...])
        dg1_ref[...] = sum(dg1_in[s] for s in range(dg1_in.shape[0]))[0:1]
        dwr_ref[...] = sums_in[0:8, :]
        dg2_ref[...] = sums_in[8:9, :]
        y_ref[...] = y_in[...]
        dx_ref[...] = dx_in[...]

    pair = dot_nn(n1t[...], dq_ref[...])
    for i in range(dwq_ref.shape[0]):
        dwq_ref[i] = pair[:, i * LANES:(i + 1) * LANES]
    dwo_ref[...] = dot_tn(o_ref[...], dh_ref[...])


def shape_of(shape, dtype):
    return jax.ShapeDtypeStruct(shape, dtype)


def solution(mesh):
    n_ep, n_pp = mesh.shape['ep'], mesh.shape['pp']
    whole = pl.BlockSpec(memory_space=VMEM)

    def device_tick(x_a, x_b, g_b, ids_a, ids_b, count_a, count_b, gain_1, gain_2, w_q, w_k, w_v, w_o, w_r, w_1, w_3, w_2):
        seq_len, d_model = x_a.shape[2], x_a.shape[3]
        heads, head_dim = w_q.shape[2], w_q.shape[3]
        n_exp, e_local, ffn = w_r.shape[2], w_1.shape[1], w_1.shape[3]
        n_tok = n_ep * seq_len
        width = heads * head_dim
        xa, xb, gb = x_a[0, 0], x_b[0, 0], g_b[0, 0]
        wq = jnp.transpose(w_q[0], (1, 0, 2))
        wk, wv, wo = w_k[0, :, 0], w_v[0, :, 0], w_o[0].reshape(width, d_model)
        wr = jnp.transpose(w_r[0])
        tok, rows = (n_ep, seq_len, d_model), (n_tok, d_model)
        head_out = [shape_of(tok, BF16), shape_of(tok, BF16), shape_of(rows, BF16), shape_of(rows, BF16),
                    shape_of((n_tok, LANES), F32), shape_of((n_tok, LANES), F32), shape_of((n_tok, LANES), F32),
                    shape_of((n_tok, LANES), F32), shape_of((n_tok, LANES), F32), shape_of(rows, BF16), shape_of(rows, BF16),
                    shape_of(rows, BF16), shape_of((n_tok, width), BF16), shape_of((n_tok, head_dim), BF16),
                    shape_of((n_tok, head_dim), BF16), shape_of((n_ep, heads * seq_len, seq_len), F32),
                    shape_of((n_tok, width), BF16)]
        (xb_all, gb_all, n2a, n2b, wta, m_a, wtb, m_b, rtb, ha, hb, n1, q, k, v, probs, attn) = pl.pallas_call(
            functools.partial(head_kernel, n_ep, heads),
            out_shape=head_out,
            in_specs=[pl.BlockSpec(memory_space=pltpu.HBM)] * 14,
            out_specs=[whole] * len(head_out),
            scratch_shapes=[VMEM(tok, BF16), VMEM((8, LANES), jnp.int32), VMEM((n_ep, 8, LANES), jnp.int32),
                            VMEM((2, seq_len), jnp.int32), VMEM((2, seq_len), jnp.int32), VMEM((1, n_exp), jnp.int32),
                            VMEM((1, n_exp), jnp.int32), VMEM((1, d_model), BF16), VMEM((1, d_model), BF16),
                            VMEM((d_model, width), BF16), VMEM((d_model, head_dim), BF16), VMEM((d_model, head_dim), BF16),
                            VMEM((width, d_model), BF16), VMEM((n_exp, d_model), BF16), VMEM((LANES, d_model), BF16),
                            pltpu.SemaphoreType.DMA((13 + heads,)), pltpu.SemaphoreType.DMA((12,)),
                            pltpu.SemaphoreType.DMA((12,))],
            compiler_params=pltpu.CompilerParams(collective_id=0, has_side_effects=True, vmem_limit_bytes=HEAD_VMEM),
            name='head',
        )(*[pltpu.with_memory_space_constraint(arg, pltpu.HBM) for arg in (
            ids_a[0, 0].T, ids_b[0, 0].T, count_a[0], count_b[0], xa, xb, gb, gain_1, gain_2, wq, wk, wv, wo, wr)])

        n_tile = ffn // FFN_TILE

        def const(*shape):
            return pl.BlockSpec(shape, lambda e, f: (0,) * len(shape))
        hbm = pl.BlockSpec(memory_space=pltpu.HBM)
        r_a, r_b, dw1, dw3, dw2 = pl.pallas_call(
            functools.partial(moe_kernel, e_local),
            grid=(e_local, n_tile),
            out_shape=[shape_of(rows, F32), shape_of((n_tok, d_model + LANES), F32), shape_of((e_local, d_model, ffn), F32),
                       shape_of((e_local, d_model, ffn), F32), shape_of((e_local, ffn, d_model), F32)],
            in_specs=[const(*rows)] * 3 + [const(n_tok, LANES)] * 4 + [hbm] * 3,
            out_specs=[const(*rows), const(n_tok, d_model + LANES), hbm, hbm, hbm],
            scratch_shapes=[VMEM(rows, BF16), VMEM(rows, BF16), VMEM((d_model, n_tok), BF16), VMEM(rows, BF16),
                            VMEM(rows, F32), VMEM(rows, F32), VMEM(rows, F32), VMEM((n_tok, n_tok), BF16),
                            VMEM((n_tok, n_tok), BF16), VMEM((n_tok, LANES), F32), VMEM((RING, d_model, FFN_TILE), F32),
                            VMEM((RING, d_model, FFN_TILE), F32), VMEM((RING, FFN_TILE, d_model), F32),
                            VMEM((RING, d_model, FFN_TILE), BF16), VMEM((RING, d_model, FFN_TILE), BF16),
                            VMEM((RING, FFN_TILE, d_model), BF16), pltpu.SemaphoreType.DMA((RING, 3)),
                            pltpu.SemaphoreType.DMA((RING, 3)), pltpu.SMEM((2,), jnp.int32)],
            compiler_params=pltpu.CompilerParams(dimension_semantics=('arbitrary', 'arbitrary'),
                                                 vmem_limit_bytes=MOE_VMEM),
            name='moe',
        )(n2a, n2b, gb_all.reshape(rows), wta, m_a, wtb, m_b, w_1[0], w_3[0], w_2[0])

        small = (16, d_model)
        block, wide = (seq_len, d_model), (seq_len, d_model + LANES)
        y_in, dx_in, dq, dk, dv, dh, dg1_in, sums = pl.pallas_call(
            functools.partial(tail_kernel, n_ep, n_pp, heads),
            out_shape=[shape_of(block, BF16), shape_of(block, BF16), shape_of((n_tok, width), BF16),
                       shape_of((n_tok, head_dim), BF16), shape_of((n_tok, head_dim), BF16), shape_of(tok, BF16),
                       shape_of((n_ep, 8, d_model), F32), shape_of(small, F32)],
            in_specs=[whole] * 19,
            out_specs=[whole] * 8,
            scratch_shapes=[VMEM(wide, F32)] * 4 + [VMEM(block, F32)] * 4 + [VMEM(small, F32)] * 4
            + [VMEM(block, BF16), VMEM(block, BF16), VMEM((d_model, width), BF16), VMEM((LANES, d_model), BF16),
               pltpu.SemaphoreType.DMA((13,)), pltpu.SemaphoreType.DMA((13,))],
            compiler_params=pltpu.CompilerParams(collective_id=1, has_side_effects=True, vmem_limit_bytes=TAIL_VMEM),
            name='tail',
        )(r_a.reshape(tok), r_b.reshape((n_ep,) + wide), ha, hb, n2b, gb_all, rtb, xb_all, q, k, v, probs,
          gain_1, gain_2, wq, wk, wv, wo, wr)

        pair = 2
        steps = heads // pair

        def held(*shape):
            return pl.BlockSpec(shape, lambda i: (0,) * len(shape))
        cols = pl.BlockSpec((n_tok, pair * head_dim), lambda i: (0, i))
        dwq, dwk, dwv, dwo, dg1, dg2, dwr, y_next, dx_prev = pl.pallas_call(
            dense_kernel,
            grid=(steps,),
            out_shape=[shape_of((heads, d_model, head_dim), F32), shape_of((d_model, head_dim), F32),
                       shape_of((d_model, head_dim), F32), shape_of((width, d_model), F32), shape_of((1, d_model), F32),
                       shape_of((1, d_model), F32), shape_of((n_exp, d_model), F32), shape_of(block, BF16), shape_of(block, BF16)],
            in_specs=[held(*rows), cols, cols, held(n_tok, head_dim), held(n_tok, head_dim), held(*rows),
                      held(n_ep, 8, d_model), held(*small), held(*block), held(*block)],
            out_specs=[pl.BlockSpec((pair, d_model, head_dim), lambda i: (i, 0, 0)), held(d_model, head_dim),
                       held(d_model, head_dim), pl.BlockSpec((pair * head_dim, d_model), lambda i: (i, 0)),
                       held(1, d_model), held(1, d_model), held(n_exp, d_model), held(*block), held(*block)],
            scratch_shapes=[VMEM((d_model, n_tok), BF16)],
            compiler_params=pltpu.CompilerParams(dimension_semantics=('arbitrary',), vmem_limit_bytes=DENSE_VMEM),
            name='dense',
        )(n1, attn, dq, dk, dv, dh.reshape(rows), dg1_in, sums, y_in, dx_in)
        return (y_next[None, None], dx_prev[None, None], dg1, dg2, jnp.transpose(dwq, (1, 0, 2))[None], dwk[None, :, None],
                dwv[None, :, None], dwo.reshape(w_o.shape), jnp.transpose(dwr)[None], dw1[None], dw3[None], dw2[None])

    tok_spec = P(('dp', 'pp'), 'ep', None, None)
    cnt_spec = P(('dp', 'pp'), 'ep', None)
    gain_spec = P('pp', None)
    attn_spec = P('pp', None, None, None)
    router_spec = P('pp', None, None)
    expert_spec = P('pp', 'ep', None, None)
    gain_out = P(('dp', 'pp'), None)
    attn_out_spec = P(('dp', 'pp'), None, None, None)
    router_out = P(('dp', 'pp'), None, None)
    expert_out_spec = P(('dp', 'pp'), 'ep', None, None)
    in_specs = (tok_spec, tok_spec, tok_spec, tok_spec, tok_spec, cnt_spec, cnt_spec, gain_spec, gain_spec,
                attn_spec, attn_spec, attn_spec, attn_spec, router_spec, expert_spec, expert_spec, expert_spec)
    out_specs = (tok_spec, tok_spec, gain_out, gain_out, attn_out_spec, attn_out_spec, attn_out_spec, attn_out_spec,
                 router_out, expert_out_spec, expert_out_spec, expert_out_spec)
    return jax.shard_map(device_tick, mesh=mesh, in_specs=in_specs, out_specs=out_specs, check_vma=False)
```

```python
import functools

import jax
import jax.numpy as jnp
from jax import lax
from jax.experimental import pallas as pl
from jax.experimental.pallas import tpu as pltpu
from jax.sharding import PartitionSpec as P

NORM_EPS = 1e-6
MASK_VALUE = -1e30
F32 = jnp.float32
BF16 = jnp.bfloat16
MESH = pl.DeviceIdType.MESH
VMEM = pltpu.VMEM
FFN_TILE = 256
LANES = 128
ROW_SIZES = (128, 192, 320, 512)
RING = 3
HEAD_VMEM = 34 * 2 ** 20
MOE_VMEM = 44 * 2 ** 20
TAIL_VMEM = 30 * 2 ** 20
DENSE_VMEM = 24 * 2 ** 20


def dot_nn(lhs, rhs):
    return lax.dot_general(lhs, rhs, (((1,), (0,)), ((), ())), preferred_element_type=F32)


def dot_nt(lhs, rhs):
    return lax.dot_general(lhs, rhs, (((1,), (1,)), ((), ())), preferred_element_type=F32)


def dot_tn(lhs, rhs):
    return lax.dot_general(lhs, rhs, (((0,), (0,)), ((), ())), preferred_element_type=F32)


def ep_peers():
    me = lax.axis_index('ep')
    partner = me + 1 - 2 * lax.rem(me, 2)
    across = lax.rem(me + 2, 4)
    diag = lax.rem(partner + 2, 4)
    return me, partner, across, diag


def greet(peers):
    barrier = pltpu.get_barrier_semaphore()
    for peer in peers:
        pl.semaphore_signal(barrier, inc=1, device_id=peer, device_id_type=MESH)
    pl.semaphore_wait(barrier, len(peers))


def push(src, dst, sems, idx, peer):
    return pltpu.make_async_remote_copy(src_ref=src, dst_ref=dst, send_sem=sems[0].at[idx], recv_sem=sems[1].at[idx],
                                        device_id=peer, device_id_type=MESH)


def stack_heads(wide, heads, head_dim):
    return jnp.concatenate([wide[:, h * head_dim:(h + 1) * head_dim] for h in range(heads)], axis=0)


def unstack_heads(tall, heads, seq_len):
    return jnp.concatenate([tall[h * seq_len:(h + 1) * seq_len] for h in range(heads)], axis=1)


def rms_inv(x_f32):
    return lax.rsqrt(jnp.mean(x_f32 * x_f32, axis=-1, keepdims=True) + NORM_EPS)


def attention_rows(x_bf, gain, wq, wk, wv, wo, n_seq, heads):
    seq_len, head_dim = x_bf.shape[0] // n_seq, wk.shape[1]
    x_f32 = x_bf.astype(F32)
    normed = (x_f32 * rms_inv(x_f32) * gain).astype(BF16)
    query = dot_nn(normed, wq).astype(BF16)
    key = dot_nn(normed, wk).astype(BF16)
    value = dot_nn(normed, wv).astype(BF16)
    row = lax.rem(lax.broadcasted_iota(jnp.int32, (heads * seq_len, seq_len), 0), seq_len)
    col = lax.broadcasted_iota(jnp.int32, (heads * seq_len, seq_len), 1)
    causal = row >= col
    outs, probs_all = [], []
    for s in range(n_seq):
        rows = slice(s * seq_len, (s + 1) * seq_len)
        scores = dot_nt(stack_heads(query[rows], heads, head_dim), key[rows]) * head_dim ** -0.5
        scores = jnp.where(causal, scores, MASK_VALUE)
        expd = jnp.exp(scores - jnp.max(scores, axis=-1, keepdims=True))
        probs = expd / jnp.sum(expd, axis=-1, keepdims=True)
        probs_all.append(probs)
        outs.append(unstack_heads(dot_nn(probs.astype(BF16), value[rows]).astype(BF16), heads, seq_len))
    attn = jnp.concatenate(outs, axis=0)
    hidden = (x_f32 + dot_nn(attn, wo)).astype(BF16)
    return hidden, (normed, query, key, value, probs_all, attn)


def route_rows(hidden, gain, wr, cols, counts, base, n_seq):
    seq_len = hidden.shape[0] // n_seq
    h_f32 = hidden.astype(F32)
    normed = (h_f32 * rms_inv(h_f32) * gain).astype(BF16)
    logits = dot_nn(normed, wr)
    lane = lax.broadcasted_iota(jnp.int32, (seq_len, LANES), 1).astype(F32)
    lower = (lax.broadcasted_iota(jnp.int32, (seq_len, seq_len), 0)
             > lax.broadcasted_iota(jnp.int32, (seq_len, seq_len), 1)).astype(F32).astype(BF16)
    weights, masks, routes = [], [], []
    for s in range(n_seq):
        id0, id1 = cols[s][base], cols[s][base + 1]
        hot0, hot1 = (lane == id0).astype(F32), (lane == id1).astype(F32)
        rank = dot_nn(lower, (hot0 + hot1).astype(BF16))
        rank1 = rank + (id0 == id1).astype(F32)
        kept0 = hot0 * (rank < counts[s]).astype(F32)
        kept1 = hot1 * (rank1 < counts[s]).astype(F32)
        part = logits[s * seq_len:(s + 1) * seq_len]
        sel0 = jnp.sum(jnp.where(hot0 > 0, part, 0.0), axis=-1, keepdims=True)
        sel1 = jnp.sum(jnp.where(hot1 > 0, part, 0.0), axis=-1, keepdims=True)
        top = jnp.maximum(sel0, sel1)
        exp0, exp1 = jnp.exp(sel0 - top), jnp.exp(sel1 - top)
        gate0, gate1 = exp0 / (exp0 + exp1), exp1 / (exp0 + exp1)
        weights.append(kept0 * gate0 + kept1 * gate1)
        masks.append(jnp.maximum(kept0, kept1))
        keep0 = jnp.sum(kept0, axis=-1, keepdims=True)
        keep1 = jnp.sum(kept1, axis=-1, keepdims=True)
        route = jnp.zeros((seq_len, LANES), F32)
        for i, item in enumerate((id0, id1, gate0, gate1, keep0, keep1)):
            route = jnp.where(lane == i, item, route)
        routes.append(route)
    return normed, jnp.concatenate(weights, 0), jnp.concatenate(masks, 0), jnp.concatenate(routes, 0)


def head_kernel(n_ep, heads, ida_hbm, idb_hbm, cta_hbm, ctb_hbm, xa_hbm, xb_hbm, gb_hbm, gain1_hbm, gain2_hbm, wq_hbm, wk_hbm,
                wv_hbm, wo_hbm, wr_hbm,
                xb_all, gb_all, n2a_ref, n2b_ref, wta_ref, ma_ref, wtb_ref, mb_ref, rtb_ref, ha_ref, hb_ref,
                n1_ref, q_ref, k_ref, v_ref, p_ref, o_ref,
                xa_all, pk_ref, pk_all, ida_ref, idb_ref, cta_ref, ctb_ref, gain1_ref, gain2_ref, wq_s, wk_ref, wv_ref, wo_ref,
                wr_ref, wr_s, load_sem, send_sem, recv_sem):
    me, partner, across, diag = ep_peers()
    sems = (send_sem, recv_sem)
    seq_len = xb_all.shape[1]
    moves = [(ida_hbm, ida_ref), (idb_hbm, idb_ref), (cta_hbm, cta_ref), (ctb_hbm, ctb_ref), (xb_hbm, xb_all.at[me]),
             (xa_hbm, xa_all.at[me]), (gb_hbm, gb_all.at[me]), (gain1_hbm, gain1_ref), (gain2_hbm, gain2_ref)]
    moves += [(wq_hbm.at[h], wq_s.at[:, pl.ds(h * LANES, LANES)]) for h in range(heads)]
    moves += [(wk_hbm, wk_ref), (wv_hbm, wv_ref), (wo_hbm, wo_ref), (wr_hbm, wr_ref)]
    loads = [pltpu.make_async_copy(src, dst, load_sem.at[i]) for i, (src, dst) in enumerate(moves)]
    for load in loads:
        load.start()
    greet(({'ep': partner}, {'ep': across}))
    landing = (pk_all, xb_all, xa_all, gb_all)
    far, near, relay = [], [], []
    for i in range(4):
        own = pk_ref if i == 0 else landing[i].at[me]
        far.append(push(own, landing[i].at[me], sems, 3 * i, {'ep': across}))
        near.append(push(own, landing[i].at[me], sems, 3 * i + 1, {'ep': partner}))
        relay.append(push(landing[i].at[across], landing[i].at[across], sems, 3 * i + 2, {'ep': partner}))

    def leave(i):
        far[i].start()
        near[i].start()

    for load in loads[0:4]:
        load.wait()
    pk_ref[...] = jnp.zeros_like(pk_ref)
    pk_ref[0:2, :] = ida_ref[...]
    pk_ref[2:4, :] = idb_ref[...]
    pk_ref[4:5, 0:cta_ref.shape[1]] = cta_ref[...]
    pk_ref[5:6, 0:ctb_ref.shape[1]] = ctb_ref[...]
    pk_all[me] = pk_ref[...]
    loads[4].wait()
    leave(1)
    leave(0)
    loads[5].wait()
    leave(2)
    loads[6].wait()
    leave(3)
    for load in loads[7:]:
        load.wait()
    wr_s[...] = jnp.zeros_like(wr_s)
    wr_s[0:wr_ref.shape[0], :] = wr_ref[...]
    wr = wr_s[...].T
    gain1, gain2 = gain1_ref[...].astype(F32), gain2_ref[...].astype(F32)

    def pair_b(pair):
        x_pair = jnp.concatenate([xb_all[s] for s in pair], axis=0)
        hidden, (normed, query, key, value, probs, attn) = attention_rows(
            x_pair, gain1, wq_s[...], wk_ref[...], wv_ref[...], wo_ref[...], len(pair), heads)
        cols, counts = routing_of(pair)
        routed = route_rows(hidden, gain2, wr, cols, [c[1] for c in counts], 2, len(pair))
        for n, s in enumerate(pair):
            rows, part = pl.ds(pl.multiple_of(s * seq_len, seq_len), seq_len), slice(n * seq_len, (n + 1) * seq_len)
            n1_ref[rows, :], q_ref[rows, :], k_ref[rows, :] = normed[part], query[part], key[part]
            v_ref[rows, :], o_ref[rows, :], hb_ref[rows, :] = value[part], attn[part], hidden[part]
            p_ref[s] = probs[n]
            n2b_ref[rows, :], wtb_ref[rows, :], mb_ref[rows, :], rtb_ref[rows, :] = [item[part] for item in routed]

    def pair_a(pair):
        x_pair = jnp.concatenate([xa_all[s] for s in pair], axis=0)
        hidden, _ = attention_rows(x_pair, gain1, wq_s[...], wk_ref[...], wv_ref[...], wo_ref[...], len(pair), heads)
        cols, counts = routing_of(pair)
        routed = route_rows(hidden, gain2, wr, cols, [c[0] for c in counts], 0, len(pair))
        for n, s in enumerate(pair):
            rows, part = pl.ds(pl.multiple_of(s * seq_len, seq_len), seq_len), slice(n * seq_len, (n + 1) * seq_len)
            ha_ref[rows, :] = hidden[part]
            n2a_ref[rows, :], wta_ref[rows, :], ma_ref[rows, :] = [item[part] for item in routed[:3]]

    def routing_of(pair):
        packed = [pk_all[s].astype(F32) for s in pair]
        flat = jnp.concatenate(packed + [jnp.zeros((LANES - 8 * len(pair), LANES), F32)], axis=0).T
        cols = [[flat[:, 8 * n + r:8 * n + r + 1] for r in range(4)] for n in range(len(pair))]
        return cols, [(item[4:5, :], item[5:6, :]) for item in packed]

    near[0].wait_recv()
    near[1].wait_recv()
    pair_b((me, partner))
    far[0].wait_recv()
    relay[0].start()
    far[1].wait_recv()
    relay[1].start()
    near[2].wait_recv()
    pair_a((me, partner))
    relay[0].wait_recv()
    relay[1].wait_recv()
    far[2].wait_recv()
    relay[2].start()
    pair_b((across, diag))
    relay[2].wait_recv()
    far[3].wait_recv()
    relay[3].start()
    pair_a((across, diag))
    near[3].wait_recv()
    relay[3].wait_recv()
    for i in range(4):
        far[i].wait_send()
        near[i].wait_send()
        relay[i].wait_send()


def moe_kernel(e_local, n2a_ref, n2b_ref, g_ref, wta_ref, ma_ref, wtb_ref, mb_ref, w1_hbm, w3_hbm, w2_hbm,
               ra_ref, rb_ref, dw1_ref, dw3_ref, dw2_ref, x_a, x_b, xbt, dexp, acc_a, acc_b, dacc, put_a, put_b, wcol, ring_1, ring_3, ring_2,
               w1_all, w3_all, w2_all, ring_sem, load_sem, blocks):
    expert, tile = pl.program_id(0), pl.program_id(1)
    n_tile = pl.num_programs(1)
    step = expert * n_tile + tile
    slot = lax.rem(step, RING)

    def leaving(step, slot):
        expert, start = step // n_tile, pl.multiple_of(lax.rem(step, n_tile) * FFN_TILE, FFN_TILE)
        span = pl.ds(start, FFN_TILE)
        return [pltpu.make_async_copy(ring_1.at[slot], dw1_ref.at[expert, :, span], ring_sem.at[slot, 0]),
                pltpu.make_async_copy(ring_3.at[slot], dw3_ref.at[expert, :, span], ring_sem.at[slot, 1]),
                pltpu.make_async_copy(ring_2.at[slot], dw2_ref.at[expert, span, :], ring_sem.at[slot, 2])]

    def coming(step, slot):
        expert, start = step // n_tile, pl.multiple_of(lax.rem(step, n_tile) * FFN_TILE, FFN_TILE)
        span = pl.ds(start, FFN_TILE)
        return [pltpu.make_async_copy(w1_hbm.at[expert, :, span], w1_all.at[slot], load_sem.at[slot, 0]),
                pltpu.make_async_copy(w3_hbm.at[expert, :, span], w3_all.at[slot], load_sem.at[slot, 1]),
                pltpu.make_async_copy(w2_hbm.at[expert, span, :], w2_all.at[slot], load_sem.at[slot, 2])]

    @pl.when(step == 0)
    def _():
        for ahead in range(RING):
            for copy in coming(ahead, ahead):
                copy.start()

    n_tok, d_model = n2a_ref.shape
    here = lax.axis_index('ep') * e_local + expert

    def by_rows(which, work):
        for rows in ROW_SIZES:
            pl.when(blocks[which] == rows)(functools.partial(work, rows))

    @pl.when(tile == 0)
    def _():
        mine = lax.broadcasted_iota(jnp.int32, (n_tok, LANES), 1) == here
        mine_t = lax.broadcasted_iota(jnp.int32, (LANES, n_tok), 0) == here
        lower = (lax.broadcasted_iota(jnp.int32, (n_tok, n_tok), 0)
                 > lax.broadcasted_iota(jnp.int32, (n_tok, n_tok), 1)).astype(F32).astype(BF16)
        slot_col = lax.broadcasted_iota(jnp.int32, (n_tok, n_tok), 1).astype(F32)
        slot_row = lax.broadcasted_iota(jnp.int32, (n_tok, n_tok), 0).astype(F32)

        def plan(which, mask_ref, put):
            mask = mask_ref[...]
            place = jnp.where(mask > 0, dot_nn(lower, mask.astype(BF16)), -1.0)
            place_col = jnp.sum(jnp.where(mine, place, 0.0), axis=-1, keepdims=True)
            place_row = jnp.sum(jnp.where(mine_t, place.T, 0.0), axis=0, keepdims=True)
            put[...] = (slot_col == place_col).astype(F32).astype(BF16)
            total = jnp.sum(jnp.where(mine, mask, 0.0)).astype(jnp.int32)
            size = jnp.int32(n_tok)
            for rows in ROW_SIZES[-2::-1]:
                size = jnp.where(total <= rows, rows, size)
            blocks[which] = size
            return (slot_row == place_row).astype(F32).astype(BF16)

        take_a, take_b = plan(0, ma_ref, put_a), plan(1, mb_ref, put_b)
        wcol[...] = jnp.broadcast_to(jnp.sum(jnp.where(mine, wta_ref[...], 0.0), axis=-1, keepdims=True), (n_tok, LANES))
        wt_b = jnp.sum(jnp.where(mine, wtb_ref[...], 0.0), axis=-1, keepdims=True)
        scaled = (wt_b * g_ref[...].astype(F32)).astype(BF16)

        def fetch_a(rows):
            x_a[0:rows, :] = dot_nn(take_a[0:rows], n2a_ref[...]).astype(BF16)
            acc_a[0:rows, :] = jnp.zeros((rows, d_model), F32)

        def fetch_b(rows):
            fetched = dot_nn(take_b[0:rows], n2b_ref[...])
            x_b[0:rows, :] = fetched.astype(BF16)
            xbt[:, 0:rows] = fetched.T.astype(BF16)
            dexp[0:rows, :] = dot_nn(take_b[0:rows], scaled).astype(BF16)
            acc_b[0:rows, :] = jnp.zeros((rows, d_model), F32)
            dacc[0:rows, :] = jnp.zeros((rows, d_model), F32)

        by_rows(0, fetch_a)
        by_rows(1, fetch_b)

    @pl.when((tile == 0) & (expert == 0))
    def _():
        ra_ref[...] = jnp.zeros_like(ra_ref)
        rb_ref[...] = jnp.zeros_like(rb_ref)

    for copy in coming(step, slot):
        copy.wait()

    @pl.when(step >= RING)
    def _():
        for copy in leaving(step - RING, slot):
            copy.wait()

    w1_ref, w3_ref, w2_ref = w1_all.at[slot], w3_all.at[slot], w2_all.at[slot]

    def forward(x, rows):
        gate_pre, up_pre = dot_nn(x[0:rows, :], w1_ref[...]), dot_nn(x[0:rows, :], w3_ref[...])
        sig = jax.nn.sigmoid(gate_pre)
        return gate_pre, up_pre, sig, (gate_pre * sig * up_pre).astype(BF16)

    def run_a(rows):
        act = forward(x_a, rows)[3]
        acc_a[0:rows, :] += dot_nn(act, w2_ref[...])

    def run_b(rows):
        gate_pre, up_pre, sig, act = forward(x_b, rows)
        acc_b[0:rows, :] += dot_nn(act, w2_ref[...])
        d_exp = dexp[0:rows, :]
        d_act = dot_nt(d_exp, w2_ref[...]).astype(BF16).astype(F32)
        d_up = (d_act * gate_pre * sig).astype(BF16)
        d_gate = (d_act * up_pre * sig * (1.0 + gate_pre * (1.0 - sig))).astype(BF16)
        ring_1[slot] = dot_nn(xbt[:, 0:rows], d_gate)
        ring_3[slot] = dot_nn(xbt[:, 0:rows], d_up)
        ring_2[slot] = dot_tn(act, d_exp)
        dacc[0:rows, :] += dot_nt(d_gate, w1_ref[...]) + dot_nt(d_up, w3_ref[...])

    by_rows(1, run_b)
    for copy in leaving(step, slot):
        copy.start()
    by_rows(0, run_a)

    @pl.when(step + RING < pl.num_programs(0) * n_tile)
    def _():
        for copy in coming(step + RING, slot):
            copy.start()

    def return_a(rows):
        ra_ref[...] += wcol[:, 0:1] * dot_nn(put_a[:, 0:rows], acc_a[0:rows, :].astype(BF16))

    def return_b(rows):
        put = put_b[:, 0:rows]
        rb_ref[:, 0:d_model] += dot_nn(put, dacc[0:rows, :].astype(BF16))
        out_b = dot_nn(put, acc_b[0:rows, :].astype(BF16))
        pick = jnp.sum(out_b * g_ref[...].astype(F32), axis=-1, keepdims=True)
        lane = lax.broadcasted_iota(jnp.int32, (n_tok, LANES), 1)
        rb_ref[:, d_model:] += jnp.where(lane == here, pick, 0.0)

    @pl.when(tile == pl.num_programs(1) - 1)
    def _():
        by_rows(0, return_a)
        by_rows(1, return_b)

    @pl.when(step == pl.num_programs(0) * n_tile - 1)
    def _():
        for back in range(RING - 1, -1, -1):
            for copy in leaving(step - back, lax.rem(step - back, RING)):
                copy.wait()


def tail_kernel(n_ep, n_pp, heads, ra_ref, rb_ref, ha_ref, hb_ref, n2b_ref, gb_ref, rtb_ref, x_ref, q_ref, k_ref, v_ref,
                p_ref, gain1_ref, gain2_ref, wq_ref, wk_ref, wv_ref, wo_ref, wr_ref,
                y_ref, dx_ref, dq_ref, dk_ref, dv_ref, dh_all, dg1_ref, sums_ref,
                near_b, swap_b, sum_b, far_b, near_a, swap_a, sum_a, far_a, small, small_1, small_2, small_3,
                y_own, dx_own, wq_s, wr_s, send_sem, recv_sem):
    me, partner, across, diag = ep_peers()
    stage = lax.axis_index('pp')
    later, earlier = lax.rem(stage + 1, n_pp), lax.rem(stage + n_pp - 1, n_pp)
    seq_len, d_model = y_ref.shape
    sems = (send_sem, recv_sem)
    near, over = {'ep': partner}, {'ep': across}
    greet((near, over, {'pp': later}, {'pp': earlier}))
    swap_b_c = push(rb_ref.at[diag], swap_b, sems, 0, near)
    near_b_c = push(rb_ref.at[partner], near_b, sems, 1, near)
    swap_a_c = push(ra_ref.at[diag], swap_a, sems, 2, near)
    near_a_c = push(ra_ref.at[partner], near_a, sems, 3, near)
    far_b_c = push(sum_b, far_b, sems, 4, over)
    far_a_c = push(sum_a, far_a, sems, 5, over)
    swap_b_c.start()
    near_b_c.start()
    swap_a_c.start()
    near_a_c.start()
    for h in range(heads):
        wq_s[:, h * LANES:(h + 1) * LANES] = wq_ref[h]
    wr_s[...] = jnp.zeros_like(wr_s)
    wr_s[0:wr_ref.shape[0], :] = wr_ref[...]
    swap_b_c.wait_recv()
    sum_b[...] = rb_ref[across] + swap_b[...]
    far_b_c.start()
    swap_a_c.wait_recv()
    sum_a[...] = ra_ref[across] + swap_a[...]

    gain1, gain2 = gain1_ref[...].astype(F32), gain2_ref[...].astype(F32)
    mine = pl.ds(pl.multiple_of(me * seq_len, seq_len), seq_len)
    route = rtb_ref[mine, :]
    id0, id1, gate0, gate1, keep0, keep1 = [route[:, i:i + 1] for i in range(6)]
    lane = lax.broadcasted_iota(jnp.int32, (seq_len, LANES), 1).astype(F32)
    hot0, hot1 = (lane == id0).astype(F32), (lane == id1).astype(F32)
    h_f32 = hb_ref[mine, :].astype(F32)
    inv = rms_inv(h_f32)
    h_hat = h_f32 * inv
    near_b_c.wait_recv()
    far_b_c.wait_recv()
    total = rb_ref[me] + near_b[...] + far_b[...]
    dots = total[:, d_model:]
    d_gate0 = jnp.where(keep0 > 0, jnp.sum(hot0 * dots, axis=-1, keepdims=True), 0.0)
    d_gate1 = jnp.where(keep1 > 0, jnp.sum(hot1 * dots, axis=-1, keepdims=True), 0.0)
    mean_gate = gate0 * d_gate0 + gate1 * d_gate1
    d_logits = (hot0 * (gate0 * (d_gate0 - mean_gate)) + hot1 * (gate1 * (d_gate1 - mean_gate))).astype(BF16)
    d_normed = total[:, :d_model] + dot_nn(d_logits, wr_s[...])
    d_hat = d_normed * gain2
    d_in = inv * (d_hat - h_hat * jnp.mean(d_hat * h_hat, axis=-1, keepdims=True))
    dh_all[me] = (d_in + gb_ref[me].astype(F32)).astype(BF16)
    dh_far = push(dh_all.at[me], dh_all.at[me], sems, 6, over)
    dh_near = push(dh_all.at[me], dh_all.at[me], sems, 7, near)
    dh_relay = push(dh_all.at[across], dh_all.at[across], sems, 8, near)
    dh_far.start()
    dh_near.start()
    small[0:8, :] = dot_tn(d_logits, n2b_ref[mine, :])[0:8, :]
    small[8:16, :] = jnp.broadcast_to(jnp.sum(d_normed * h_hat, axis=0, keepdims=True), (8, d_model))
    small_near = push(small, small_1, sems, 9, near)
    small_near.start()

    head_dim = wk_ref.shape[1]

    def attention_back(s):
        rows = pl.ds(pl.multiple_of(s * seq_len, seq_len), seq_len)
        d_hid = dh_all[s]
        d_out = stack_heads(dot_nt(d_hid, wo_ref[...]).astype(BF16), heads, head_dim)
        probs = p_ref[s]
        d_probs = dot_nt(d_out, v_ref[rows, :])
        d_v = dot_tn(probs.astype(BF16), d_out).astype(BF16)
        d_scores = (probs * (d_probs - jnp.sum(probs * d_probs, axis=-1, keepdims=True)) * head_dim ** -0.5).astype(BF16)
        d_q = unstack_heads(dot_nn(d_scores, k_ref[rows, :]).astype(BF16), heads, seq_len)
        d_k = dot_tn(d_scores, stack_heads(q_ref[rows, :], heads, head_dim)).astype(BF16)
        dq_ref[rows, :], dk_ref[rows, :], dv_ref[rows, :] = d_q, d_k, d_v
        d_norm1 = dot_nt(d_q, wq_s[...]) + dot_nt(d_k, wk_ref[...]) + dot_nt(d_v, wv_ref[...])
        x_f32 = x_ref[s].astype(F32)
        inv1 = rms_inv(x_f32)
        x_hat = x_f32 * inv1
        dg1_ref[s] = jnp.broadcast_to(jnp.sum(d_norm1 * x_hat, axis=0, keepdims=True), (8, d_model))
        return d_hid, d_norm1, inv1, x_hat

    d_hid, d_norm1, inv1, x_hat = attention_back(me)
    d_hat1 = d_norm1 * gain1
    d_x = inv1 * (d_hat1 - x_hat * jnp.mean(d_hat1 * x_hat, axis=-1, keepdims=True)) + d_hid.astype(F32)
    dx_own[...] = d_x.astype(BF16)
    dx_c = push(dx_own, dx_ref, sems, 11, {'pp': earlier})
    dx_c.start()
    small_near.wait_recv()
    small_2[...] = small[...] + small_1[...]
    small_far = push(small_2, small_3, sems, 10, over)
    small_far.start()
    far_a_c.start()
    dh_near.wait_recv()
    attention_back(partner)
    dh_far.wait_recv()
    dh_relay.start()
    attention_back(across)
    dh_relay.wait_recv()
    attention_back(diag)

    near_a_c.wait_recv()
    far_a_c.wait_recv()
    y_own[...] = (ha_ref[mine, :].astype(F32) + (ra_ref[me] + near_a[...] + far_a[...])).astype(BF16)
    y_c = push(y_own, y_ref, sems, 12, {'pp': later})
    y_c.start()
    small_far.wait_recv()
    sums_ref[...] = small_2[...] + small_3[...]
    dx_c.wait_recv()
    y_c.wait_recv()
    for copy in (swap_b_c, near_b_c, swap_a_c, near_a_c, far_b_c, far_a_c, dh_far, dh_near, dh_relay, small_near, small_far,
                 dx_c, y_c):
        copy.wait_send()


def dense_kernel(n1_ref, o_ref, dq_ref, dk_ref, dv_ref, dh_ref, dg1_in, sums_in, y_in, dx_in,
                 dwq_ref, dwk_ref, dwv_ref, dwo_ref, dg1_ref, dg2_ref, dwr_ref, y_ref, dx_ref, n1t):
    step = pl.program_id(0)

    @pl.when(step == 0)
    def _():
        n1t[...] = n1_ref[...].astype(F32).T.astype(BF16)
        dwk_ref[...] = dot_nn(n1t[...], dk_ref[...])
        dwv_ref[...] = dot_nn(n1t[...], dv_ref[...])
        dg1_ref[...] = sum(dg1_in[s] for s in range(dg1_in.shape[0]))[0:1]
        dwr_ref[...] = sums_in[0:8, :]
        dg2_ref[...] = sums_in[8:9, :]
        y_ref[...] = y_in[...]
        dx_ref[...] = dx_in[...]

    pair = dot_nn(n1t[...], dq_ref[...])
    for i in range(dwq_ref.shape[0]):
        dwq_ref[i] = pair[:, i * LANES:(i + 1) * LANES]
    dwo_ref[...] = dot_tn(o_ref[...], dh_ref[...])


def shape_of(shape, dtype):
    return jax.ShapeDtypeStruct(shape, dtype)


def solution(mesh):
    n_ep, n_pp = mesh.shape['ep'], mesh.shape['pp']
    whole = pl.BlockSpec(memory_space=VMEM)

    def device_tick(x_a, x_b, g_b, ids_a, ids_b, count_a, count_b, gain_1, gain_2, w_q, w_k, w_v, w_o, w_r, w_1, w_3, w_2):
        seq_len, d_model = x_a.shape[2], x_a.shape[3]
        heads, head_dim = w_q.shape[2], w_q.shape[3]
        n_exp, e_local, ffn = w_r.shape[2], w_1.shape[1], w_1.shape[3]
        n_tok = n_ep * seq_len
        width = heads * head_dim
        xa, xb, gb = x_a[0, 0], x_b[0, 0], g_b[0, 0]
        wq = jnp.transpose(w_q[0], (1, 0, 2))
        wk, wv, wo = w_k[0, :, 0], w_v[0, :, 0], w_o[0].reshape(width, d_model)
        wr = jnp.transpose(w_r[0])
        tok, rows = (n_ep, seq_len, d_model), (n_tok, d_model)
        head_out = [shape_of(tok, BF16), shape_of(tok, BF16), shape_of(rows, BF16), shape_of(rows, BF16),
                    shape_of((n_tok, LANES), F32), shape_of((n_tok, LANES), F32), shape_of((n_tok, LANES), F32),
                    shape_of((n_tok, LANES), F32), shape_of((n_tok, LANES), F32), shape_of(rows, BF16), shape_of(rows, BF16),
                    shape_of(rows, BF16), shape_of((n_tok, width), BF16), shape_of((n_tok, head_dim), BF16),
                    shape_of((n_tok, head_dim), BF16), shape_of((n_ep, heads * seq_len, seq_len), F32),
                    shape_of((n_tok, width), BF16)]
        (xb_all, gb_all, n2a, n2b, wta, m_a, wtb, m_b, rtb, ha, hb, n1, q, k, v, probs, attn) = pl.pallas_call(
            functools.partial(head_kernel, n_ep, heads),
            out_shape=head_out,
            in_specs=[pl.BlockSpec(memory_space=pltpu.HBM)] * 14,
            out_specs=[whole] * len(head_out),
            scratch_shapes=[VMEM(tok, BF16), VMEM((8, LANES), jnp.int32), VMEM((n_ep, 8, LANES), jnp.int32),
                            VMEM((2, seq_len), jnp.int32), VMEM((2, seq_len), jnp.int32), VMEM((1, n_exp), jnp.int32),
                            VMEM((1, n_exp), jnp.int32), VMEM((1, d_model), BF16), VMEM((1, d_model), BF16),
                            VMEM((d_model, width), BF16), VMEM((d_model, head_dim), BF16), VMEM((d_model, head_dim), BF16),
                            VMEM((width, d_model), BF16), VMEM((n_exp, d_model), BF16), VMEM((LANES, d_model), BF16),
                            pltpu.SemaphoreType.DMA((13 + heads,)), pltpu.SemaphoreType.DMA((12,)),
                            pltpu.SemaphoreType.DMA((12,))],
            compiler_params=pltpu.CompilerParams(collective_id=0, has_side_effects=True, vmem_limit_bytes=HEAD_VMEM),
            name='head',
        )(*[pltpu.with_memory_space_constraint(arg, pltpu.HBM) for arg in (
            ids_a[0, 0].T, ids_b[0, 0].T, count_a[0], count_b[0], xa, xb, gb, gain_1, gain_2, wq, wk, wv, wo, wr)])

        n_tile = ffn // FFN_TILE

        def const(*shape):
            return pl.BlockSpec(shape, lambda e, f: (0,) * len(shape))
        hbm = pl.BlockSpec(memory_space=pltpu.HBM)
        r_a, r_b, dw1, dw3, dw2 = pl.pallas_call(
            functools.partial(moe_kernel, e_local),
            grid=(e_local, n_tile),
            out_shape=[shape_of(rows, F32), shape_of((n_tok, d_model + LANES), F32), shape_of((e_local, d_model, ffn), F32),
                       shape_of((e_local, d_model, ffn), F32), shape_of((e_local, ffn, d_model), F32)],
            in_specs=[const(*rows)] * 3 + [const(n_tok, LANES)] * 4 + [hbm] * 3,
            out_specs=[const(*rows), const(n_tok, d_model + LANES), hbm, hbm, hbm],
            scratch_shapes=[VMEM(rows, BF16), VMEM(rows, BF16), VMEM((d_model, n_tok), BF16), VMEM(rows, BF16),
                            VMEM(rows, F32), VMEM(rows, F32), VMEM(rows, F32), VMEM((n_tok, n_tok), BF16),
                            VMEM((n_tok, n_tok), BF16), VMEM((n_tok, LANES), F32), VMEM((RING, d_model, FFN_TILE), F32),
                            VMEM((RING, d_model, FFN_TILE), F32), VMEM((RING, FFN_TILE, d_model), F32),
                            VMEM((RING, d_model, FFN_TILE), BF16), VMEM((RING, d_model, FFN_TILE), BF16),
                            VMEM((RING, FFN_TILE, d_model), BF16), pltpu.SemaphoreType.DMA((RING, 3)),
                            pltpu.SemaphoreType.DMA((RING, 3)), pltpu.SMEM((2,), jnp.int32)],
            compiler_params=pltpu.CompilerParams(dimension_semantics=('arbitrary', 'arbitrary'),
                                                 vmem_limit_bytes=MOE_VMEM),
            name='moe',
        )(n2a, n2b, gb_all.reshape(rows), wta, m_a, wtb, m_b, w_1[0], w_3[0], w_2[0])

        small = (16, d_model)
        block, wide = (seq_len, d_model), (seq_len, d_model + LANES)
        y_in, dx_in, dq, dk, dv, dh, dg1_in, sums = pl.pallas_call(
            functools.partial(tail_kernel, n_ep, n_pp, heads),
            out_shape=[shape_of(block, BF16), shape_of(block, BF16), shape_of((n_tok, width), BF16),
                       shape_of((n_tok, head_dim), BF16), shape_of((n_tok, head_dim), BF16), shape_of(tok, BF16),
                       shape_of((n_ep, 8, d_model), F32), shape_of(small, F32)],
            in_specs=[whole] * 19,
            out_specs=[whole] * 8,
            scratch_shapes=[VMEM(wide, F32)] * 4 + [VMEM(block, F32)] * 4 + [VMEM(small, F32)] * 4
            + [VMEM(block, BF16), VMEM(block, BF16), VMEM((d_model, width), BF16), VMEM((LANES, d_model), BF16),
               pltpu.SemaphoreType.DMA((13,)), pltpu.SemaphoreType.DMA((13,))],
            compiler_params=pltpu.CompilerParams(collective_id=1, has_side_effects=True, vmem_limit_bytes=TAIL_VMEM),
            name='tail',
        )(r_a.reshape(tok), r_b.reshape((n_ep,) + wide), ha, hb, n2b, gb_all, rtb, xb_all, q, k, v, probs,
          gain_1, gain_2, wq, wk, wv, wo, wr)

        pair = 2
        steps = heads // pair

        def held(*shape):
            return pl.BlockSpec(shape, lambda i: (0,) * len(shape))
        cols = pl.BlockSpec((n_tok, pair * head_dim), lambda i: (0, i))
        dwq, dwk, dwv, dwo, dg1, dg2, dwr, y_next, dx_prev = pl.pallas_call(
            dense_kernel,
            grid=(steps,),
            out_shape=[shape_of((heads, d_model, head_dim), F32), shape_of((d_model, head_dim), F32),
                       shape_of((d_model, head_dim), F32), shape_of((width, d_model), F32), shape_of((1, d_model), F32),
                       shape_of((1, d_model), F32), shape_of((n_exp, d_model), F32), shape_of(block, BF16), shape_of(block, BF16)],
            in_specs=[held(*rows), cols, cols, held(n_tok, head_dim), held(n_tok, head_dim), held(*rows),
                      held(n_ep, 8, d_model), held(*small), held(*block), held(*block)],
            out_specs=[pl.BlockSpec((pair, d_model, head_dim), lambda i: (i, 0, 0)), held(d_model, head_dim),
                       held(d_model, head_dim), pl.BlockSpec((pair * head_dim, d_model), lambda i: (i, 0)),
                       held(1, d_model), held(1, d_model), held(n_exp, d_model), held(*block), held(*block)],
            scratch_shapes=[VMEM((d_model, n_tok), BF16)],
            compiler_params=pltpu.CompilerParams(dimension_semantics=('arbitrary',), vmem_limit_bytes=DENSE_VMEM),
            name='dense',
        )(n1, attn, dq, dk, dv, dh.reshape(rows), dg1_in, sums, y_in, dx_in)
        return (y_next[None, None], dx_prev[None, None], dg1, dg2, jnp.transpose(dwq, (1, 0, 2))[None], dwk[None, :, None],
                dwv[None, :, None], dwo.reshape(w_o.shape), jnp.transpose(dwr)[None], dw1[None], dw3[None], dw2[None])

    tok_spec = P(('dp', 'pp'), 'ep', None, None)
    cnt_spec = P(('dp', 'pp'), 'ep', None)
    gain_spec = P('pp', None)
    attn_spec = P('pp', None, None, None)
    router_spec = P('pp', None, None)
    expert_spec = P('pp', 'ep', None, None)
    gain_out = P(('dp', 'pp'), None)
    attn_out_spec = P(('dp', 'pp'), None, None, None)
    router_out = P(('dp', 'pp'), None, None)
    expert_out_spec = P(('dp', 'pp'), 'ep', None, None)
    in_specs = (tok_spec, tok_spec, tok_spec, tok_spec, tok_spec, cnt_spec, cnt_spec, gain_spec, gain_spec,
                attn_spec, attn_spec, attn_spec, attn_spec, router_spec, expert_spec, expert_spec, expert_spec)
    out_specs = (tok_spec, tok_spec, gain_out, gain_out, attn_out_spec, attn_out_spec, attn_out_spec, attn_out_spec,
                 router_out, expert_out_spec, expert_out_spec, expert_out_spec)
    return jax.shard_map(device_tick, mesh=mesh, in_specs=in_specs, out_specs=out_specs, check_vma=False)
```

```python
import functools

import jax
import jax.numpy as jnp
from jax import lax
from jax.experimental import pallas as pl
from jax.experimental.pallas import tpu as pltpu
from jax.sharding import PartitionSpec as P

NORM_EPS = 1e-6
MASK_VALUE = -1e30
F32 = jnp.float32
BF16 = jnp.bfloat16
MESH = pl.DeviceIdType.MESH
VMEM = pltpu.VMEM
FFN_TILE = 256
LANES = 128
ROW_SIZES = (128, 192, 320, 512)
RING = 3
CHUNKS = 4
HEAD_VMEM = 34 * 2 ** 20
MOE_VMEM = 44 * 2 ** 20
TAIL_VMEM = 30 * 2 ** 20
DENSE_VMEM = 24 * 2 ** 20


def dot_nn(lhs, rhs):
    return lax.dot_general(lhs, rhs, (((1,), (0,)), ((), ())), preferred_element_type=F32)


def dot_nt(lhs, rhs):
    return lax.dot_general(lhs, rhs, (((1,), (1,)), ((), ())), preferred_element_type=F32)


def dot_tn(lhs, rhs):
    return lax.dot_general(lhs, rhs, (((0,), (0,)), ((), ())), preferred_element_type=F32)


def ep_peers():
    me = lax.axis_index('ep')
    partner = me + 1 - 2 * lax.rem(me, 2)
    across = lax.rem(me + 2, 4)
    diag = lax.rem(partner + 2, 4)
    return me, partner, across, diag


def greet(peers):
    barrier = pltpu.get_barrier_semaphore()
    for peer in peers:
        pl.semaphore_signal(barrier, inc=1, device_id=peer, device_id_type=MESH)
    pl.semaphore_wait(barrier, len(peers))


def push(src, dst, sems, idx, peer):
    return pltpu.make_async_remote_copy(src_ref=src, dst_ref=dst, send_sem=sems[0].at[idx], recv_sem=sems[1].at[idx],
                                        device_id=peer, device_id_type=MESH)


def stack_heads(wide, heads, head_dim):
    return jnp.concatenate([wide[:, h * head_dim:(h + 1) * head_dim] for h in range(heads)], axis=0)


def unstack_heads(tall, heads, seq_len):
    return jnp.concatenate([tall[h * seq_len:(h + 1) * seq_len] for h in range(heads)], axis=1)


def rms_inv(x_f32):
    return lax.rsqrt(jnp.mean(x_f32 * x_f32, axis=-1, keepdims=True) + NORM_EPS)


def attention_rows(x_bf, gain, wq, wk, wv, wo, n_seq, heads):
    seq_len, head_dim = x_bf.shape[0] // n_seq, wk.shape[1]
    x_f32 = x_bf.astype(F32)
    normed = (x_f32 * rms_inv(x_f32) * gain).astype(BF16)
    query = dot_nn(normed, wq).astype(BF16)
    key = dot_nn(normed, wk).astype(BF16)
    value = dot_nn(normed, wv).astype(BF16)
    row = lax.rem(lax.broadcasted_iota(jnp.int32, (heads * seq_len, seq_len), 0), seq_len)
    col = lax.broadcasted_iota(jnp.int32, (heads * seq_len, seq_len), 1)
    causal = row >= col
    outs, probs_all = [], []
    for s in range(n_seq):
        rows = slice(s * seq_len, (s + 1) * seq_len)
        scores = dot_nt(stack_heads(query[rows], heads, head_dim), key[rows]) * head_dim ** -0.5
        scores = jnp.where(causal, scores, MASK_VALUE)
        expd = jnp.exp(scores - jnp.max(scores, axis=-1, keepdims=True))
        probs = expd / jnp.sum(expd, axis=-1, keepdims=True)
        probs_all.append(probs)
        outs.append(unstack_heads(dot_nn(probs.astype(BF16), value[rows]).astype(BF16), heads, seq_len))
    attn = jnp.concatenate(outs, axis=0)
    hidden = (x_f32 + dot_nn(attn, wo)).astype(BF16)
    return hidden, (normed, query, key, value, probs_all, attn)


def route_rows(hidden, gain, wr, cols, counts, base, n_seq):
    seq_len = hidden.shape[0] // n_seq
    h_f32 = hidden.astype(F32)
    normed = (h_f32 * rms_inv(h_f32) * gain).astype(BF16)
    logits = dot_nn(normed, wr)
    lane = lax.broadcasted_iota(jnp.int32, (seq_len, LANES), 1).astype(F32)
    lower = (lax.broadcasted_iota(jnp.int32, (seq_len, seq_len), 0)
             > lax.broadcasted_iota(jnp.int32, (seq_len, seq_len), 1)).astype(F32).astype(BF16)
    weights, masks, routes = [], [], []
    for s in range(n_seq):
        id0, id1 = cols[s][base], cols[s][base + 1]
        hot0, hot1 = (lane == id0).astype(F32), (lane == id1).astype(F32)
        rank = dot_nn(lower, (hot0 + hot1).astype(BF16))
        rank1 = rank + (id0 == id1).astype(F32)
        kept0 = hot0 * (rank < counts[s]).astype(F32)
        kept1 = hot1 * (rank1 < counts[s]).astype(F32)
        part = logits[s * seq_len:(s + 1) * seq_len]
        sel0 = jnp.sum(jnp.where(hot0 > 0, part, 0.0), axis=-1, keepdims=True)
        sel1 = jnp.sum(jnp.where(hot1 > 0, part, 0.0), axis=-1, keepdims=True)
        top = jnp.maximum(sel0, sel1)
        exp0, exp1 = jnp.exp(sel0 - top), jnp.exp(sel1 - top)
        gate0, gate1 = exp0 / (exp0 + exp1), exp1 / (exp0 + exp1)
        weights.append(kept0 * gate0 + kept1 * gate1)
        masks.append(jnp.maximum(kept0, kept1))
        keep0 = jnp.sum(kept0, axis=-1, keepdims=True)
        keep1 = jnp.sum(kept1, axis=-1, keepdims=True)
        route = jnp.zeros((seq_len, LANES), F32)
        for i, item in enumerate((id0, id1, gate0, gate1, keep0, keep1)):
            route = jnp.where(lane == i, item, route)
        routes.append(route)
    return normed, jnp.concatenate(weights, 0), jnp.concatenate(masks, 0), jnp.concatenate(routes, 0)


def head_kernel(n_ep, heads, ida_hbm, idb_hbm, cta_hbm, ctb_hbm, xa_hbm, xb_hbm, gb_hbm, gain1_hbm, gain2_hbm, wq_hbm, wk_hbm,
                wv_hbm, wo_hbm, wr_hbm,
                xb_all, gb_all, n2a_ref, n2b_ref, wta_ref, ma_ref, wtb_ref, mb_ref, rtb_ref, ha_ref, hb_ref,
                n1_ref, q_ref, k_ref, v_ref, p_ref, o_ref,
                xa_all, pk_ref, pk_all, ida_ref, idb_ref, cta_ref, ctb_ref, gain1_ref, gain2_ref, wq_s, wk_ref, wv_ref, wo_ref,
                wr_ref, wr_s, load_sem, send_sem, recv_sem):
    me, partner, across, diag = ep_peers()
    sems = (send_sem, recv_sem)
    seq_len = xb_all.shape[1]
    moves = [(ida_hbm, ida_ref), (idb_hbm, idb_ref), (cta_hbm, cta_ref), (ctb_hbm, ctb_ref), (xb_hbm, xb_all.at[me]),
             (xa_hbm, xa_all.at[me]), (gb_hbm, gb_all.at[me]), (gain1_hbm, gain1_ref), (gain2_hbm, gain2_ref)]
    moves += [(wq_hbm.at[h], wq_s.at[:, pl.ds(h * LANES, LANES)]) for h in range(heads)]
    moves += [(wk_hbm, wk_ref), (wv_hbm, wv_ref), (wo_hbm, wo_ref), (wr_hbm, wr_ref)]
    loads = [pltpu.make_async_copy(src, dst, load_sem.at[i]) for i, (src, dst) in enumerate(moves)]
    for load in loads:
        load.start()
    greet(({'ep': partner}, {'ep': across}))
    landing = (pk_all, xb_all, xa_all, gb_all)
    far, near, relay = [], [], []
    for i in range(4):
        own = pk_ref if i == 0 else landing[i].at[me]
        far.append(push(own, landing[i].at[me], sems, 3 * i, {'ep': across}))
        near.append(push(own, landing[i].at[me], sems, 3 * i + 1, {'ep': partner}))
        relay.append(push(landing[i].at[across], landing[i].at[across], sems, 3 * i + 2, {'ep': partner}))

    def leave(i):
        far[i].start()
        near[i].start()

    for load in loads[0:4]:
        load.wait()
    pk_ref[...] = jnp.zeros_like(pk_ref)
    pk_ref[0:2, :] = ida_ref[...]
    pk_ref[2:4, :] = idb_ref[...]
    pk_ref[4:5, 0:cta_ref.shape[1]] = cta_ref[...]
    pk_ref[5:6, 0:ctb_ref.shape[1]] = ctb_ref[...]
    pk_all[me] = pk_ref[...]
    loads[4].wait()
    leave(1)
    leave(0)
    loads[5].wait()
    leave(2)
    loads[6].wait()
    leave(3)
    for load in loads[7:]:
        load.wait()
    wr_s[...] = jnp.zeros_like(wr_s)
    wr_s[0:wr_ref.shape[0], :] = wr_ref[...]
    wr = wr_s[...].T
    gain1, gain2 = gain1_ref[...].astype(F32), gain2_ref[...].astype(F32)

    def pair_b(pair):
        x_pair = jnp.concatenate([xb_all[s] for s in pair], axis=0)
        hidden, (normed, query, key, value, probs, attn) = attention_rows(
            x_pair, gain1, wq_s[...], wk_ref[...], wv_ref[...], wo_ref[...], len(pair), heads)
        cols, counts = routing_of(pair)
        routed = route_rows(hidden, gain2, wr, cols, [c[1] for c in counts], 2, len(pair))
        for n, s in enumerate(pair):
            rows, part = pl.ds(pl.multiple_of(s * seq_len, seq_len), seq_len), slice(n * seq_len, (n + 1) * seq_len)
            n1_ref[rows, :], q_ref[rows, :], k_ref[rows, :] = normed[part], query[part], key[part]
            v_ref[rows, :], o_ref[rows, :], hb_ref[rows, :] = value[part], attn[part], hidden[part]
            p_ref[s] = probs[n]
            n2b_ref[rows, :], wtb_ref[rows, :], mb_ref[rows, :], rtb_ref[rows, :] = [item[part] for item in routed]

    def pair_a(pair):
        x_pair = jnp.concatenate([xa_all[s] for s in pair], axis=0)
        hidden, _ = attention_rows(x_pair, gain1, wq_s[...], wk_ref[...], wv_ref[...], wo_ref[...], len(pair), heads)
        cols, counts = routing_of(pair)
        routed = route_rows(hidden, gain2, wr, cols, [c[0] for c in counts], 0, len(pair))
        for n, s in enumerate(pair):
            rows, part = pl.ds(pl.multiple_of(s * seq_len, seq_len), seq_len), slice(n * seq_len, (n + 1) * seq_len)
            ha_ref[rows, :] = hidden[part]
            n2a_ref[rows, :], wta_ref[rows, :], ma_ref[rows, :] = [item[part] for item in routed[:3]]

    def routing_of(pair):
        packed = [pk_all[s].astype(F32) for s in pair]
        flat = jnp.concatenate(packed + [jnp.zeros((LANES - 8 * len(pair), LANES), F32)], axis=0).T
        cols = [[flat[:, 8 * n + r:8 * n + r + 1] for r in range(4)] for n in range(len(pair))]
        return cols, [(item[4:5, :], item[5:6, :]) for item in packed]

    near[0].wait_recv()
    near[1].wait_recv()
    pair_b((me, partner))
    far[0].wait_recv()
    relay[0].start()
    far[1].wait_recv()
    relay[1].start()
    near[2].wait_recv()
    pair_a((me, partner))
    relay[0].wait_recv()
    relay[1].wait_recv()
    far[2].wait_recv()
    relay[2].start()
    pair_b((across, diag))
    relay[2].wait_recv()
    far[3].wait_recv()
    relay[3].start()
    pair_a((across, diag))
    near[3].wait_recv()
    relay[3].wait_recv()
    for i in range(4):
        far[i].wait_send()
        near[i].wait_send()
        relay[i].wait_send()


def moe_kernel(e_local, n2a_ref, n2b_ref, g_ref, wta_ref, ma_ref, wtb_ref, mb_ref, w1_hbm, w3_hbm, w2_hbm,
               ra_ref, rb_ref, rd_ref, dw1_ref, dw3_ref, dw2_ref, x_a, x_b, xbt, dexp, acc_a, acc_b, dacc, put_a, put_b, wcol, dots, ring_1, ring_3, ring_2,
               w1_all, w3_all, w2_all, ring_sem, load_sem, blocks):
    expert, tile = pl.program_id(0), pl.program_id(1)
    n_tile = pl.num_programs(1)
    step = expert * n_tile + tile
    slot = lax.rem(step, RING)

    def leaving(step, slot):
        expert, start = step // n_tile, pl.multiple_of(lax.rem(step, n_tile) * FFN_TILE, FFN_TILE)
        span = pl.ds(start, FFN_TILE)
        return [pltpu.make_async_copy(ring_1.at[slot], dw1_ref.at[expert, :, span], ring_sem.at[slot, 0]),
                pltpu.make_async_copy(ring_3.at[slot], dw3_ref.at[expert, :, span], ring_sem.at[slot, 1]),
                pltpu.make_async_copy(ring_2.at[slot], dw2_ref.at[expert, span, :], ring_sem.at[slot, 2])]

    def coming(step, slot):
        expert, start = step // n_tile, pl.multiple_of(lax.rem(step, n_tile) * FFN_TILE, FFN_TILE)
        span = pl.ds(start, FFN_TILE)
        return [pltpu.make_async_copy(w1_hbm.at[expert, :, span], w1_all.at[slot], load_sem.at[slot, 0]),
                pltpu.make_async_copy(w3_hbm.at[expert, :, span], w3_all.at[slot], load_sem.at[slot, 1]),
                pltpu.make_async_copy(w2_hbm.at[expert, span, :], w2_all.at[slot], load_sem.at[slot, 2])]

    @pl.when(step == 0)
    def _():
        for ahead in range(RING):
            for copy in coming(ahead, ahead):
                copy.start()

    n_tok, d_model = n2a_ref.shape
    here = lax.axis_index('ep') * e_local + expert

    def by_rows(which, work):
        for rows in ROW_SIZES:
            pl.when(blocks[which] == rows)(functools.partial(work, rows))

    @pl.when(tile == 0)
    def _():
        mine = lax.broadcasted_iota(jnp.int32, (n_tok, LANES), 1) == here
        mine_t = lax.broadcasted_iota(jnp.int32, (LANES, n_tok), 0) == here
        lower = (lax.broadcasted_iota(jnp.int32, (n_tok, n_tok), 0)
                 > lax.broadcasted_iota(jnp.int32, (n_tok, n_tok), 1)).astype(F32).astype(BF16)
        slot_col = lax.broadcasted_iota(jnp.int32, (n_tok, n_tok), 1).astype(F32)
        slot_row = lax.broadcasted_iota(jnp.int32, (n_tok, n_tok), 0).astype(F32)

        def plan(which, mask_ref, put):
            mask = mask_ref[...]
            place = jnp.where(mask > 0, dot_nn(lower, mask.astype(BF16)), -1.0)
            place_col = jnp.sum(jnp.where(mine, place, 0.0), axis=-1, keepdims=True)
            place_row = jnp.sum(jnp.where(mine_t, place.T, 0.0), axis=0, keepdims=True)
            put[...] = (slot_col == place_col).astype(F32).astype(BF16)
            total = jnp.sum(jnp.where(mine, mask, 0.0)).astype(jnp.int32)
            size = jnp.int32(n_tok)
            for rows in ROW_SIZES[-2::-1]:
                size = jnp.where(total <= rows, rows, size)
            blocks[which] = size
            return (slot_row == place_row).astype(F32).astype(BF16)

        take_a, take_b = plan(0, ma_ref, put_a), plan(1, mb_ref, put_b)
        wcol[...] = jnp.broadcast_to(jnp.sum(jnp.where(mine, wta_ref[...], 0.0), axis=-1, keepdims=True), (n_tok, LANES))
        wt_b = jnp.sum(jnp.where(mine, wtb_ref[...], 0.0), axis=-1, keepdims=True)
        scaled = (wt_b * g_ref[...].astype(F32)).astype(BF16)

        def fetch_a(rows):
            x_a[0:rows, :] = dot_nn(take_a[0:rows], n2a_ref[...]).astype(BF16)
            acc_a[0:rows, :] = jnp.zeros((rows, d_model), F32)

        def fetch_b(rows):
            fetched = dot_nn(take_b[0:rows], n2b_ref[...])
            x_b[0:rows, :] = fetched.astype(BF16)
            xbt[:, 0:rows] = fetched.T.astype(BF16)
            dexp[0:rows, :] = dot_nn(take_b[0:rows], scaled).astype(BF16)
            acc_b[0:rows, :] = jnp.zeros((rows, d_model), F32)
            dacc[0:rows, :] = jnp.zeros((rows, d_model), F32)

        by_rows(0, fetch_a)
        by_rows(1, fetch_b)

    @pl.when((tile == 0) & (expert == 0))
    def _():
        ra_ref[...] = jnp.zeros_like(ra_ref)
        rb_ref[...] = jnp.zeros_like(rb_ref)
        dots[...] = jnp.zeros_like(dots)

    for copy in coming(step, slot):
        copy.wait()

    @pl.when(step >= RING)
    def _():
        for copy in leaving(step - RING, slot):
            copy.wait()

    w1_ref, w3_ref, w2_ref = w1_all.at[slot], w3_all.at[slot], w2_all.at[slot]

    def forward(x, rows):
        gate_pre, up_pre = dot_nn(x[0:rows, :], w1_ref[...]), dot_nn(x[0:rows, :], w3_ref[...])
        sig = jax.nn.sigmoid(gate_pre)
        return gate_pre, up_pre, sig, (gate_pre * sig * up_pre).astype(BF16)

    def run_a(rows):
        act = forward(x_a, rows)[3]
        acc_a[0:rows, :] += dot_nn(act, w2_ref[...])

    def run_b(rows):
        gate_pre, up_pre, sig, act = forward(x_b, rows)
        acc_b[0:rows, :] += dot_nn(act, w2_ref[...])
        d_exp = dexp[0:rows, :]
        d_act = dot_nt(d_exp, w2_ref[...]).astype(BF16).astype(F32)
        d_up = (d_act * gate_pre * sig).astype(BF16)
        d_gate = (d_act * up_pre * sig * (1.0 + gate_pre * (1.0 - sig))).astype(BF16)
        ring_1[slot] = dot_nn(xbt[:, 0:rows], d_gate)
        ring_3[slot] = dot_nn(xbt[:, 0:rows], d_up)
        ring_2[slot] = dot_tn(act, d_exp)
        dacc[0:rows, :] += dot_nt(d_gate, w1_ref[...]) + dot_nt(d_up, w3_ref[...])

    by_rows(1, run_b)
    for copy in leaving(step, slot):
        copy.start()
    by_rows(0, run_a)

    @pl.when(step + RING < pl.num_programs(0) * n_tile)
    def _():
        for copy in coming(step + RING, slot):
            copy.start()

    def return_a(rows):
        ra_ref[...] += wcol[:, 0:1] * dot_nn(put_a[:, 0:rows], acc_a[0:rows, :].astype(BF16))

    def return_b(rows):
        put = put_b[:, 0:rows]
        rb_ref[...] += dot_nn(put, dacc[0:rows, :].astype(BF16))
        out_b = dot_nn(put, acc_b[0:rows, :].astype(BF16))
        pick = jnp.sum(out_b * g_ref[...].astype(F32), axis=-1, keepdims=True)
        lane = lax.broadcasted_iota(jnp.int32, (n_tok, LANES), 1)
        dots[...] += jnp.where(lane == here, pick, 0.0)

    @pl.when(tile == pl.num_programs(1) - 1)
    def _():
        by_rows(0, return_a)
        by_rows(1, return_b)

    @pl.when(step == pl.num_programs(0) * n_tile - 1)
    def _():
        flat = dots[...].T
        n_src, n_exp, seq_len = rd_ref.shape
        for src in range(n_src):
            rd_ref[src] = flat[0:n_exp, src * seq_len:(src + 1) * seq_len]
        for back in range(RING - 1, -1, -1):
            for copy in leaving(step - back, lax.rem(step - back, RING)):
                copy.wait()


def tail_kernel(n_ep, n_pp, heads, ra_ref, rb_ref, rd_ref, ha_ref, hb_ref, n2b_ref, gb_ref, rtb_ref, x_ref, q_ref, k_ref, v_ref,
                p_ref, gain1_ref, gain2_ref, wq_ref, wk_ref, wv_ref, wo_ref, wr_ref,
                y_ref, dx_ref, dq_ref, dk_ref, dv_ref, dh_all, dg1_ref, sums_ref,
                near_b, swap_b, sum_b, far_b, near_a, swap_a, sum_a, far_a, near_d, swap_d, sum_d, far_d, small, small_1, small_2, small_3,
                y_own, dx_own, wq_s, wr_s, send_sem, recv_sem):
    me, partner, across, diag = ep_peers()
    stage = lax.axis_index('pp')
    later, earlier = lax.rem(stage + 1, n_pp), lax.rem(stage + n_pp - 1, n_pp)
    seq_len, d_model = y_ref.shape
    sems = (send_sem, recv_sem)
    near, over = {'ep': partner}, {'ep': across}
    greet((near, over, {'pp': later}, {'pp': earlier}))
    span = seq_len // CHUNKS
    parts = [pl.ds(c * span, span) for c in range(CHUNKS)]

    def chunked(src, dst, base, peer):
        return [push(src.at[part], dst.at[part], sems, base + c, peer) for c, part in enumerate(parts)]

    swap_b_c = chunked(rb_ref.at[diag], swap_b, 13, near)
    swap_a_c = chunked(ra_ref.at[diag], swap_a, 13 + CHUNKS, near)
    far_b_c = chunked(sum_b, far_b, 13 + 2 * CHUNKS, over)
    far_a_c = chunked(sum_a, far_a, 13 + 3 * CHUNKS, over)
    y_c = chunked(y_own, y_ref, 13 + 4 * CHUNKS, {'pp': later})
    swap_d_c = push(rd_ref.at[diag], swap_d, sems, 0, near)
    near_b_c = push(rb_ref.at[partner], near_b, sems, 1, near)
    near_d_c = push(rd_ref.at[partner], near_d, sems, 2, near)
    near_a_c = push(ra_ref.at[partner], near_a, sems, 3, near)
    far_d_c = push(sum_d, far_d, sems, 4, over)
    swap_d_c.start()
    for copy in swap_b_c:
        copy.start()
    for copy in (near_d_c, near_b_c, *swap_a_c, near_a_c):
        copy.start()
    swap_d_c.wait_recv()
    sum_d[...] = rd_ref[across] + swap_d[...]
    for c, part in enumerate(parts):
        swap_b_c[c].wait_recv()
        sum_b[part, :] = rb_ref[across, part, :] + swap_b[part, :]
        far_b_c[c].start()
        if c == 0:
            far_d_c.start()
    for c, part in enumerate(parts):
        swap_a_c[c].wait_recv()
        sum_a[part, :] = ra_ref[across, part, :] + swap_a[part, :]
        if c == 0:
            far_a_c[c].start()
    for h in range(heads):
        wq_s[:, h * LANES:(h + 1) * LANES] = wq_ref[h]
    wr_s[...] = jnp.zeros_like(wr_s)
    wr_s[0:wr_ref.shape[0], :] = wr_ref[...]

    gain1, gain2 = gain1_ref[...].astype(F32), gain2_ref[...].astype(F32)
    mine = pl.ds(pl.multiple_of(me * seq_len, seq_len), seq_len)
    route = rtb_ref[mine, :]
    id0, id1, gate0, gate1, keep0, keep1 = [route[:, i:i + 1] for i in range(6)]
    lane = lax.broadcasted_iota(jnp.int32, (seq_len, LANES), 1).astype(F32)
    hot0, hot1 = (lane == id0).astype(F32), (lane == id1).astype(F32)
    h_f32 = hb_ref[mine, :].astype(F32)
    inv = rms_inv(h_f32)
    h_hat = h_f32 * inv
    near_d_c.wait_recv()
    far_d_c.wait_recv()
    tile = rd_ref[me] + near_d[...] + far_d[...]
    dots = jnp.concatenate([tile, jnp.zeros((LANES - tile.shape[0], seq_len), F32)], axis=0).T
    d_gate0 = jnp.where(keep0 > 0, jnp.sum(hot0 * dots, axis=-1, keepdims=True), 0.0)
    d_gate1 = jnp.where(keep1 > 0, jnp.sum(hot1 * dots, axis=-1, keepdims=True), 0.0)
    mean_gate = gate0 * d_gate0 + gate1 * d_gate1
    d_logits = (hot0 * (gate0 * (d_gate0 - mean_gate)) + hot1 * (gate1 * (d_gate1 - mean_gate))).astype(BF16)
    d_routed = dot_nn(d_logits, wr_s[...])
    near_b_c.wait_recv()
    for copy in far_b_c:
        copy.wait_recv()
    d_normed = (rb_ref[me] + near_b[...] + far_b[...]) + d_routed
    d_hat = d_normed * gain2
    d_in = inv * (d_hat - h_hat * jnp.mean(d_hat * h_hat, axis=-1, keepdims=True))
    dh_all[me] = (d_in + gb_ref[me].astype(F32)).astype(BF16)
    dh_far = push(dh_all.at[me], dh_all.at[me], sems, 6, over)
    dh_near = push(dh_all.at[me], dh_all.at[me], sems, 7, near)
    dh_relay = push(dh_all.at[across], dh_all.at[across], sems, 8, near)
    dh_far.start()
    dh_near.start()
    for copy in far_a_c[1:]:
        copy.start()
    small[0:8, :] = dot_tn(d_logits, n2b_ref[mine, :])[0:8, :]
    small[8:16, :] = jnp.broadcast_to(jnp.sum(d_normed * h_hat, axis=0, keepdims=True), (8, d_model))
    small_near = push(small, small_1, sems, 9, near)
    small_near.start()

    head_dim = wk_ref.shape[1]

    def attention_back(s):
        rows = pl.ds(pl.multiple_of(s * seq_len, seq_len), seq_len)
        d_hid = dh_all[s]
        d_out = stack_heads(dot_nt(d_hid, wo_ref[...]).astype(BF16), heads, head_dim)
        probs = p_ref[s]
        d_probs = dot_nt(d_out, v_ref[rows, :])
        d_v = dot_tn(probs.astype(BF16), d_out).astype(BF16)
        d_scores = (probs * (d_probs - jnp.sum(probs * d_probs, axis=-1, keepdims=True)) * head_dim ** -0.5).astype(BF16)
        d_q = unstack_heads(dot_nn(d_scores, k_ref[rows, :]).astype(BF16), heads, seq_len)
        d_k = dot_tn(d_scores, stack_heads(q_ref[rows, :], heads, head_dim)).astype(BF16)
        dq_ref[rows, :], dk_ref[rows, :], dv_ref[rows, :] = d_q, d_k, d_v
        d_norm1 = dot_nt(d_q, wq_s[...]) + dot_nt(d_k, wk_ref[...]) + dot_nt(d_v, wv_ref[...])
        x_f32 = x_ref[s].astype(F32)
        inv1 = rms_inv(x_f32)
        x_hat = x_f32 * inv1
        dg1_ref[s] = jnp.broadcast_to(jnp.sum(d_norm1 * x_hat, axis=0, keepdims=True), (8, d_model))
        return d_hid, d_norm1, inv1, x_hat

    d_hid, d_norm1, inv1, x_hat = attention_back(me)
    d_hat1 = d_norm1 * gain1
    d_x = inv1 * (d_hat1 - x_hat * jnp.mean(d_hat1 * x_hat, axis=-1, keepdims=True)) + d_hid.astype(F32)
    dx_own[...] = d_x.astype(BF16)
    dx_c = push(dx_own, dx_ref, sems, 11, {'pp': earlier})
    dx_c.start()
    small_near.wait_recv()
    small_2[...] = small[...] + small_1[...]
    small_far = push(small_2, small_3, sems, 10, over)
    small_far.start()
    near_a_c.wait_recv()

    def leave_y(c):
        part = parts[c]
        far_a_c[c].wait_recv()
        own = pl.ds(pl.multiple_of(me * seq_len + c * span, span), span)
        y_own[part, :] = (ha_ref[own, :].astype(F32)
                          + (ra_ref[me, part, :] + near_a[part, :] + far_a[part, :])).astype(BF16)
        y_c[c].start()

    leave_y(0)
    dh_near.wait_recv()
    attention_back(partner)
    dh_far.wait_recv()
    dh_relay.start()
    leave_y(1)
    attention_back(across)
    leave_y(2)
    dh_relay.wait_recv()
    attention_back(diag)
    leave_y(3)
    small_far.wait_recv()
    sums_ref[...] = small_2[...] + small_3[...]
    dx_c.wait_recv()
    for copy in y_c:
        copy.wait_recv()
    for copy in (*swap_b_c, *swap_a_c, *far_b_c, *far_a_c, *y_c, swap_d_c, near_b_c, near_d_c, near_a_c, far_d_c, dh_far, dh_near,
                 dh_relay, small_near, small_far, dx_c):
        copy.wait_send()


def dense_kernel(n1_ref, o_ref, dq_ref, dk_ref, dv_ref, dh_ref, dg1_in, sums_in, y_in, dx_in,
                 dwq_ref, dwk_ref, dwv_ref, dwo_ref, dg1_ref, dg2_ref, dwr_ref, y_ref, dx_ref, n1t):
    step = pl.program_id(0)

    @pl.when(step == 0)
    def _():
        n1t[...] = n1_ref[...].astype(F32).T.astype(BF16)
        dwk_ref[...] = dot_nn(n1t[...], dk_ref[...])
        dwv_ref[...] = dot_nn(n1t[...], dv_ref[...])
        dg1_ref[...] = sum(dg1_in[s] for s in range(dg1_in.shape[0]))[0:1]
        dwr_ref[...] = sums_in[0:8, :]
        dg2_ref[...] = sums_in[8:9, :]
        y_ref[...] = y_in[...]
        dx_ref[...] = dx_in[...]

    pair = dot_nn(n1t[...], dq_ref[...])
    for i in range(dwq_ref.shape[0]):
        dwq_ref[i] = pair[:, i * LANES:(i + 1) * LANES]
    dwo_ref[...] = dot_tn(o_ref[...], dh_ref[...])


def shape_of(shape, dtype):
    return jax.ShapeDtypeStruct(shape, dtype)


def solution(mesh):
    n_ep, n_pp = mesh.shape['ep'], mesh.shape['pp']
    whole = pl.BlockSpec(memory_space=VMEM)

    def device_tick(x_a, x_b, g_b, ids_a, ids_b, count_a, count_b, gain_1, gain_2, w_q, w_k, w_v, w_o, w_r, w_1, w_3, w_2):
        seq_len, d_model = x_a.shape[2], x_a.shape[3]
        heads, head_dim = w_q.shape[2], w_q.shape[3]
        n_exp, e_local, ffn = w_r.shape[2], w_1.shape[1], w_1.shape[3]
        n_tok = n_ep * seq_len
        width = heads * head_dim
        xa, xb, gb = x_a[0, 0], x_b[0, 0], g_b[0, 0]
        wq = jnp.transpose(w_q[0], (1, 0, 2))
        wk, wv, wo = w_k[0, :, 0], w_v[0, :, 0], w_o[0].reshape(width, d_model)
        wr = jnp.transpose(w_r[0])
        tok, rows = (n_ep, seq_len, d_model), (n_tok, d_model)
        head_out = [shape_of(tok, BF16), shape_of(tok, BF16), shape_of(rows, BF16), shape_of(rows, BF16),
                    shape_of((n_tok, LANES), F32), shape_of((n_tok, LANES), F32), shape_of((n_tok, LANES), F32),
                    shape_of((n_tok, LANES), F32), shape_of((n_tok, LANES), F32), shape_of(rows, BF16), shape_of(rows, BF16),
                    shape_of(rows, BF16), shape_of((n_tok, width), BF16), shape_of((n_tok, head_dim), BF16),
                    shape_of((n_tok, head_dim), BF16), shape_of((n_ep, heads * seq_len, seq_len), F32),
                    shape_of((n_tok, width), BF16)]
        (xb_all, gb_all, n2a, n2b, wta, m_a, wtb, m_b, rtb, ha, hb, n1, q, k, v, probs, attn) = pl.pallas_call(
            functools.partial(head_kernel, n_ep, heads),
            out_shape=head_out,
            in_specs=[pl.BlockSpec(memory_space=pltpu.HBM)] * 14,
            out_specs=[whole] * len(head_out),
            scratch_shapes=[VMEM(tok, BF16), VMEM((8, LANES), jnp.int32), VMEM((n_ep, 8, LANES), jnp.int32),
                            VMEM((2, seq_len), jnp.int32), VMEM((2, seq_len), jnp.int32), VMEM((1, n_exp), jnp.int32),
                            VMEM((1, n_exp), jnp.int32), VMEM((1, d_model), BF16), VMEM((1, d_model), BF16),
                            VMEM((d_model, width), BF16), VMEM((d_model, head_dim), BF16), VMEM((d_model, head_dim), BF16),
                            VMEM((width, d_model), BF16), VMEM((n_exp, d_model), BF16), VMEM((LANES, d_model), BF16),
                            pltpu.SemaphoreType.DMA((13 + heads,)), pltpu.SemaphoreType.DMA((12,)),
                            pltpu.SemaphoreType.DMA((12,))],
            compiler_params=pltpu.CompilerParams(collective_id=0, has_side_effects=True, vmem_limit_bytes=HEAD_VMEM),
            name='head',
        )(*[pltpu.with_memory_space_constraint(arg, pltpu.HBM) for arg in (
            ids_a[0, 0].T, ids_b[0, 0].T, count_a[0], count_b[0], xa, xb, gb, gain_1, gain_2, wq, wk, wv, wo, wr)])

        n_tile = ffn // FFN_TILE

        def const(*shape):
            return pl.BlockSpec(shape, lambda e, f: (0,) * len(shape))
        hbm = pl.BlockSpec(memory_space=pltpu.HBM)
        r_a, r_b, r_d, dw1, dw3, dw2 = pl.pallas_call(
            functools.partial(moe_kernel, e_local),
            grid=(e_local, n_tile),
            out_shape=[shape_of(rows, F32), shape_of(rows, F32), shape_of((n_ep, n_exp, seq_len), F32), shape_of((e_local, d_model, ffn), F32),
                       shape_of((e_local, d_model, ffn), F32), shape_of((e_local, ffn, d_model), F32)],
            in_specs=[const(*rows)] * 3 + [const(n_tok, LANES)] * 4 + [hbm] * 3,
            out_specs=[const(*rows), const(*rows), const(n_ep, n_exp, seq_len), hbm, hbm, hbm],
            scratch_shapes=[VMEM(rows, BF16), VMEM(rows, BF16), VMEM((d_model, n_tok), BF16), VMEM(rows, BF16),
                            VMEM(rows, F32), VMEM(rows, F32), VMEM(rows, F32), VMEM((n_tok, n_tok), BF16),
                            VMEM((n_tok, n_tok), BF16), VMEM((n_tok, LANES), F32), VMEM((n_tok, LANES), F32), VMEM((RING, d_model, FFN_TILE), F32),
                            VMEM((RING, d_model, FFN_TILE), F32), VMEM((RING, FFN_TILE, d_model), F32),
                            VMEM((RING, d_model, FFN_TILE), BF16), VMEM((RING, d_model, FFN_TILE), BF16),
                            VMEM((RING, FFN_TILE, d_model), BF16), pltpu.SemaphoreType.DMA((RING, 3)),
                            pltpu.SemaphoreType.DMA((RING, 3)), pltpu.SMEM((2,), jnp.int32)],
            compiler_params=pltpu.CompilerParams(dimension_semantics=('arbitrary', 'arbitrary'),
                                                 vmem_limit_bytes=MOE_VMEM),
            name='moe',
        )(n2a, n2b, gb_all.reshape(rows), wta, m_a, wtb, m_b, w_1[0], w_3[0], w_2[0])

        small = (16, d_model)
        block = (seq_len, d_model)
        y_in, dx_in, dq, dk, dv, dh, dg1_in, sums = pl.pallas_call(
            functools.partial(tail_kernel, n_ep, n_pp, heads),
            out_shape=[shape_of(block, BF16), shape_of(block, BF16), shape_of((n_tok, width), BF16),
                       shape_of((n_tok, head_dim), BF16), shape_of((n_tok, head_dim), BF16), shape_of(tok, BF16),
                       shape_of((n_ep, 8, d_model), F32), shape_of(small, F32)],
            in_specs=[whole] * 20,
            out_specs=[whole] * 8,
            scratch_shapes=[VMEM(block, F32)] * 8 + [VMEM((n_exp, seq_len), F32)] * 4 + [VMEM(small, F32)] * 4
            + [VMEM(block, BF16), VMEM(block, BF16), VMEM((d_model, width), BF16), VMEM((LANES, d_model), BF16),
               pltpu.SemaphoreType.DMA((13 + 5 * CHUNKS,)), pltpu.SemaphoreType.DMA((13 + 5 * CHUNKS,))],
            compiler_params=pltpu.CompilerParams(collective_id=1, has_side_effects=True, vmem_limit_bytes=TAIL_VMEM),
            name='tail',
        )(r_a.reshape(tok), r_b.reshape(tok), r_d, ha, hb, n2b, gb_all, rtb, xb_all, q, k, v, probs,
          gain_1, gain_2, wq, wk, wv, wo, wr)

        pair = 2
        steps = heads // pair

        def held(*shape):
            return pl.BlockSpec(shape, lambda i: (0,) * len(shape))
        cols = pl.BlockSpec((n_tok, pair * head_dim), lambda i: (0, i))
        dwq, dwk, dwv, dwo, dg1, dg2, dwr, y_next, dx_prev = pl.pallas_call(
            dense_kernel,
            grid=(steps,),
            out_shape=[shape_of((heads, d_model, head_dim), F32), shape_of((d_model, head_dim), F32),
                       shape_of((d_model, head_dim), F32), shape_of((width, d_model), F32), shape_of((1, d_model), F32),
                       shape_of((1, d_model), F32), shape_of((n_exp, d_model), F32), shape_of(block, BF16), shape_of(block, BF16)],
            in_specs=[held(*rows), cols, cols, held(n_tok, head_dim), held(n_tok, head_dim), held(*rows),
                      held(n_ep, 8, d_model), held(*small), held(*block), held(*block)],
            out_specs=[pl.BlockSpec((pair, d_model, head_dim), lambda i: (i, 0, 0)), held(d_model, head_dim),
                       held(d_model, head_dim), pl.BlockSpec((pair * head_dim, d_model), lambda i: (i, 0)),
                       held(1, d_model), held(1, d_model), held(n_exp, d_model), held(*block), held(*block)],
            scratch_shapes=[VMEM((d_model, n_tok), BF16)],
            compiler_params=pltpu.CompilerParams(dimension_semantics=('arbitrary',), vmem_limit_bytes=DENSE_VMEM),
            name='dense',
        )(n1, attn, dq, dk, dv, dh.reshape(rows), dg1_in, sums, y_in, dx_in)
        return (y_next[None, None], dx_prev[None, None], dg1, dg2, jnp.transpose(dwq, (1, 0, 2))[None], dwk[None, :, None],
                dwv[None, :, None], dwo.reshape(w_o.shape), jnp.transpose(dwr)[None], dw1[None], dw3[None], dw2[None])

    tok_spec = P(('dp', 'pp'), 'ep', None, None)
    cnt_spec = P(('dp', 'pp'), 'ep', None)
    gain_spec = P('pp', None)
    attn_spec = P('pp', None, None, None)
    router_spec = P('pp', None, None)
    expert_spec = P('pp', 'ep', None, None)
    gain_out = P(('dp', 'pp'), None)
    attn_out_spec = P(('dp', 'pp'), None, None, None)
    router_out = P(('dp', 'pp'), None, None)
    expert_out_spec = P(('dp', 'pp'), 'ep', None, None)
    in_specs = (tok_spec, tok_spec, tok_spec, tok_spec, tok_spec, cnt_spec, cnt_spec, gain_spec, gain_spec,
                attn_spec, attn_spec, attn_spec, attn_spec, router_spec, expert_spec, expert_spec, expert_spec)
    out_specs = (tok_spec, tok_spec, gain_out, gain_out, attn_out_spec, attn_out_spec, attn_out_spec, attn_out_spec,
                 router_out, expert_out_spec, expert_out_spec, expert_out_spec)
    return jax.shard_map(device_tick, mesh=mesh, in_specs=in_specs, out_specs=out_specs, check_vma=False)
```

```python
import functools

import jax
import jax.numpy as jnp
from jax import lax
from jax.experimental import pallas as pl
from jax.experimental.pallas import tpu as pltpu
from jax.sharding import PartitionSpec as P

NORM_EPS = 1e-6
MASK_VALUE = -1e30
F32 = jnp.float32
BF16 = jnp.bfloat16
MESH = pl.DeviceIdType.MESH
VMEM = pltpu.VMEM
FFN_TILE = 512
LANES = 128
ROW_SIZES = (128, 192, 320, 512)
MOVE_SIZES = (192, 512)
RING = 2
CHUNKS = 4
HEAD_VMEM = 34 * 2 ** 20
MOE_VMEM = 44 * 2 ** 20
TAIL_VMEM = 30 * 2 ** 20
DENSE_VMEM = 24 * 2 ** 20


def dot_nn(lhs, rhs):
    return lax.dot_general(lhs, rhs, (((1,), (0,)), ((), ())), preferred_element_type=F32)


def dot_nt(lhs, rhs):
    return lax.dot_general(lhs, rhs, (((1,), (1,)), ((), ())), preferred_element_type=F32)


def dot_tn(lhs, rhs):
    return lax.dot_general(lhs, rhs, (((0,), (0,)), ((), ())), preferred_element_type=F32)


def ep_peers():
    me = lax.axis_index('ep')
    partner = me + 1 - 2 * lax.rem(me, 2)
    across = lax.rem(me + 2, 4)
    diag = lax.rem(partner + 2, 4)
    return me, partner, across, diag


def greet(peers):
    barrier = pltpu.get_barrier_semaphore()
    for peer in peers:
        pl.semaphore_signal(barrier, inc=1, device_id=peer, device_id_type=MESH)
    pl.semaphore_wait(barrier, len(peers))


def push(src, dst, sems, idx, peer):
    return pltpu.make_async_remote_copy(src_ref=src, dst_ref=dst, send_sem=sems[0].at[idx], recv_sem=sems[1].at[idx],
                                        device_id=peer, device_id_type=MESH)


def stack_heads(wide, heads, head_dim):
    return jnp.concatenate([wide[:, h * head_dim:(h + 1) * head_dim] for h in range(heads)], axis=0)


def unstack_heads(tall, heads, seq_len):
    return jnp.concatenate([tall[h * seq_len:(h + 1) * seq_len] for h in range(heads)], axis=1)


def rms_inv(x_f32):
    return lax.rsqrt(jnp.mean(x_f32 * x_f32, axis=-1, keepdims=True) + NORM_EPS)


def attention_rows(x_bf, gain, wq, wk, wv, wo, n_seq, heads):
    seq_len, head_dim = x_bf.shape[0] // n_seq, wk.shape[1]
    x_f32 = x_bf.astype(F32)
    normed = (x_f32 * rms_inv(x_f32) * gain).astype(BF16)
    query = dot_nn(normed, wq).astype(BF16)
    key = dot_nn(normed, wk).astype(BF16)
    value = dot_nn(normed, wv).astype(BF16)
    row = lax.rem(lax.broadcasted_iota(jnp.int32, (heads * seq_len, seq_len), 0), seq_len)
    col = lax.broadcasted_iota(jnp.int32, (heads * seq_len, seq_len), 1)
    causal = row >= col
    outs, probs_all = [], []
    for s in range(n_seq):
        rows = slice(s * seq_len, (s + 1) * seq_len)
        scores = dot_nt(stack_heads(query[rows], heads, head_dim), key[rows]) * head_dim ** -0.5
        scores = jnp.where(causal, scores, MASK_VALUE)
        expd = jnp.exp(scores - jnp.max(scores, axis=-1, keepdims=True))
        probs = expd / jnp.sum(expd, axis=-1, keepdims=True)
        probs_all.append(probs)
        outs.append(unstack_heads(dot_nn(probs.astype(BF16), value[rows]).astype(BF16), heads, seq_len))
    attn = jnp.concatenate(outs, axis=0)
    hidden = (x_f32 + dot_nn(attn, wo)).astype(BF16)
    return hidden, (normed, query, key, value, probs_all, attn)


def route_rows(hidden, gain, wr, cols, counts, base, n_seq):
    seq_len = hidden.shape[0] // n_seq
    h_f32 = hidden.astype(F32)
    normed = (h_f32 * rms_inv(h_f32) * gain).astype(BF16)
    logits = dot_nn(normed, wr)
    lane = lax.broadcasted_iota(jnp.int32, (seq_len, LANES), 1).astype(F32)
    lower = (lax.broadcasted_iota(jnp.int32, (seq_len, seq_len), 0)
             > lax.broadcasted_iota(jnp.int32, (seq_len, seq_len), 1)).astype(F32).astype(BF16)
    weights, masks, routes = [], [], []
    for s in range(n_seq):
        id0, id1 = cols[s][base], cols[s][base + 1]
        hot0, hot1 = (lane == id0).astype(F32), (lane == id1).astype(F32)
        rank = dot_nn(lower, (hot0 + hot1).astype(BF16))
        rank1 = rank + (id0 == id1).astype(F32)
        kept0 = hot0 * (rank < counts[s]).astype(F32)
        kept1 = hot1 * (rank1 < counts[s]).astype(F32)
        part = logits[s * seq_len:(s + 1) * seq_len]
        sel0 = jnp.sum(jnp.where(hot0 > 0, part, 0.0), axis=-1, keepdims=True)
        sel1 = jnp.sum(jnp.where(hot1 > 0, part, 0.0), axis=-1, keepdims=True)
        top = jnp.maximum(sel0, sel1)
        exp0, exp1 = jnp.exp(sel0 - top), jnp.exp(sel1 - top)
        gate0, gate1 = exp0 / (exp0 + exp1), exp1 / (exp0 + exp1)
        weights.append(kept0 * gate0 + kept1 * gate1)
        masks.append(jnp.maximum(kept0, kept1))
        keep0 = jnp.sum(kept0, axis=-1, keepdims=True)
        keep1 = jnp.sum(kept1, axis=-1, keepdims=True)
        route = jnp.zeros((seq_len, LANES), F32)
        for i, item in enumerate((id0, id1, gate0, gate1, keep0, keep1)):
            route = jnp.where(lane == i, item, route)
        routes.append(route)
    return normed, jnp.concatenate(weights, 0), jnp.concatenate(masks, 0), jnp.concatenate(routes, 0)


def head_kernel(n_ep, heads, ida_hbm, idb_hbm, cta_hbm, ctb_hbm, xa_hbm, xb_hbm, gb_hbm, gain1_hbm, gain2_hbm, wq_hbm, wk_hbm,
                wv_hbm, wo_hbm, wr_hbm,
                xb_all, gb_all, n2a_ref, n2b_ref, wta_ref, ma_ref, wtb_ref, mb_ref, rtb_ref, ha_ref, hb_ref,
                n1_ref, q_ref, k_ref, v_ref, p_ref, o_ref,
                xa_all, pk_ref, pk_all, ida_ref, idb_ref, cta_ref, ctb_ref, gain1_ref, gain2_ref, wq_s, wk_ref, wv_ref, wo_ref,
                wr_ref, wr_s, load_sem, send_sem, recv_sem):
    me, partner, across, diag = ep_peers()
    sems = (send_sem, recv_sem)
    seq_len = xb_all.shape[1]
    moves = [(ida_hbm, ida_ref), (idb_hbm, idb_ref), (cta_hbm, cta_ref), (ctb_hbm, ctb_ref), (xb_hbm, xb_all.at[me]),
             (xa_hbm, xa_all.at[me]), (gb_hbm, gb_all.at[me]), (gain1_hbm, gain1_ref), (gain2_hbm, gain2_ref)]
    moves += [(wq_hbm.at[h], wq_s.at[:, pl.ds(h * LANES, LANES)]) for h in range(heads)]
    moves += [(wk_hbm, wk_ref), (wv_hbm, wv_ref), (wo_hbm, wo_ref), (wr_hbm, wr_ref)]
    loads = [pltpu.make_async_copy(src, dst, load_sem.at[i]) for i, (src, dst) in enumerate(moves)]
    for load in loads:
        load.start()
    greet(({'ep': partner}, {'ep': across}))
    landing = (pk_all, xb_all, xa_all, gb_all)
    far, near, relay = [], [], []
    for i in range(4):
        own = pk_ref if i == 0 else landing[i].at[me]
        far.append(push(own, landing[i].at[me], sems, 3 * i, {'ep': across}))
        near.append(push(own, landing[i].at[me], sems, 3 * i + 1, {'ep': partner}))
        relay.append(push(landing[i].at[across], landing[i].at[across], sems, 3 * i + 2, {'ep': partner}))

    def leave(i):
        far[i].start()
        near[i].start()

    for load in loads[0:4]:
        load.wait()
    pk_ref[...] = jnp.zeros_like(pk_ref)
    pk_ref[0:2, :] = ida_ref[...]
    pk_ref[2:4, :] = idb_ref[...]
    pk_ref[4:5, 0:cta_ref.shape[1]] = cta_ref[...]
    pk_ref[5:6, 0:ctb_ref.shape[1]] = ctb_ref[...]
    pk_all[me] = pk_ref[...]
    loads[4].wait()
    leave(1)
    leave(0)
    loads[5].wait()
    leave(2)
    loads[6].wait()
    leave(3)
    for load in loads[7:]:
        load.wait()
    wr_s[...] = jnp.zeros_like(wr_s)
    wr_s[0:wr_ref.shape[0], :] = wr_ref[...]
    wr = wr_s[...].T
    gain1, gain2 = gain1_ref[...].astype(F32), gain2_ref[...].astype(F32)

    def pair_b(pair):
        x_pair = jnp.concatenate([xb_all[s] for s in pair], axis=0)
        hidden, (normed, query, key, value, probs, attn) = attention_rows(
            x_pair, gain1, wq_s[...], wk_ref[...], wv_ref[...], wo_ref[...], len(pair), heads)
        cols, counts = routing_of(pair)
        routed = route_rows(hidden, gain2, wr, cols, [c[1] for c in counts], 2, len(pair))
        for n, s in enumerate(pair):
            rows, part = pl.ds(pl.multiple_of(s * seq_len, seq_len), seq_len), slice(n * seq_len, (n + 1) * seq_len)
            n1_ref[rows, :], q_ref[rows, :], k_ref[rows, :] = normed[part], query[part], key[part]
            v_ref[rows, :], o_ref[rows, :], hb_ref[rows, :] = value[part], attn[part], hidden[part]
            p_ref[s] = probs[n]
            n2b_ref[rows, :], wtb_ref[rows, :], mb_ref[rows, :], rtb_ref[rows, :] = [item[part] for item in routed]

    def pair_a(pair):
        x_pair = jnp.concatenate([xa_all[s] for s in pair], axis=0)
        hidden, _ = attention_rows(x_pair, gain1, wq_s[...], wk_ref[...], wv_ref[...], wo_ref[...], len(pair), heads)
        cols, counts = routing_of(pair)
        routed = route_rows(hidden, gain2, wr, cols, [c[0] for c in counts], 0, len(pair))
        for n, s in enumerate(pair):
            rows, part = pl.ds(pl.multiple_of(s * seq_len, seq_len), seq_len), slice(n * seq_len, (n + 1) * seq_len)
            ha_ref[rows, :] = hidden[part]
            n2a_ref[rows, :], wta_ref[rows, :], ma_ref[rows, :] = [item[part] for item in routed[:3]]

    def routing_of(pair):
        packed = [pk_all[s].astype(F32) for s in pair]
        flat = jnp.concatenate(packed + [jnp.zeros((LANES - 8 * len(pair), LANES), F32)], axis=0).T
        cols = [[flat[:, 8 * n + r:8 * n + r + 1] for r in range(4)] for n in range(len(pair))]
        return cols, [(item[4:5, :], item[5:6, :]) for item in packed]

    near[0].wait_recv()
    near[1].wait_recv()
    pair_b((me, partner))
    far[0].wait_recv()
    relay[0].start()
    far[1].wait_recv()
    relay[1].start()
    near[2].wait_recv()
    pair_a((me, partner))
    relay[0].wait_recv()
    relay[1].wait_recv()
    far[2].wait_recv()
    relay[2].start()
    pair_b((across, diag))
    relay[2].wait_recv()
    far[3].wait_recv()
    relay[3].start()
    pair_a((across, diag))
    near[3].wait_recv()
    relay[3].wait_recv()
    for i in range(4):
        far[i].wait_send()
        near[i].wait_send()
        relay[i].wait_send()


def moe_kernel(e_local, n2a_ref, n2b_ref, g_ref, wta_ref, ma_ref, wtb_ref, mb_ref, w1_hbm, w3_hbm, w2_hbm,
               ra_ref, rb_ref, rd_ref, dw1_ref, dw3_ref, dw2_ref, x_a, x_b, xbt, dexp, acc_a, acc_b, dacc, put_a, put_b, wcol, dots, ring_13, ring_2,
               w13_all, w2_all, ring_sem, load_sem, blocks):
    expert, tile = pl.program_id(0), pl.program_id(1)
    n_tile = pl.num_programs(1)
    step = expert * n_tile + tile
    slot = lax.rem(step, RING)

    def leaving(step, slot):
        expert, start = step // n_tile, pl.multiple_of(lax.rem(step, n_tile) * FFN_TILE, FFN_TILE)
        span = pl.ds(start, FFN_TILE)
        return [pltpu.make_async_copy(ring_13.at[slot, :, 0:FFN_TILE], dw1_ref.at[expert, :, span], ring_sem.at[slot, 0]),
                pltpu.make_async_copy(ring_13.at[slot, :, FFN_TILE:2 * FFN_TILE], dw3_ref.at[expert, :, span], ring_sem.at[slot, 1]),
                pltpu.make_async_copy(ring_2.at[slot], dw2_ref.at[expert, span, :], ring_sem.at[slot, 2])]

    def coming(step, slot):
        expert, start = step // n_tile, pl.multiple_of(lax.rem(step, n_tile) * FFN_TILE, FFN_TILE)
        span = pl.ds(start, FFN_TILE)
        return [pltpu.make_async_copy(w1_hbm.at[expert, :, span], w13_all.at[slot, :, 0:FFN_TILE], load_sem.at[slot, 0]),
                pltpu.make_async_copy(w3_hbm.at[expert, :, span], w13_all.at[slot, :, FFN_TILE:2 * FFN_TILE], load_sem.at[slot, 1]),
                pltpu.make_async_copy(w2_hbm.at[expert, span, :], w2_all.at[slot], load_sem.at[slot, 2])]

    @pl.when(step == 0)
    def _():
        for ahead in range(RING):
            for copy in coming(ahead, ahead):
                copy.start()

    n_tok, d_model = n2a_ref.shape
    here = lax.axis_index('ep') * e_local + expert

    def by_rows(which, work, sizes=ROW_SIZES):
        below = 0
        for rows in sizes:
            pl.when((blocks[which] > below) & (blocks[which] <= rows))(functools.partial(work, rows))
            below = rows

    @pl.when(tile == 0)
    def _():
        mine = lax.broadcasted_iota(jnp.int32, (n_tok, LANES), 1) == here
        mine_t = lax.broadcasted_iota(jnp.int32, (LANES, n_tok), 0) == here
        lower = (lax.broadcasted_iota(jnp.int32, (n_tok, n_tok), 0)
                 > lax.broadcasted_iota(jnp.int32, (n_tok, n_tok), 1)).astype(F32).astype(BF16)
        slot_col = lax.broadcasted_iota(jnp.int32, (n_tok, n_tok), 1).astype(F32)
        slot_row = lax.broadcasted_iota(jnp.int32, (n_tok, n_tok), 0).astype(F32)

        def plan(which, mask_ref, put):
            mask = mask_ref[...]
            place = jnp.where(mask > 0, dot_nn(lower, mask.astype(BF16)), -1.0)
            place_col = jnp.sum(jnp.where(mine, place, 0.0), axis=-1, keepdims=True)
            place_row = jnp.sum(jnp.where(mine_t, place.T, 0.0), axis=0, keepdims=True)
            put[...] = (slot_col == place_col).astype(F32).astype(BF16)
            total = jnp.sum(jnp.where(mine, mask, 0.0)).astype(jnp.int32)
            size = jnp.int32(n_tok)
            for rows in ROW_SIZES[-2::-1]:
                size = jnp.where(total <= rows, rows, size)
            blocks[which] = size
            return (slot_row == place_row).astype(F32).astype(BF16)

        take_a, take_b = plan(0, ma_ref, put_a), plan(1, mb_ref, put_b)
        wcol[...] = jnp.broadcast_to(jnp.sum(jnp.where(mine, wta_ref[...], 0.0), axis=-1, keepdims=True), (n_tok, LANES))
        wt_b = jnp.sum(jnp.where(mine, wtb_ref[...], 0.0), axis=-1, keepdims=True)
        scaled = (wt_b * g_ref[...].astype(F32)).astype(BF16)

        def fetch_a(rows):
            x_a[0:rows, :] = dot_nn(take_a[0:rows], n2a_ref[...]).astype(BF16)
            acc_a[0:rows, :] = jnp.zeros((rows, d_model), F32)

        def fetch_b(rows):
            fetched = dot_nn(take_b[0:rows], n2b_ref[...])
            x_b[0:rows, :] = fetched.astype(BF16)
            xbt[:, 0:rows] = fetched.T.astype(BF16)
            dexp[0:rows, :] = dot_nn(take_b[0:rows], scaled).astype(BF16)
            acc_b[0:rows, :] = jnp.zeros((rows, d_model), F32)
            dacc[0:rows, :] = jnp.zeros((rows, d_model), F32)

        by_rows(0, fetch_a, MOVE_SIZES)
        by_rows(1, fetch_b, MOVE_SIZES)

    @pl.when((tile == 0) & (expert == 0))
    def _():
        ra_ref[...] = jnp.zeros_like(ra_ref)
        rb_ref[...] = jnp.zeros_like(rb_ref)
        dots[...] = jnp.zeros_like(dots)

    for copy in coming(step, slot):
        copy.wait()

    @pl.when(step >= RING)
    def _():
        for copy in leaving(step - RING, slot):
            copy.wait()

    w13_ref, w2_ref = w13_all.at[slot], w2_all.at[slot]

    def forward(x, rows):
        both = dot_nn(x[0:rows, :], w13_ref[...])
        gate_pre, up_pre = both[:, 0:FFN_TILE], both[:, FFN_TILE:]
        sig = jax.nn.sigmoid(gate_pre)
        return gate_pre, up_pre, sig, (gate_pre * sig * up_pre).astype(BF16)

    def run_a(rows):
        act = forward(x_a, rows)[3]
        acc_a[0:rows, :] += dot_nn(act, w2_ref[...])

    def run_b(rows):
        gate_pre, up_pre, sig, act = forward(x_b, rows)
        acc_b[0:rows, :] += dot_nn(act, w2_ref[...])
        d_exp = dexp[0:rows, :]
        d_act = dot_nt(d_exp, w2_ref[...]).astype(BF16).astype(F32)
        d_up = (d_act * gate_pre * sig).astype(BF16)
        d_gate = (d_act * up_pre * sig * (1.0 + gate_pre * (1.0 - sig))).astype(BF16)
        d_both = jnp.concatenate([d_gate, d_up], axis=1)
        ring_13[slot] = dot_nn(xbt[:, 0:rows], d_both)
        ring_2[slot] = dot_tn(act, d_exp)
        dacc[0:rows, :] += dot_nt(d_both, w13_ref[...])

    by_rows(1, run_b)
    for copy in leaving(step, slot):
        copy.start()
    by_rows(0, run_a)

    @pl.when(step + RING < pl.num_programs(0) * n_tile)
    def _():
        for copy in coming(step + RING, slot):
            copy.start()

    def return_a(rows):
        ra_ref[...] += wcol[:, 0:1] * dot_nn(put_a[:, 0:rows], acc_a[0:rows, :].astype(BF16))

    def return_b(rows):
        put = put_b[:, 0:rows]
        rb_ref[...] += dot_nn(put, dacc[0:rows, :].astype(BF16))
        out_b = dot_nn(put, acc_b[0:rows, :].astype(BF16))
        pick = jnp.sum(out_b * g_ref[...].astype(F32), axis=-1, keepdims=True)
        lane = lax.broadcasted_iota(jnp.int32, (n_tok, LANES), 1)
        dots[...] += jnp.where(lane == here, pick, 0.0)

    @pl.when(tile == pl.num_programs(1) - 1)
    def _():
        by_rows(0, return_a, MOVE_SIZES)
        by_rows(1, return_b, MOVE_SIZES)

    @pl.when(step == pl.num_programs(0) * n_tile - 1)
    def _():
        flat = dots[...].T
        n_src, n_exp, seq_len = rd_ref.shape
        for src in range(n_src):
            rd_ref[src] = flat[0:n_exp, src * seq_len:(src + 1) * seq_len]
        for back in range(RING - 1, -1, -1):
            for copy in leaving(step - back, lax.rem(step - back, RING)):
                copy.wait()


def tail_kernel(n_ep, n_pp, heads, ra_ref, rb_ref, rd_ref, ha_ref, hb_ref, n2b_ref, gb_ref, rtb_ref, x_ref, q_ref, k_ref, v_ref,
                p_ref, gain1_ref, gain2_ref, wq_ref, wk_ref, wv_ref, wo_ref, wr_ref,
                y_ref, dx_ref, dq_ref, dk_ref, dv_ref, dh_all, dg1_ref, sums_ref,
                near_b, swap_b, sum_b, far_b, near_a, swap_a, sum_a, far_a, near_d, swap_d, sum_d, far_d, small, small_1, small_2, small_3,
                y_own, dx_own, wq_s, wr_s, send_sem, recv_sem):
    me, partner, across, diag = ep_peers()
    stage = lax.axis_index('pp')
    later, earlier = lax.rem(stage + 1, n_pp), lax.rem(stage + n_pp - 1, n_pp)
    seq_len, d_model = y_ref.shape
    sems = (send_sem, recv_sem)
    near, over = {'ep': partner}, {'ep': across}
    greet((near, over, {'pp': later}, {'pp': earlier}))
    span = seq_len // CHUNKS
    parts = [pl.ds(c * span, span) for c in range(CHUNKS)]

    def chunked(src, dst, base, peer):
        return [push(src.at[part], dst.at[part], sems, base + c, peer) for c, part in enumerate(parts)]

    swap_b_c = chunked(rb_ref.at[diag], swap_b, 13, near)
    swap_a_c = chunked(ra_ref.at[diag], swap_a, 13 + CHUNKS, near)
    far_b_c = chunked(sum_b, far_b, 13 + 2 * CHUNKS, over)
    far_a_c = chunked(sum_a, far_a, 13 + 3 * CHUNKS, over)
    y_c = chunked(y_own, y_ref, 13 + 4 * CHUNKS, {'pp': later})
    swap_d_c = push(rd_ref.at[diag], swap_d, sems, 0, near)
    near_b_c = push(rb_ref.at[partner], near_b, sems, 1, near)
    near_d_c = push(rd_ref.at[partner], near_d, sems, 2, near)
    near_a_c = push(ra_ref.at[partner], near_a, sems, 3, near)
    far_d_c = push(sum_d, far_d, sems, 4, over)
    swap_d_c.start()
    for copy in swap_b_c:
        copy.start()
    for copy in (near_d_c, near_b_c, *swap_a_c, near_a_c):
        copy.start()
    swap_d_c.wait_recv()
    sum_d[...] = rd_ref[across] + swap_d[...]
    for c, part in enumerate(parts):
        swap_b_c[c].wait_recv()
        sum_b[part, :] = rb_ref[across, part, :] + swap_b[part, :]
        far_b_c[c].start()
        if c == 0:
            far_d_c.start()
    for c, part in enumerate(parts):
        swap_a_c[c].wait_recv()
        sum_a[part, :] = ra_ref[across, part, :] + swap_a[part, :]
        if c == 0:
            far_a_c[c].start()
    for h in range(heads):
        wq_s[:, h * LANES:(h + 1) * LANES] = wq_ref[h]
    wr_s[...] = jnp.zeros_like(wr_s)
    wr_s[0:wr_ref.shape[0], :] = wr_ref[...]

    gain1, gain2 = gain1_ref[...].astype(F32), gain2_ref[...].astype(F32)
    mine = pl.ds(pl.multiple_of(me * seq_len, seq_len), seq_len)
    route = rtb_ref[mine, :]
    id0, id1, gate0, gate1, keep0, keep1 = [route[:, i:i + 1] for i in range(6)]
    lane = lax.broadcasted_iota(jnp.int32, (seq_len, LANES), 1).astype(F32)
    hot0, hot1 = (lane == id0).astype(F32), (lane == id1).astype(F32)
    h_f32 = hb_ref[mine, :].astype(F32)
    inv = rms_inv(h_f32)
    h_hat = h_f32 * inv
    near_d_c.wait_recv()
    far_d_c.wait_recv()
    tile = rd_ref[me] + near_d[...] + far_d[...]
    dots = jnp.concatenate([tile, jnp.zeros((LANES - tile.shape[0], seq_len), F32)], axis=0).T
    d_gate0 = jnp.where(keep0 > 0, jnp.sum(hot0 * dots, axis=-1, keepdims=True), 0.0)
    d_gate1 = jnp.where(keep1 > 0, jnp.sum(hot1 * dots, axis=-1, keepdims=True), 0.0)
    mean_gate = gate0 * d_gate0 + gate1 * d_gate1
    d_logits = (hot0 * (gate0 * (d_gate0 - mean_gate)) + hot1 * (gate1 * (d_gate1 - mean_gate))).astype(BF16)
    d_routed = dot_nn(d_logits, wr_s[...])
    near_b_c.wait_recv()
    for copy in far_b_c:
        copy.wait_recv()
    d_normed = (rb_ref[me] + near_b[...] + far_b[...]) + d_routed
    d_hat = d_normed * gain2
    d_in = inv * (d_hat - h_hat * jnp.mean(d_hat * h_hat, axis=-1, keepdims=True))
    dh_all[me] = (d_in + gb_ref[me].astype(F32)).astype(BF16)
    dh_far = push(dh_all.at[me], dh_all.at[me], sems, 6, over)
    dh_near = push(dh_all.at[me], dh_all.at[me], sems, 7, near)
    dh_relay = push(dh_all.at[across], dh_all.at[across], sems, 8, near)
    dh_far.start()
    dh_near.start()
    for copy in far_a_c[1:]:
        copy.start()
    small[0:8, :] = dot_tn(d_logits, n2b_ref[mine, :])[0:8, :]
    small[8:16, :] = jnp.broadcast_to(jnp.sum(d_normed * h_hat, axis=0, keepdims=True), (8, d_model))
    small_near = push(small, small_1, sems, 9, near)
    small_near.start()

    head_dim = wk_ref.shape[1]

    def attention_back(s):
        rows = pl.ds(pl.multiple_of(s * seq_len, seq_len), seq_len)
        d_hid = dh_all[s]
        d_out = stack_heads(dot_nt(d_hid, wo_ref[...]).astype(BF16), heads, head_dim)
        probs = p_ref[s]
        d_probs = dot_nt(d_out, v_ref[rows, :])
        d_v = dot_tn(probs.astype(BF16), d_out).astype(BF16)
        d_scores = (probs * (d_probs - jnp.sum(probs * d_probs, axis=-1, keepdims=True)) * head_dim ** -0.5).astype(BF16)
        d_q = unstack_heads(dot_nn(d_scores, k_ref[rows, :]).astype(BF16), heads, seq_len)
        d_k = dot_tn(d_scores, stack_heads(q_ref[rows, :], heads, head_dim)).astype(BF16)
        dq_ref[rows, :], dk_ref[rows, :], dv_ref[rows, :] = d_q, d_k, d_v
        d_norm1 = dot_nt(d_q, wq_s[...]) + dot_nt(d_k, wk_ref[...]) + dot_nt(d_v, wv_ref[...])
        x_f32 = x_ref[s].astype(F32)
        inv1 = rms_inv(x_f32)
        x_hat = x_f32 * inv1
        dg1_ref[s] = jnp.broadcast_to(jnp.sum(d_norm1 * x_hat, axis=0, keepdims=True), (8, d_model))
        return d_hid, d_norm1, inv1, x_hat

    d_hid, d_norm1, inv1, x_hat = attention_back(me)
    d_hat1 = d_norm1 * gain1
    d_x = inv1 * (d_hat1 - x_hat * jnp.mean(d_hat1 * x_hat, axis=-1, keepdims=True)) + d_hid.astype(F32)
    dx_own[...] = d_x.astype(BF16)
    dx_c = push(dx_own, dx_ref, sems, 11, {'pp': earlier})
    dx_c.start()
    small_near.wait_recv()
    small_2[...] = small[...] + small_1[...]
    small_far = push(small_2, small_3, sems, 10, over)
    small_far.start()
    near_a_c.wait_recv()

    def leave_y(c):
        part = parts[c]
        far_a_c[c].wait_recv()
        own = pl.ds(pl.multiple_of(me * seq_len + c * span, span), span)
        y_own[part, :] = (ha_ref[own, :].astype(F32)
                          + (ra_ref[me, part, :] + near_a[part, :] + far_a[part, :])).astype(BF16)
        y_c[c].start()

    leave_y(0)
    dh_near.wait_recv()
    attention_back(partner)
    dh_far.wait_recv()
    dh_relay.start()
    leave_y(1)
    attention_back(across)
    leave_y(2)
    dh_relay.wait_recv()
    attention_back(diag)
    leave_y(3)
    small_far.wait_recv()
    sums_ref[...] = small_2[...] + small_3[...]
    dx_c.wait_recv()
    for copy in y_c:
        copy.wait_recv()
    for copy in (*swap_b_c, *swap_a_c, *far_b_c, *far_a_c, *y_c, swap_d_c, near_b_c, near_d_c, near_a_c, far_d_c, dh_far, dh_near,
                 dh_relay, small_near, small_far, dx_c):
        copy.wait_send()


def dense_kernel(n1_ref, o_ref, dq_ref, dk_ref, dv_ref, dh_ref, dg1_in, sums_in, y_in, dx_in,
                 dwq_ref, dwk_ref, dwv_ref, dwo_ref, dg1_ref, dg2_ref, dwr_ref, y_ref, dx_ref, n1t):
    step = pl.program_id(0)

    @pl.when(step == 0)
    def _():
        n1t[...] = n1_ref[...].astype(F32).T.astype(BF16)
        dwk_ref[...] = dot_nn(n1t[...], dk_ref[...])
        dwv_ref[...] = dot_nn(n1t[...], dv_ref[...])
        dg1_ref[...] = sum(dg1_in[s] for s in range(dg1_in.shape[0]))[0:1]
        dwr_ref[...] = sums_in[0:8, :]
        dg2_ref[...] = sums_in[8:9, :]
        y_ref[...] = y_in[...]
        dx_ref[...] = dx_in[...]

    pair = dot_nn(n1t[...], dq_ref[...])
    for i in range(dwq_ref.shape[0]):
        dwq_ref[i] = pair[:, i * LANES:(i + 1) * LANES]
    dwo_ref[...] = dot_tn(o_ref[...], dh_ref[...])


def shape_of(shape, dtype):
    return jax.ShapeDtypeStruct(shape, dtype)


def solution(mesh):
    n_ep, n_pp = mesh.shape['ep'], mesh.shape['pp']
    whole = pl.BlockSpec(memory_space=VMEM)

    def device_tick(x_a, x_b, g_b, ids_a, ids_b, count_a, count_b, gain_1, gain_2, w_q, w_k, w_v, w_o, w_r, w_1, w_3, w_2):
        seq_len, d_model = x_a.shape[2], x_a.shape[3]
        heads, head_dim = w_q.shape[2], w_q.shape[3]
        n_exp, e_local, ffn = w_r.shape[2], w_1.shape[1], w_1.shape[3]
        n_tok = n_ep * seq_len
        width = heads * head_dim
        xa, xb, gb = x_a[0, 0], x_b[0, 0], g_b[0, 0]
        wq = jnp.transpose(w_q[0], (1, 0, 2))
        wk, wv, wo = w_k[0, :, 0], w_v[0, :, 0], w_o[0].reshape(width, d_model)
        wr = jnp.transpose(w_r[0])
        tok, rows = (n_ep, seq_len, d_model), (n_tok, d_model)
        head_out = [shape_of(tok, BF16), shape_of(tok, BF16), shape_of(rows, BF16), shape_of(rows, BF16),
                    shape_of((n_tok, LANES), F32), shape_of((n_tok, LANES), F32), shape_of((n_tok, LANES), F32),
                    shape_of((n_tok, LANES), F32), shape_of((n_tok, LANES), F32), shape_of(rows, BF16), shape_of(rows, BF16),
                    shape_of(rows, BF16), shape_of((n_tok, width), BF16), shape_of((n_tok, head_dim), BF16),
                    shape_of((n_tok, head_dim), BF16), shape_of((n_ep, heads * seq_len, seq_len), F32),
                    shape_of((n_tok, width), BF16)]
        (xb_all, gb_all, n2a, n2b, wta, m_a, wtb, m_b, rtb, ha, hb, n1, q, k, v, probs, attn) = pl.pallas_call(
            functools.partial(head_kernel, n_ep, heads),
            out_shape=head_out,
            in_specs=[pl.BlockSpec(memory_space=pltpu.HBM)] * 14,
            out_specs=[whole] * len(head_out),
            scratch_shapes=[VMEM(tok, BF16), VMEM((8, LANES), jnp.int32), VMEM((n_ep, 8, LANES), jnp.int32),
                            VMEM((2, seq_len), jnp.int32), VMEM((2, seq_len), jnp.int32), VMEM((1, n_exp), jnp.int32),
                            VMEM((1, n_exp), jnp.int32), VMEM((1, d_model), BF16), VMEM((1, d_model), BF16),
                            VMEM((d_model, width), BF16), VMEM((d_model, head_dim), BF16), VMEM((d_model, head_dim), BF16),
                            VMEM((width, d_model), BF16), VMEM((n_exp, d_model), BF16), VMEM((LANES, d_model), BF16),
                            pltpu.SemaphoreType.DMA((13 + heads,)), pltpu.SemaphoreType.DMA((12,)),
                            pltpu.SemaphoreType.DMA((12,))],
            compiler_params=pltpu.CompilerParams(collective_id=0, has_side_effects=True, vmem_limit_bytes=HEAD_VMEM),
            name='head',
        )(*[pltpu.with_memory_space_constraint(arg, pltpu.HBM) for arg in (
            ids_a[0, 0].T, ids_b[0, 0].T, count_a[0], count_b[0], xa, xb, gb, gain_1, gain_2, wq, wk, wv, wo, wr)])

        n_tile = ffn // FFN_TILE

        def const(*shape):
            return pl.BlockSpec(shape, lambda e, f: (0,) * len(shape))
        hbm = pl.BlockSpec(memory_space=pltpu.HBM)
        r_a, r_b, r_d, dw1, dw3, dw2 = pl.pallas_call(
            functools.partial(moe_kernel, e_local),
            grid=(e_local, n_tile),
            out_shape=[shape_of(rows, F32), shape_of(rows, F32), shape_of((n_ep, n_exp, seq_len), F32), shape_of((e_local, d_model, ffn), F32),
                       shape_of((e_local, d_model, ffn), F32), shape_of((e_local, ffn, d_model), F32)],
            in_specs=[const(*rows)] * 3 + [const(n_tok, LANES)] * 4 + [hbm] * 3,
            out_specs=[const(*rows), const(*rows), const(n_ep, n_exp, seq_len), hbm, hbm, hbm],
            scratch_shapes=[VMEM(rows, BF16), VMEM(rows, BF16), VMEM((d_model, n_tok), BF16), VMEM(rows, BF16),
                            VMEM(rows, F32), VMEM(rows, F32), VMEM(rows, F32), VMEM((n_tok, n_tok), BF16),
                            VMEM((n_tok, n_tok), BF16), VMEM((n_tok, LANES), F32), VMEM((n_tok, LANES), F32), VMEM((RING, d_model, 2 * FFN_TILE), F32),
                            VMEM((RING, FFN_TILE, d_model), F32), VMEM((RING, d_model, 2 * FFN_TILE), BF16),
                            VMEM((RING, FFN_TILE, d_model), BF16), pltpu.SemaphoreType.DMA((RING, 3)),
                            pltpu.SemaphoreType.DMA((RING, 3)), pltpu.SMEM((2,), jnp.int32)],
            compiler_params=pltpu.CompilerParams(dimension_semantics=('arbitrary', 'arbitrary'),
                                                 vmem_limit_bytes=MOE_VMEM),
            name='moe',
        )(n2a, n2b, gb_all.reshape(rows), wta, m_a, wtb, m_b, w_1[0], w_3[0], w_2[0])

        small = (16, d_model)
        block = (seq_len, d_model)
        y_in, dx_in, dq, dk, dv, dh, dg1_in, sums = pl.pallas_call(
            functools.partial(tail_kernel, n_ep, n_pp, heads),
            out_shape=[shape_of(block, BF16), shape_of(block, BF16), shape_of((n_tok, width), BF16),
                       shape_of((n_tok, head_dim), BF16), shape_of((n_tok, head_dim), BF16), shape_of(tok, BF16),
                       shape_of((n_ep, 8, d_model), F32), shape_of(small, F32)],
            in_specs=[whole] * 20,
            out_specs=[whole] * 8,
            scratch_shapes=[VMEM(block, F32)] * 8 + [VMEM((n_exp, seq_len), F32)] * 4 + [VMEM(small, F32)] * 4
            + [VMEM(block, BF16), VMEM(block, BF16), VMEM((d_model, width), BF16), VMEM((LANES, d_model), BF16),
               pltpu.SemaphoreType.DMA((13 + 5 * CHUNKS,)), pltpu.SemaphoreType.DMA((13 + 5 * CHUNKS,))],
            compiler_params=pltpu.CompilerParams(collective_id=1, has_side_effects=True, vmem_limit_bytes=TAIL_VMEM),
            name='tail',
        )(r_a.reshape(tok), r_b.reshape(tok), r_d, ha, hb, n2b, gb_all, rtb, xb_all, q, k, v, probs,
          gain_1, gain_2, wq, wk, wv, wo, wr)

        pair = 2
        steps = heads // pair

        def held(*shape):
            return pl.BlockSpec(shape, lambda i: (0,) * len(shape))
        cols = pl.BlockSpec((n_tok, pair * head_dim), lambda i: (0, i))
        dwq, dwk, dwv, dwo, dg1, dg2, dwr, y_next, dx_prev = pl.pallas_call(
            dense_kernel,
            grid=(steps,),
            out_shape=[shape_of((heads, d_model, head_dim), F32), shape_of((d_model, head_dim), F32),
                       shape_of((d_model, head_dim), F32), shape_of((width, d_model), F32), shape_of((1, d_model), F32),
                       shape_of((1, d_model), F32), shape_of((n_exp, d_model), F32), shape_of(block, BF16), shape_of(block, BF16)],
            in_specs=[held(*rows), cols, cols, held(n_tok, head_dim), held(n_tok, head_dim), held(*rows),
                      held(n_ep, 8, d_model), held(*small), held(*block), held(*block)],
            out_specs=[pl.BlockSpec((pair, d_model, head_dim), lambda i: (i, 0, 0)), held(d_model, head_dim),
                       held(d_model, head_dim), pl.BlockSpec((pair * head_dim, d_model), lambda i: (i, 0)),
                       held(1, d_model), held(1, d_model), held(n_exp, d_model), held(*block), held(*block)],
            scratch_shapes=[VMEM((d_model, n_tok), BF16)],
            compiler_params=pltpu.CompilerParams(dimension_semantics=('arbitrary',), vmem_limit_bytes=DENSE_VMEM),
            name='dense',
        )(n1, attn, dq, dk, dv, dh.reshape(rows), dg1_in, sums, y_in, dx_in)
        return (y_next[None, None], dx_prev[None, None], dg1, dg2, jnp.transpose(dwq, (1, 0, 2))[None], dwk[None, :, None],
                dwv[None, :, None], dwo.reshape(w_o.shape), jnp.transpose(dwr)[None], dw1[None], dw3[None], dw2[None])

    tok_spec = P(('dp', 'pp'), 'ep', None, None)
    cnt_spec = P(('dp', 'pp'), 'ep', None)
    gain_spec = P('pp', None)
    attn_spec = P('pp', None, None, None)
    router_spec = P('pp', None, None)
    expert_spec = P('pp', 'ep', None, None)
    gain_out = P(('dp', 'pp'), None)
    attn_out_spec = P(('dp', 'pp'), None, None, None)
    router_out = P(('dp', 'pp'), None, None)
    expert_out_spec = P(('dp', 'pp'), 'ep', None, None)
    in_specs = (tok_spec, tok_spec, tok_spec, tok_spec, tok_spec, cnt_spec, cnt_spec, gain_spec, gain_spec,
                attn_spec, attn_spec, attn_spec, attn_spec, router_spec, expert_spec, expert_spec, expert_spec)
    out_specs = (tok_spec, tok_spec, gain_out, gain_out, attn_out_spec, attn_out_spec, attn_out_spec, attn_out_spec,
                 router_out, expert_out_spec, expert_out_spec, expert_out_spec)
    return jax.shard_map(device_tick, mesh=mesh, in_specs=in_specs, out_specs=out_specs, check_vma=False)
```
